32 devices in a mesh: blade: 16 (over z, y, x), span: 2 (over core).
Axes of the slice: x: 2, y: 2, z: 4, core: 2. Of those that a mesh axis runs over, the one named last changes fastest.
Arguments:
- particles: float32 [11, 32, 64, 128], P(None, 'blade', 'span')
- filled: int32 [32, 64], P('blade', 'span'), may hold values from 2 to 96, as said below
- contact_pairs: int32 [2, 32, 64, 128], P(None, 'blade', 'span'), may hold values from 0 to 639, as said below
- contact_count: int32 [32, 64], P('blade', 'span'), may hold values from 32 to 128
- movers_out: int32 [2, 2, 16, 32], P(None, None, 'blade', 'span'), may hold values from 0 to 95, as said below
- movers_in: int32 [2, 2, 16, 32], P(None, None, 'blade', 'span'), may hold values from 0 to 127, as said below
- move_count: int32 [2, 16, 2], P(None, 'blade', 'span'), may hold values from 0 to 16, as said below
Outputs:
- advanced: float32 [11, 32, 64, 128], P(None, 'blade', 'span')
The draws below stay inside these ranges and needn't reach their ends.
Inputs may be any that keep to these rules, and one draw needn't show every extreme that they name: Live slots of a cell are its first filled ones. `contact_pairs`: every entry, counted or not, joins two live particles; direction 0 joins a slot with a higher slot of the same cell; directions never point outside the grid. The same pair may be listed more than once and then acts once per entry. `movers_out`: component 0 holds cells of the block (0 to 63), component 1 slots (below 96). Forward leavers sit in the block's last blade row, backward leavers in its first; within a device block and direction each leaver has its own cell, and each is a live slot. `movers_in`: component 0 holds cells of the block (0 to 63), component 1 slots. Arrivals from behind land in the block's first blade row, from ahead in its last; every slot is 96 or higher, and the 32 slots of one device block are all different. `move_count`: zero in the forward direction on the last blade device and in the backward direction on the first.
All inputs are finite; a program needn't handle non-finite values.
Results may differ from the reference program's by a relative error of at most 0.0001.
Values sent between devices are 32-bit elements; how exact they have to be, the bound alone decides.
A program may use at most 64 MiB of HBM per device.

```python
import jax
import jax.numpy as jnp
from jax import lax

CB = 2
CS = 32
SLOTS = 128
FILL_MOST = 96
KC = 128
MIG = 16
NB = 32
NS = 64


def fill_counts(key):
    return jax.random.randint(jax.random.fold_in(key, 7), (NB, NS), 2, FILL_MOST + 1)


def draw_filled(key, part):
    return fill_counts(key).astype(jnp.int32)


def draw_particles(key, part):
    counts = fill_counts(key)
    occupancy_marks = (jnp.arange(SLOTS) < counts[..., None]).astype(jnp.float32)
    noise_seeds = jax.random.split(jax.random.fold_in(key, 3), 5)
    patch_extents = (NB, NS, SLOTS)
    bottom_boundary = jax.random.uniform(noise_seeds[0], (2,) + patch_extents, jnp.float32)
    powder_thickness = jax.random.uniform(noise_seeds[1], (1,) + patch_extents, jnp.float32, 0.0, 4.0)
    kinematic_advance = 0.5 * jax.random.normal(noise_seeds[2], (6,) + patch_extents, jnp.float32)
    grain_halfwidth = jnp.exp(jax.random.uniform(noise_seeds[3], (1,) + patch_extents, jnp.float32, jnp.log(0.12), jnp.log(0.25)))
    grain_warmth = jax.random.uniform(noise_seeds[4], (1,) + patch_extents, jnp.float32)
    grain_record = jnp.concatenate([bottom_boundary, powder_thickness, kinematic_advance, grain_halfwidth, grain_warmth], 0)
    return (grain_record * occupancy_marks[None]).astype(jnp.float32)


def draw_contact_pairs(key, part):
    counts = fill_counts(key)
    noise_seeds = jax.random.split(jax.random.fold_in(key, 5), 3)
    direction = jax.random.randint(noise_seeds[0], (NB, NS, KC), 0, 5)
    row_idx = jnp.arange(NB)[:, None, None]
    col_idx = jnp.arange(NS)[None, :, None]
    blocked = (row_idx == NB - 1) & ((direction == 1) | (direction == 3) | (direction == 4))
    blocked = blocked | (col_idx == NS - 1) & ((direction == 2) | (direction == 3))
    blocked = blocked | (col_idx == 0) & (direction == 4)
    direction = jnp.where(blocked, 0, direction)
    row_step = jnp.where((direction == 0) | (direction == 2), 0, 1)
    col_step = jnp.where((direction == 2) | (direction == 3), 1, jnp.where(direction == 4, -1, 0))
    own_fill = jnp.broadcast_to(counts[:, :, None], (NB, NS, KC))
    other_fill = counts[row_idx + row_step, col_idx + col_step]
    draw_one = jax.random.randint(noise_seeds[1], (NB, NS, KC), 0, 1 << 20)
    draw_two = jax.random.randint(noise_seeds[2], (NB, NS, KC), 0, 1 << 20)
    self_first = draw_one % (own_fill - 1)
    self_second = self_first + 1 + draw_two % (own_fill - 1 - self_first)
    is_self = direction == 0
    first_slot = jnp.where(is_self, self_first, draw_one % own_fill)
    second_slot = jnp.where(is_self, self_second, draw_two % other_fill)
    return jnp.stack([first_slot, direction * SLOTS + second_slot]).astype(jnp.int32)


def draw_movers_out(key, part):
    blade_blocks = NB // CB
    span_blocks = NS // CS
    counts = fill_counts(key)
    noise_seeds = jax.random.split(jax.random.fold_in(key, 9), 2)
    scores = jax.random.randint(noise_seeds[0], (2, blade_blocks, span_blocks, CS), 0, 1 << 16) * CS + jnp.arange(CS)
    columns = jnp.argsort(scores, axis=-1)[..., :MIG]
    edge_row = jnp.array([CB - 1, 0])[:, None, None, None]
    cells = edge_row * CS + columns
    global_row = jnp.arange(blade_blocks)[None, :, None, None] * CB + edge_row
    global_col = jnp.arange(span_blocks)[None, None, :, None] * CS + columns
    fill_here = counts[global_row, global_col]
    slot_ids = jax.random.randint(noise_seeds[1], (2, blade_blocks, span_blocks, MIG), 0, 1 << 20) % fill_here
    joined = jnp.stack([cells, slot_ids], 1)
    return joined.reshape(2, 2, blade_blocks, span_blocks * MIG).astype(jnp.int32)


def draw_movers_in(key, part):
    blade_blocks = NB // CB
    span_blocks = NS // CS
    spare = SLOTS - FILL_MOST
    noise_seeds = jax.random.split(jax.random.fold_in(key, 13), 2)
    columns = jax.random.randint(noise_seeds[0], (2, blade_blocks, span_blocks, MIG), 0, CS)
    edge_row = jnp.array([0, CB - 1])[:, None, None, None]
    cells = edge_row * CS + columns
    scores = jax.random.randint(noise_seeds[1], (blade_blocks, span_blocks, spare), 0, 1 << 16) * spare + jnp.arange(spare)
    chosen = jnp.argsort(scores, axis=-1)[..., :2 * MIG].reshape(blade_blocks, span_blocks, 2, MIG)
    slot_ids = FILL_MOST + jnp.transpose(chosen, (2, 0, 1, 3))
    joined = jnp.stack([cells, slot_ids], 1)
    return joined.reshape(2, 2, blade_blocks, span_blocks * MIG).astype(jnp.int32)


def draw_move_count(key, part):
    blade_blocks = NB // CB
    span_blocks = NS // CS
    counts = jax.random.randint(jax.random.fold_in(key, 17), (2, blade_blocks, span_blocks), 0, MIG + 1)
    block_idx = jnp.arange(blade_blocks)[None, :, None]
    dir_idx = jnp.arange(2)[:, None, None]
    outside = (dir_idx == 0) & (block_idx == blade_blocks - 1) | (dir_idx == 1) & (block_idx == 0)
    return jnp.where(outside, 0, counts).astype(jnp.int32)


def set_ends(values, key, low, high):
    shape = values.shape
    spot = [jax.random.randint(jax.random.fold_in(key, axis), (), 0, shape[axis]) for axis in range(len(shape))]
    values = values.at[tuple(spot)].set(low)
    longest = shape.index(max(shape))
    spot[longest] = (spot[longest] + 1) % shape[longest]
    return values.at[tuple(spot)].set(high)


def setup_inputs(seed: int = 0) -> dict:
    keys = jax.random.split(jax.random.key(seed), 8)
    return {
        "particles": draw_particles(jax.random.fold_in(keys[7], 71), 0),
        "filled": draw_filled(jax.random.fold_in(keys[7], 71), 0),
        "contact_pairs": draw_contact_pairs(jax.random.fold_in(keys[7], 71), 0),
        "contact_count": set_ends(jax.random.randint(keys[3], (NB, NS), KC // 4, KC + 1), jax.random.fold_in(keys[3], 1), KC // 4, KC).astype(jnp.int32),
        "movers_out": draw_movers_out(jax.random.fold_in(keys[7], 71), 0),
        "movers_in": draw_movers_in(jax.random.fold_in(keys[7], 71), 0),
        "move_count": draw_move_count(jax.random.fold_in(keys[7], 71), 0),
    }


spring = 4.0
normal_damp = 0.5
tangent_damp = 0.3
conduct = 40.0
timestep_length = 0.05
density = 100.0
gravity = 9.81
soft_len = 0.05

def cross_product(left_vec, right_vec):
    return jnp.stack([left_vec[1] * right_vec[2] - left_vec[2] * right_vec[1], left_vec[2] * right_vec[0] - left_vec[0] * right_vec[2], left_vec[0] * right_vec[1] - left_vec[1] * right_vec[0]])

def pair_terms(first_state, second, row_shift, col_shift, occupancy_marks):
    offset = jnp.stack([row_shift, col_shift, jnp.zeros_like(row_shift)])
    gap_vec = second[0:3] + offset - first_state[0:3]
    distance = jnp.sqrt(lax.optimization_barrier(jnp.sum(gap_vec * gap_vec, axis=0)) + soft_len * soft_len)
    normal = gap_vec / distance
    rad_first = first_state[9]
    rad_second = second[9]
    intersection = rad_first + rad_second - distance
    spin_sum = rad_first * first_state[6:9] + rad_second * second[6:9]
    relative = second[3:6] - first_state[3:6] - cross_product(spin_sum, normal)
    normal_speed = lax.optimization_barrier(jnp.sum(relative * normal, axis=0))
    friction = tangent_damp * (relative - normal_speed * normal)
    contact_force = (normal_damp * normal_speed - spring * intersection) * normal + friction
    torque_dir = cross_product(normal, friction)
    denom = jnp.where(occupancy_marks > 0, rad_first + rad_second, 1.0)
    heat_flow = 2.0 * conduct * rad_first * rad_second / denom * (second[10] - first_state[10])
    on_first = jnp.concatenate([contact_force, rad_first * torque_dir, heat_flow[None]], 0) * occupancy_marks
    on_second = jnp.concatenate([-contact_force, rad_second * torque_dir, -heat_flow[None]], 0) * occupancy_marks
    return (on_first, on_second)

def accumulate(ghosted, pairs, occupancy_marks, first_row, first_col, cumulative_sums):
    components = ghosted.shape[0]
    span_all = ghosted.shape[2]
    tile_slots = ghosted.shape[3]
    flattened = ghosted.reshape(components, -1)
    row_at = (first_row + jnp.arange(pairs.shape[1], dtype=jnp.int32))[:, None, None]
    col_at = (first_col + jnp.arange(pairs.shape[2], dtype=jnp.int32))[None, :, None]
    direction = pairs[1] // tile_slots
    target = pairs[1] % tile_slots
    row_step = jnp.where((direction == 0) | (direction == 2), 0, 1).astype(jnp.int32)
    col_step = jnp.where((direction == 2) | (direction == 3), 1, jnp.where(direction == 4, -1, 0)).astype(jnp.int32)
    first_at = ((row_at * span_all + col_at) * tile_slots + pairs[0]).reshape(-1)
    second_at = (((row_at + row_step) * span_all + col_at + col_step) * tile_slots + target).reshape(-1)
    first_state = jnp.take(flattened, first_at, axis=1)
    second = jnp.take(flattened, second_at, axis=1)
    on_first, on_second = pair_terms(first_state, second, row_step.reshape(-1).astype(jnp.float32), col_step.reshape(-1).astype(jnp.float32), occupancy_marks.reshape(-1))
    return cumulative_sums.at[:, first_at].add(on_first).at[:, second_at].add(on_second)

def advance(grain_record, cumulative_sums, occupancy_marks):
    grain_halfwidth = grain_record[9]
    safe_radius = grain_halfwidth + (1.0 - occupancy_marks)
    grain_inertia = density * safe_radius ** 3
    accel_vec = cumulative_sums[0:3] / grain_inertia
    accel_vec = jnp.concatenate([accel_vec[0:2], accel_vec[2:3] - gravity], 0)
    translational_rate = grain_record[3:6] + timestep_length * accel_vec
    spin_rate = grain_record[6:9] + timestep_length * cumulative_sums[3:6] / (0.4 * grain_inertia * safe_radius * safe_radius)
    grain_location = grain_record[0:3] + timestep_length * translational_rate
    grain_warmth = grain_record[10] + timestep_length * cumulative_sums[6] / grain_inertia
    return jnp.concatenate([grain_location, translational_rate, spin_rate, grain_halfwidth[None], grain_warmth[None]], 0) * occupancy_marks

def reference(particles, filled, contact_pairs, contact_count, movers_out, movers_in, move_count):
    components = particles.shape[0]
    ghosted = jnp.pad(particles, ((0, 0), (1, 1), (1, 1), (0, 0)))
    live_pairs = (jnp.arange(KC, dtype=jnp.int32) < contact_count[..., None]).astype(jnp.float32)
    empty = jnp.zeros((7, (NB + 2) * (NS + 2) * SLOTS), jnp.float32)

    def block_step(block_index, cumulative_sums):
        first_row = (block_index * CB).astype(jnp.int32)
        pairs = lax.dynamic_slice_in_dim(contact_pairs, first_row, CB, 1)
        occupancy_marks = lax.dynamic_slice_in_dim(live_pairs, first_row, CB, 0)
        return accumulate(ghosted, pairs, occupancy_marks, first_row + 1, 1, cumulative_sums)
    cumulative_sums = lax.fori_loop(0, NB // CB, block_step, empty)
    cumulative_sums = cumulative_sums.reshape(7, NB + 2, NS + 2, SLOTS)[:, 1:-1, 1:-1]
    occupancy_marks = (jnp.arange(SLOTS, dtype=jnp.int32) < filled[..., None]).astype(jnp.float32)
    stepped = advance(particles, cumulative_sums, occupancy_marks)
    blade_blocks = NB // CB
    span_blocks = NS // CS
    flattened = stepped.reshape(components, -1)
    block_row = jnp.arange(blade_blocks, dtype=jnp.int32)[None, :, None, None]
    block_col = jnp.arange(span_blocks, dtype=jnp.int32)[None, None, :, None]

    def global_at(cells, slot_ids):
        return ((block_row * CB + cells // CS) * NS + block_col * CS + cells % CS) * SLOTS + slot_ids
    leaving = movers_out.reshape(2, 2, blade_blocks, span_blocks, MIG)
    sources = global_at(leaving[:, 0], leaving[:, 1])
    moving = (jnp.arange(MIG, dtype=jnp.int32) < move_count[..., None]).astype(jnp.float32)
    initial = jnp.take(flattened, sources.reshape(-1), axis=1).reshape(components, 2, blade_blocks, span_blocks, MIG)
    sent = initial * moving
    signs_dir = jnp.array([-1.0, 1.0], jnp.float32).reshape(2, 1, 1, 1)
    sent = sent.at[0].add(signs_dir * moving)
    flattened = flattened.at[:, sources.reshape(-1)].set((initial * (1.0 - moving)).reshape(components, -1))
    arriving = movers_in.reshape(2, 2, blade_blocks, span_blocks, MIG)
    targets = global_at(arriving[:, 0], arriving[:, 1])
    flattened = flattened.at[:, targets[0, 1:].reshape(-1)].set(sent[:, 0, :-1].reshape(components, -1))
    flattened = flattened.at[:, targets[1, :-1].reshape(-1)].set(sent[:, 1, 1:].reshape(components, -1))
    return flattened.reshape(particles.shape)
```

```python
import functools

import jax
import jax.numpy as jnp
from jax import lax
from jax.experimental import pallas as pl
from jax.experimental.pallas import tpu as pltpu
from jax.sharding import PartitionSpec as P

spring = 4.0
normal_damp = 0.5
tangent_damp = 0.3
conduct = 40.0
timestep_length = 0.05
density = 100.0
gravity = 9.81
soft_len = 0.05
row_steps = (0, 1, 0, 1, 1)
col_steps = (0, 0, 1, 1, -1)
MESH = pl.DeviceIdType.MESH
TILE = 8
VMEM_GRANT = 16 << 20


def cross(a, b):
    return (
        a[1] * b[2] - a[2] * b[1],
        a[2] * b[0] - a[0] * b[2],
        a[0] * b[1] - a[1] * b[0],
    )


def lanes_of(table, index):
    return jnp.take_along_axis(table, index, axis=1, mode="promise_in_bounds")


def pair_terms(first, second, row_shift, col_shift, live):
    gap = (
        second[0] + row_shift - first[0],
        second[1] + col_shift - first[1],
        second[2] - first[2],
    )
    distance = jnp.sqrt(gap[0] * gap[0] + gap[1] * gap[1] + gap[2] * gap[2] + soft_len * soft_len)
    inverse = 1.0 / distance
    normal = tuple(g * inverse for g in gap)
    rad_first, rad_second = first[9], second[9]
    intersection = rad_first + rad_second - distance
    spin = tuple(rad_first * first[6 + c] + rad_second * second[6 + c] for c in range(3))
    turn = cross(spin, normal)
    relative = tuple(second[3 + c] - first[3 + c] - turn[c] for c in range(3))
    speed = relative[0] * normal[0] + relative[1] * normal[1] + relative[2] * normal[2]
    friction = tuple(tangent_damp * (relative[c] - speed * normal[c]) for c in range(3))
    push = normal_damp * speed - spring * intersection
    force = tuple(push * normal[c] + friction[c] for c in range(3))
    torque = cross(normal, friction)
    denom = jnp.where(live, rad_first + rad_second, 1.0)
    heat = 2.0 * conduct * rad_first * rad_second / denom * (second[10] - first[10])
    on_first = force + tuple(rad_first * t for t in torque) + (heat,)
    on_second = tuple(-f for f in force) + tuple(rad_second * t for t in torque) + (-heat,)
    keep = lambda v: jnp.where(live, v, 0.0)
    return [keep(v) for v in on_first], [keep(v) for v in on_second]


def kernel(
    shape,
    blades,
    spans,
    parts_hbm,
    filled_hbm,
    pairs_hbm,
    count_hbm,
    out_movers_hbm,
    in_movers_hbm,
    move_count_hbm,
    out_ref,
    ghost,
    pairs_ref,
    count_own,
    count_prev,
    filled_ref,
    out_movers,
    in_movers,
    move_count,
    first_terms,
    second_terms,
    count_wide,
    filled_wide,
    totals,
    owed_low,
    owed_high,
    msg_out,
    msg_in,
    local_sem,
    send_sem,
    recv_sem,
):
    components, rows, cols, slots = shape
    movers = out_movers.shape[3]
    wide = cols + 2
    i = lax.axis_index("blade")
    j = lax.axis_index("span")
    has = {}
    for di in (-1, 0, 1):
        for dj in (-1, 0, 1):
            if (di, dj) != (0, 0):
                a, b = i + di, j + dj
                has[di, dj] = (a >= 0) & (a < blades) & (b >= 0) & (b < spans)

    own_cols = slice(TILE, TILE + cols)
    own = [
        pltpu.make_async_copy(source, target, local_sem.at[n])
        for n, (source, target) in enumerate(
            (
                (count_hbm, count_own),
                (filled_hbm, filled_ref),
                (pairs_hbm, pairs_ref.at[:, 1 : rows + 1]),
                (parts_hbm, ghost.at[:, 1 : rows + 1, own_cols, :]),
                (out_movers_hbm, out_movers),
                (in_movers_hbm, in_movers),
                (move_count_hbm, move_count),
            )
        )
    ]
    barrier = pltpu.get_barrier_semaphore()
    expected = jnp.int32(0)
    for (di, dj), there in has.items():
        expected = expected + there.astype(jnp.int32)

        @pl.when(there)
        def _(di=di, dj=dj):
            pl.semaphore_signal(
                barrier, inc=1, device_id=(i + di, j + dj), device_id_type=MESH
            )

    for copy in own:
        copy.start()
    pl.semaphore_wait(barrier, expected)

    def remote(which, source, target, di, dj):
        return pltpu.make_async_remote_copy(
            src_ref=source,
            dst_ref=target,
            send_sem=send_sem.at[which],
            recv_sem=recv_sem.at[which],
            device_id=(i + di, j + dj),
            device_id_type=MESH,
        )

    low = slice(0, 1)
    high = slice(cols - 1, cols)
    left = slice(TILE - 1, TILE)
    right = slice(TILE + cols, TILE + cols + 1)
    last = slice(rows - 1, rows)
    after = slice(rows + 1, rows + 2)
    moves = (
        (parts_hbm.at[:, 0:1], ghost.at[:, after, own_cols, :], -1, 0),
        (parts_hbm.at[:, :, low, :], ghost.at[:, 1 : rows + 1, right, :], 0, -1),
        (parts_hbm.at[:, :, high, :], ghost.at[:, 1 : rows + 1, left, :], 0, 1),
        (parts_hbm.at[:, 0:1, low, :], ghost.at[:, after, right, :], -1, -1),
        (parts_hbm.at[:, 0:1, high, :], ghost.at[:, after, left, :], -1, 1),
        (parts_hbm.at[:, last], ghost.at[:, 0:1, own_cols, :], 1, 0),
        (pairs_hbm.at[:, last], pairs_ref.at[:, 0:1], 1, 0),
        (count_hbm, count_prev, 1, 0),
        (totals.at[1:rows, wide - 1], owed_low.at[1:rows], 0, 1),
        (totals.at[1:rows, 0], owed_high.at[1:rows], 0, -1),
        (msg_out.at[0], msg_in.at[0], 1, 0),
        (msg_out.at[1], msg_in.at[1], -1, 0),
        (totals.at[0:1, wide - 1], owed_low.at[0:1], 0, 1),
        (totals.at[0:1, 0], owed_high.at[0:1], 0, -1),
    )
    copies = [
        (remote(n, source, target, di, dj), di, dj)
        for n, (source, target, di, dj) in enumerate(moves)
    ]

    def start(*which):
        for w in which:
            copy, di, dj = copies[w]

            @pl.when(has[di, dj])
            def _(copy=copy):
                copy.start()

    def arrive(*which):
        for w in which:
            copy, di, dj = copies[w]

            @pl.when(has[-di, -dj])
            def _(copy=copy):
                copy.wait_recv()

    def sent(*which):
        for w in which:
            copy, di, dj = copies[w]

            @pl.when(has[di, dj])
            def _(copy=copy):
                copy.wait_send()

    start(1, 2, 3, 4, 7, 6, 5, 0)

    diagonal = lax.broadcasted_iota(jnp.int32, (cols, cols), 0) == lax.broadcasted_iota(
        jnp.int32, (cols, cols), 1
    )

    def spread(source, r, target, at):
        line = jnp.broadcast_to(source[r : r + 1, :].astype(jnp.float32), (cols, cols))
        column = jnp.sum(jnp.where(diagonal, line, 0.0), axis=1, keepdims=True)
        target[at] = jnp.broadcast_to(column, (cols, slots))

    def clear(n, _):
        for r in range(rows):
            totals[r, n] = jnp.zeros((8, slots), jnp.float32)
        return 0

    lax.fori_loop(0, wide, clear, 0)
    lane = lax.broadcasted_iota(jnp.int32, (TILE, slots), 1)
    lane_f = lane.astype(jnp.float32)
    groups = cols // TILE

    def force_row(r, headings):
        def group(g, _):
            at = pl.multiple_of(g * TILE, TILE)
            ids = pairs_ref[0, r, pl.ds(at, TILE), :]
            code = pairs_ref[1, r, pl.ds(at, TILE), :]
            heading = code // slots
            target = code - heading * slots
            live = lane_f < count_wide[r, pl.ds(at, TILE), :]
            ids = jnp.clip(ids, 0, slots - 1)
            first = [
                lanes_of(ghost[c, r, pl.ds(at + TILE, TILE), :], ids) for c in range(components)
            ]
            second = [None] * components
            for n, d in enumerate(headings):
                pick = heading == d
                for c in range(components):
                    rows_at = pl.ds(at + TILE + col_steps[d], TILE)
                    value = lanes_of(ghost[c, r + row_steps[d], rows_at, :], target)
                    second[c] = value if n == 0 else jnp.where(pick, value, second[c])
            row_shift = jnp.where((heading == 0) | (heading == 2), 0.0, 1.0)
            col_shift = jnp.where(
                (heading == 2) | (heading == 3), 1.0, jnp.where(heading == 4, -1.0, 0.0)
            )
            on_first, on_second = pair_terms(first, second, row_shift, col_shift, live)
            zero = jnp.zeros((TILE, slots), jnp.float32)
            base = (r * cols + g * TILE) * 8
            for c, (a, b) in enumerate(zip(on_first + [zero], on_second + [zero])):
                first_terms[pl.ds(base + c, TILE, stride=8), :] = a
                second_terms[pl.ds(base + c, TILE, stride=8), :] = b
            return 0

        lax.fori_loop(0, groups, group, 0)

    slot_ids = lax.broadcasted_iota(jnp.int32, (slots, slots), 0)

    def scatter_row(r, near_too, headings):
        count = len(headings) * 8

        def group(g, _):
            at = pl.multiple_of(g * TILE, TILE)
            ids = pairs_ref[0, r, pl.ds(at, TILE), :]
            code = pairs_ref[1, r, pl.ds(at, TILE), :]
            heading = code // slots
            target = code - heading * slots
            for n in range(TILE):
                base = pl.multiple_of((r * cols + g * TILE + n) * 8, 8)
                b = second_terms[pl.ds(base, 8), :]
                head = heading[n : n + 1]
                terms = jnp.concatenate(
                    [jnp.where(head == d, b, 0.0) for d in headings], axis=0
                )
                hot = jnp.where(slot_ids == target[n : n + 1], 1.0, 0.0)
                if near_too:
                    a = first_terms[pl.ds(base, 8), :]
                    zero = jnp.zeros((8, slots), jnp.float32)
                    near = jnp.concatenate([a] + [zero] * (len(headings) - 1), axis=0)
                    terms = jnp.concatenate([near, terms], axis=1)
                    near_hot = jnp.where(slot_ids == ids[n : n + 1], 1.0, 0.0)
                    hot = jnp.concatenate([near_hot, hot], axis=1)
                coarse = terms.astype(jnp.bfloat16).astype(jnp.float32)
                split = jnp.concatenate([coarse, terms - coarse], axis=0).astype(jnp.bfloat16)
                summed = lax.dot_general(
                    split,
                    hot.astype(jnp.bfloat16),
                    (((1,), (1,)), ((), ())),
                    preferred_element_type=jnp.float32,
                )
                summed = summed[:count] + summed[count:]
                for m, d in enumerate(headings):
                    col = g * TILE + n + 1 + col_steps[d]
                    totals[r - 1 + row_steps[d], col] += summed[m * 8 : m * 8 + 8]
            return 0

        lax.fori_loop(0, groups, group, 0)

    def step_row(r):
        for g in range(groups):
            cells = slice(g * TILE, (g + 1) * TILE)
            sums = []
            for c in range(7):
                s = totals[r, 1 + g * TILE : 1 + (g + 1) * TILE, c, :]
                sums.append(s)
            live = lane_f < filled_wide[r, cells, :]
            state = [ghost[c, r + 1, TILE + g * TILE : TILE + (g + 1) * TILE, :] for c in range(components)]
            safe = jnp.where(live, state[9], 1.0)
            mass = density * safe * safe * safe
            inverse = 1.0 / mass
            spin_inverse = 1.0 / (0.4 * mass * safe * safe)
            keep = lambda v: jnp.where(live, v, 0.0)
            for c in range(3):
                accel = sums[c] * inverse
                if c == 2:
                    accel = accel - gravity
                speed = state[3 + c] + timestep_length * accel
                out_ref[c, r, cells, :] = keep(state[c] + timestep_length * speed)
                out_ref[3 + c, r, cells, :] = keep(speed)
                out_ref[6 + c, r, cells, :] = keep(
                    state[6 + c] + timestep_length * sums[3 + c] * spin_inverse
                )
            out_ref[9, r, cells, :] = keep(state[9])
            out_ref[10, r, cells, :] = keep(state[10] + timestep_length * sums[6] * inverse)

    line_lane = lax.broadcasted_iota(jnp.int32, (1, slots), 1)
    cell_ids = lax.broadcasted_iota(jnp.int32, (cols, slots), 0)
    lane_ids = lax.broadcasted_iota(jnp.int32, (cols, slots), 1)

    def leave(direction, r):
        cell_line = jnp.full((1, slots), -1, jnp.int32)
        slot_line = jnp.zeros((1, slots), jnp.int32)
        for k in range(movers):
            cell_line = jnp.where(line_lane == k, out_movers[direction, 0, 0, k] - r * cols, cell_line)
            slot_line = jnp.where(line_lane == k, out_movers[direction, 1, 0, k], slot_line)
        moving = line_lane < move_count[0, 0, direction]
        chosen = (cell_ids == cell_line) & moving
        slot_f = jnp.where(chosen, jnp.broadcast_to(slot_line + 1, (cols, slots)).astype(jnp.float32), 0.0)
        slot_of = jnp.sum(slot_f, axis=1, keepdims=True).astype(jnp.int32) - 1
        slot_of = jnp.broadcast_to(slot_of, (cols, slots))
        leaving = lane_ids == slot_of
        index = jnp.maximum(slot_of, 0)
        shift = jnp.where(moving, -1.0 if direction == 0 else 1.0, 0.0)
        for c in range(components):
            value = out_ref[c, r]
            spread = lanes_of(value, index)
            line = jnp.sum(jnp.where(chosen, spread, 0.0), axis=0, keepdims=True)
            if c == 0:
                line = line + shift
            msg_out[direction, c : c + 1, :] = line
            out_ref[c, r] = jnp.where(leaving, 0.0, value)

    def put(direction, r, there):
        key = jnp.zeros((1, slots), jnp.int32)
        cell_line = jnp.full((1, slots), -1, jnp.int32)
        for k in range(movers):
            hit = line_lane == in_movers[direction, 1, 0, k]
            key = jnp.where(hit, k, key)
            cell_line = jnp.where(hit, in_movers[direction, 0, 0, k] - r * cols, cell_line)
        cell_line = jnp.where(there, cell_line, -1)
        landing = cell_ids == cell_line
        key = jnp.broadcast_to(key, (msg_in.shape[1], slots))
        values = lanes_of(msg_in[direction], key)
        for c in range(components):
            out_ref[c, r] = jnp.where(landing, values[c : c + 1], out_ref[c, r])

    every, inside, across = (0, 1, 2, 3, 4), (0, 2), (1, 3, 4)
    for c in range(msg_out.shape[1] - components):
        for d in range(2):
            msg_out[d, components + c : components + c + 1, :] = jnp.zeros((1, slots), jnp.float32)
    for copy in own:
        copy.wait()
    for r in range(rows):
        spread(count_own, r, count_wide, r + 1)
        spread(filled_ref, r, filled_wide, r)
    arrive(1, 2)
    for r in range(1, rows):
        force_row(r, every)
        scatter_row(r, True, every)
    arrive(7, 6, 5)
    spread(count_prev, rows - 1, count_wide, 0)
    count_wide[0] = jnp.where(has[-1, 0], count_wide[0], 0.0)
    force_row(0, across)
    scatter_row(0, False, across)
    arrive(3, 4, 0)
    force_row(rows, every)
    scatter_row(rows, True, inside)
    start(8, 9, 12, 13)
    arrive(8, 9)

    def add_owed(r):
        totals[r, 1] += jnp.where(has[0, -1], owed_low[r], 0.0)
        totals[r, cols] += jnp.where(has[0, 1], owed_high[r], 0.0)

    for r in range(1, rows):
        add_owed(r)
        step_row(r)
    if rows > 1:
        leave(0, rows - 1)
        start(10)
    arrive(12, 13)
    add_owed(0)
    step_row(0)
    if rows == 1:
        leave(0, 0)
        start(10)
    leave(1, 0)
    start(11)
    sent(*range(10), 12, 13)
    arrive(10)
    put(0, 0, has[-1, 0])
    arrive(11)
    put(1, rows - 1, has[1, 0])
    sent(10, 11)


def body(blades, spans, particles, filled, contact_pairs, contact_count, movers_out, movers_in, move_count):
    components, rows, cols, slots = particles.shape
    padded = -(-components // 8) * 8
    f32, i32 = jnp.float32, jnp.int32
    remote_copies = 14
    return pl.pallas_call(
        functools.partial(kernel, particles.shape, blades, spans),
        out_shape=pltpu.VMEM(particles.shape, f32),
        in_specs=[pl.BlockSpec(memory_space=pl.ANY)] * 7,
        out_specs=pl.BlockSpec(memory_space=pltpu.VMEM),
        scratch_shapes=[
            pltpu.VMEM((components, rows + 2, cols + 2 * TILE, slots), f32),
            pltpu.VMEM((2, rows + 1, cols, contact_pairs.shape[3]), i32),
            pltpu.VMEM((rows, cols), i32),
            pltpu.VMEM((rows, cols), i32),
            pltpu.VMEM((rows, cols), i32),
            pltpu.SMEM(movers_out.shape, i32),
            pltpu.SMEM(movers_in.shape, i32),
            pltpu.SMEM((1, 1, 2), i32),
            pltpu.VMEM(((rows + 1) * cols * 8, slots), f32),
            pltpu.VMEM(((rows + 1) * cols * 8, slots), f32),
            pltpu.VMEM((rows + 1, cols, slots), f32),
            pltpu.VMEM((rows, cols, slots), f32),
            pltpu.VMEM((rows, cols + 2, 8, slots), f32),
            pltpu.VMEM((rows, 8, slots), f32),
            pltpu.VMEM((rows, 8, slots), f32),
            pltpu.VMEM((2, padded, slots), f32),
            pltpu.VMEM((2, padded, slots), f32),
            pltpu.SemaphoreType.DMA((7,)),
            pltpu.SemaphoreType.DMA((remote_copies,)),
            pltpu.SemaphoreType.DMA((remote_copies,)),
        ],
        compiler_params=pltpu.CompilerParams(collective_id=0, has_side_effects=True, vmem_limit_bytes=VMEM_GRANT),
    )(
        *(
            pltpu.with_memory_space_constraint(x, pltpu.HBM)
            for x in (
                particles,
                filled,
                contact_pairs,
                contact_count,
                movers_out,
                movers_in,
                jnp.transpose(move_count, (1, 2, 0)),
            )
        )
    )


def solution(mesh):
    sizes = dict(mesh.shape)
    return jax.shard_map(
        functools.partial(body, sizes["blade"], sizes["span"]),
        mesh=mesh,
        in_specs=(
            P(None, "blade", "span", None),
            P("blade", "span"),
            P(None, "blade", "span", None),
            P("blade", "span"),
            P(None, None, "blade", "span"),
            P(None, None, "blade", "span"),
            P(None, "blade", "span"),
        ),
        out_specs=P(None, "blade", "span", None),
        check_vma=False,
    )
```

```python
import functools

import jax
import jax.numpy as jnp
from jax import lax
from jax.experimental import pallas as pl
from jax.experimental.pallas import tpu as pltpu
from jax.sharding import PartitionSpec as P

spring = 4.0
normal_damp = 0.5
tangent_damp = 0.3
conduct = 40.0
timestep_length = 0.05
density = 100.0
gravity = 9.81
soft_len = 0.05
row_steps = (0, 1, 0, 1, 1)
col_steps = (0, 0, 1, 1, -1)
MESH = pl.DeviceIdType.MESH
TILE = 8
VMEM_GRANT = 16 << 20


def cross(a, b):
    return (
        a[1] * b[2] - a[2] * b[1],
        a[2] * b[0] - a[0] * b[2],
        a[0] * b[1] - a[1] * b[0],
    )


def lanes_of(table, index):
    return jnp.take_along_axis(table, index, axis=1, mode="promise_in_bounds")


def pair_terms(first, second, row_shift, col_shift, live):
    gap = (
        second[0] + row_shift - first[0],
        second[1] + col_shift - first[1],
        second[2] - first[2],
    )
    distance = jnp.sqrt(gap[0] * gap[0] + gap[1] * gap[1] + gap[2] * gap[2] + soft_len * soft_len)
    inverse = 1.0 / distance
    normal = tuple(g * inverse for g in gap)
    rad_first, rad_second = first[9], second[9]
    intersection = rad_first + rad_second - distance
    spin = tuple(rad_first * first[6 + c] + rad_second * second[6 + c] for c in range(3))
    turn = cross(spin, normal)
    relative = tuple(second[3 + c] - first[3 + c] - turn[c] for c in range(3))
    speed = relative[0] * normal[0] + relative[1] * normal[1] + relative[2] * normal[2]
    friction = tuple(tangent_damp * (relative[c] - speed * normal[c]) for c in range(3))
    push = normal_damp * speed - spring * intersection
    force = tuple(push * normal[c] + friction[c] for c in range(3))
    torque = cross(normal, friction)
    denom = jnp.where(live, rad_first + rad_second, 1.0)
    heat = 2.0 * conduct * rad_first * rad_second / denom * (second[10] - first[10])
    on_first = force + tuple(rad_first * t for t in torque) + (heat,)
    on_second = tuple(-f for f in force) + tuple(rad_second * t for t in torque) + (-heat,)
    keep = lambda v: jnp.where(live, v, 0.0)
    return [keep(v) for v in on_first], [keep(v) for v in on_second]


def chunks_of(cols):
    ghost_cuts = [0] + [n + 1 for n in range(TILE, cols, TILE)] + [cols]
    owed_cuts = [0] + [n - 1 for n in range(TILE, cols, TILE)] + [cols]
    return list(zip(ghost_cuts, ghost_cuts[1:])), list(zip(owed_cuts, owed_cuts[1:]))


def packing(components, slots, movers):
    live = slots - 2 * movers
    spare = slots - live
    pieces = live // spare
    riders = components // (pieces + 1) if live % spare == 0 else 0
    return live, spare, pieces, riders


def kernel(
    shape,
    blades,
    spans,
    parts_hbm,
    filled_hbm,
    pairs_hbm,
    count_hbm,
    out_movers_hbm,
    in_movers_hbm,
    move_count_hbm,
    out_ref,
    ghost,
    packed,
    pairs_ref,
    count_own,
    filled_ref,
    out_movers,
    in_movers,
    move_count,
    first_terms,
    second_terms,
    count_wide,
    filled_wide,
    totals,
    edge_out,
    owed_low,
    owed_high,
    late_low,
    late_high,
    owed,
    owed_diag,
    msg_out,
    msg_in,
    landed,
    local_sem,
    send_sem,
    recv_sem,
):
    components, rows, cols, slots = shape
    movers = out_movers.shape[3]
    wide = cols + 2
    groups = cols // TILE
    live_slots, spare, pieces, riders = packing(components, slots, movers)
    carried = components - riders
    ghost_chunks, owed_chunks = chunks_of(cols)
    i = lax.axis_index("blade")
    j = lax.axis_index("span")
    has = {}
    for di in (-1, 0, 1):
        for dj in (-1, 0, 1):
            if (di, dj) != (0, 0):
                a, b = i + di, j + dj
                has[di, dj] = (a >= 0) & (a < blades) & (b >= 0) & (b < spans)

    own_cols = slice(TILE, TILE + cols)
    own = [
        pltpu.make_async_copy(source, target, local_sem.at[n])
        for n, (source, target) in enumerate(
            (
                (parts_hbm.at[:, 0], ghost.at[:, 0, own_cols, :]),
                (count_hbm, count_own),
                (filled_hbm, filled_ref),
                (pairs_hbm, pairs_ref),
                (parts_hbm.at[:, 1:rows], ghost.at[:, 1:rows, own_cols, :]),
                (out_movers_hbm, out_movers),
                (in_movers_hbm, in_movers),
                (move_count_hbm, move_count),
            )
        )
    ]
    barrier = pltpu.get_barrier_semaphore()
    expected = jnp.int32(0)
    for (di, dj), there in has.items():
        expected = expected + there.astype(jnp.int32)

        @pl.when(there)
        def _(di=di, dj=dj):
            pl.semaphore_signal(
                barrier, inc=1, device_id=(i + di, j + dj), device_id_type=MESH
            )

    for copy in own:
        copy.start()

    moves = {}

    def move(name, source, target, di, dj):
        n = len(moves)
        copy = pltpu.make_async_remote_copy(
            src_ref=source,
            dst_ref=target,
            send_sem=send_sem.at[n],
            recv_sem=recv_sem.at[n],
            device_id=(i + di, j + dj),
            device_id_type=MESH,
        )
        moves[name] = (copy, di, dj)

    low = slice(0, 1)
    high = slice(cols - 1, cols)
    left = slice(TILE - 1, TILE)
    right = slice(TILE + cols, TILE + cols + 1)
    for n, (a, b) in enumerate(ghost_chunks):
        target = ghost.at[0:carried, rows, TILE + a : TILE + b, :]
        move(("ghost", n), packed.at[:, a:b], target, -1, 0)
    move("corner right", parts_hbm.at[:, 0, low, :], ghost.at[:, rows, right, :], -1, -1)
    move("corner left", parts_hbm.at[:, 0, high, :], ghost.at[:, rows, left, :], -1, 1)
    move("side right", parts_hbm.at[:, :, low, :], ghost.at[:, 0:rows, right, :], 0, -1)
    move("side left", parts_hbm.at[:, :, high, :], ghost.at[:, 0:rows, left, :], 0, 1)
    move("edge low", edge_out.at[1], owed_low, 0, 1)
    move("edge high", edge_out.at[0], owed_high, 0, -1)
    move("late low", totals.at[rows, wide - 1], late_low, 0, 1)
    move("late high", totals.at[rows, 0], late_high, 0, -1)
    for n, (a, b) in enumerate(owed_chunks):
        move(("owed", n), totals.at[rows, 1 + a : 1 + b], owed.at[a:b], 1, 0)
    move("diag low", totals.at[rows, wide - 1], owed_diag.at[0], 1, 1)
    move("diag high", totals.at[rows, 0], owed_diag.at[1], 1, -1)
    move("forward", msg_out.at[0], msg_in.at[0], 1, 0)
    move("backward", msg_out.at[1], msg_in.at[1], -1, 0)

    def start(*which):
        for w in which:
            copy, di, dj = moves[w]

            @pl.when(has[di, dj])
            def _(copy=copy):
                copy.start()

    def arrive(*which):
        for w in which:
            copy, di, dj = moves[w]

            @pl.when(has[-di, -dj])
            def _(copy=copy):
                copy.wait_recv()

    def sent(*which):
        for w in which:
            copy, di, dj = moves[w]

            @pl.when(has[di, dj])
            def _(copy=copy):
                copy.wait_send()

    diagonal = lax.broadcasted_iota(jnp.int32, (cols, cols), 0) == lax.broadcasted_iota(
        jnp.int32, (cols, cols), 1
    )
    lane = lax.broadcasted_iota(jnp.int32, (TILE, slots), 1)
    lane_f = lane.astype(jnp.float32)
    slot_ids = lax.broadcasted_iota(jnp.int32, (slots, slots), 0)
    line_lane = lax.broadcasted_iota(jnp.int32, (1, slots), 1)
    cell_ids = lax.broadcasted_iota(jnp.int32, (cols, slots), 0)
    lane_ids = lax.broadcasted_iota(jnp.int32, (cols, slots), 1)

    def spread(source, r, target, at):
        line = jnp.broadcast_to(source[r : r + 1, :].astype(jnp.float32), (cols, cols))
        column = jnp.sum(jnp.where(diagonal, line, 0.0), axis=1, keepdims=True)
        target[at] = jnp.broadcast_to(column, (cols, slots))

    def clear(n, _):
        for r in range(rows + 1):
            totals[r, n] = jnp.zeros((8, slots), jnp.float32)
        return 0

    def pack():
        for c in range(carried):
            value = ghost[c, 0, own_cols, :]
            if c < riders * pieces:
                rider, piece = carried + c // pieces, c % pieces
                shift = live_slots - piece * spare
                moved = pltpu.roll(ghost[rider, 0, own_cols, :], shift, 1)
                value = jnp.where(lane_ids < live_slots, value, moved)
            packed[c] = value

    def unpack(at):
        for e in range(riders):
            value = None
            for piece in range(pieces):
                shift = (piece * spare - live_slots) % slots
                moved = pltpu.roll(ghost[e * pieces + piece, rows, TILE + at : 2 * TILE + at, :], shift, 1)
                value = moved if piece == 0 else jnp.where(lane >= piece * spare, moved, value)
            ghost[carried + e, rows, TILE + at : 2 * TILE + at, :] = value

    def tiles_of(g):
        return g * TILE if isinstance(g, int) else pl.multiple_of(g * TILE, TILE)

    def contacts_of(r, g):
        at = tiles_of(g)
        ids = pairs_ref[0, r, pl.ds(at, TILE), :]
        code = pairs_ref[1, r, pl.ds(at, TILE), :]
        heading = code // slots
        return ids, heading, code - heading * slots

    def forces(r, g, headings):
        at = tiles_of(g)
        ids, heading, target = contacts_of(r, g)
        live = lane_f < count_wide[r, pl.ds(at, TILE), :]
        first = [
            lanes_of(ghost[c, r, pl.ds(at + TILE, TILE), :], ids) for c in range(components)
        ]
        second = [None] * components
        for n, d in enumerate(headings):
            pick = heading == d
            for c in range(components):
                rows_at = pl.ds(at + TILE + col_steps[d], TILE)
                value = lanes_of(ghost[c, r + row_steps[d], rows_at, :], target)
                second[c] = value if n == 0 else jnp.where(pick, value, second[c])
        row_shift = jnp.where((heading == 0) | (heading == 2), 0.0, 1.0)
        col_shift = jnp.where(
            (heading == 2) | (heading == 3), 1.0, jnp.where(heading == 4, -1.0, 0.0)
        )
        on_first, on_second = pair_terms(first, second, row_shift, col_shift, live)
        zero = jnp.zeros((TILE, slots), jnp.float32)
        base = (r * cols + g * TILE) * 8
        for c, (a, b) in enumerate(zip(on_first + [zero], on_second + [zero])):
            first_terms[pl.ds(base + c, TILE, stride=8), :] = a
            second_terms[pl.ds(base + c, TILE, stride=8), :] = b

    def summed_of(r, g, n, contacts, headings, near_too):
        ids, heading, target = contacts
        base = (r * cols + g * TILE + n) * 8
        if not isinstance(base, int):
            base = pl.multiple_of(base, 8)
        b = second_terms[pl.ds(base, 8), :]
        head = heading[n : n + 1]
        terms = jnp.concatenate([jnp.where(head == d, b, 0.0) for d in headings], axis=0)
        hot = jnp.where(slot_ids == target[n : n + 1], 1.0, 0.0)
        if near_too:
            a = first_terms[pl.ds(base, 8), :]
            zero = jnp.zeros((8, slots), jnp.float32)
            near = jnp.concatenate([a] + [zero] * (len(headings) - 1), axis=0)
            terms = jnp.concatenate([near, terms], axis=1)
            near_hot = jnp.where(slot_ids == ids[n : n + 1], 1.0, 0.0)
            hot = jnp.concatenate([near_hot, hot], axis=1)
        coarse = terms.astype(jnp.bfloat16).astype(jnp.float32)
        split = jnp.concatenate([coarse, terms - coarse], axis=0).astype(jnp.bfloat16)
        summed = lax.dot_general(
            split,
            hot.astype(jnp.bfloat16),
            (((1,), (1,)), ((), ())),
            preferred_element_type=jnp.float32,
        )
        count = len(headings) * 8
        return summed[:count] + summed[count:]

    every = (0, 1, 2, 3, 4)

    def scatter(r, g):
        contacts = contacts_of(r, g)
        for n in range(TILE):
            summed = summed_of(r, g, n, contacts, every, True)
            for m, d in enumerate(every):
                col = g * TILE + n + 1 + col_steps[d]
                totals[r + row_steps[d], col] += summed[m * 8 : m * 8 + 8]

    def group_of(r, g):
        forces(r, g, every)
        scatter(r, g)

    def step(state, sums, live):
        safe = jnp.where(live, state[9], 1.0)
        mass = density * safe * safe * safe
        inverse = 1.0 / mass
        spin_inverse = 1.0 / (0.4 * mass * safe * safe)
        new = [None] * components
        for c in range(3):
            accel = sums[c] * inverse
            if c == 2:
                accel = accel - gravity
            speed = state[3 + c] + timestep_length * accel
            new[c] = state[c] + timestep_length * speed
            new[3 + c] = speed
            new[6 + c] = state[6 + c] + timestep_length * sums[3 + c] * spin_inverse
        new[9] = state[9]
        new[10] = state[10] + timestep_length * sums[6] * inverse
        return [jnp.where(live, v, 0.0) for v in new]

    def step_group(r, g):
        cells = slice(g * TILE, (g + 1) * TILE)
        sums = [totals[r, 1 + g * TILE : 1 + (g + 1) * TILE, c, :] for c in range(7)]
        live = lane_f < filled_wide[r, cells, :]
        state = [ghost[c, r, TILE + g * TILE : 2 * TILE + g * TILE, :] for c in range(components)]
        for c, value in enumerate(step(state, sums, live)):
            out_ref[c, r, cells, :] = value

    def list_of(direction, r):
        cell_line = jnp.full((1, slots), -1, jnp.int32)
        slot_line = jnp.zeros((1, slots), jnp.int32)
        for k in range(movers):
            cell_line = jnp.where(line_lane == k, out_movers[direction, 0, 0, k] - r * cols, cell_line)
            slot_line = jnp.where(line_lane == k, out_movers[direction, 1, 0, k], slot_line)
        cell_line = jnp.where(line_lane < move_count[0, 0, direction], cell_line, -1)
        return cell_line, slot_line

    def chosen_of(cell_line, slot_line):
        chosen = cell_ids == cell_line
        slot_f = jnp.where(chosen, jnp.broadcast_to(slot_line + 1, (cols, slots)).astype(jnp.float32), 0.0)
        slot_of = jnp.sum(slot_f, axis=1, keepdims=True).astype(jnp.int32) - 1
        slot_of = jnp.broadcast_to(slot_of, (cols, slots))
        index = jnp.maximum(slot_of, 0)

        def line_of(value):
            return jnp.sum(jnp.where(chosen, lanes_of(value, index), 0.0), axis=0, keepdims=True)

        return line_of, lane_ids == slot_of

    def put(direction, r, there, message):
        key = jnp.zeros((1, slots), jnp.int32)
        cell_line = jnp.full((1, slots), -1, jnp.int32)
        for k in range(movers):
            hit = line_lane == in_movers[direction, 1, 0, k]
            key = jnp.where(hit, k, key)
            cell_line = jnp.where(hit, in_movers[direction, 0, 0, k] - r * cols, cell_line)
        cell_line = jnp.where(there, cell_line, -1)
        landing = cell_ids == cell_line
        key = jnp.broadcast_to(key, message.shape)
        values = lanes_of(message, key)
        for c in range(components):
            out_ref[c, r] = jnp.where(landing, values[c : c + 1], out_ref[c, r])

    lax.fori_loop(0, wide, clear, 0)
    msg_out[...] = jnp.zeros(msg_out.shape, jnp.float32)
    landed[...] = jnp.zeros(landed.shape, jnp.float32)
    own[0].wait()
    pack()
    pl.semaphore_wait(barrier, expected)
    start("side right", "side left", ("ghost", 0), "corner left", "corner right")
    start(*(("ghost", n) for n in range(1, groups)))
    for copy in own[1:]:
        copy.wait()
    for r in range(rows):
        spread(count_own, r, count_wide, r)
        spread(filled_ref, r, filled_wide, r)

    def inner(n, r):
        group_of(r, n)
        return r

    def outer(n, r):
        group_of(r, (groups - 1) * n)
        return r

    for r in range(rows - 1):
        lax.fori_loop(1, groups - 1, inner, r)
    arrive("side right", "side left")
    for r in range(rows - 1):
        lax.fori_loop(0, 2, outer, r)
    last = rows - 1
    forces(last, groups - 1, (2,))
    ahead = summed_of(last, groups - 1, TILE - 1, contacts_of(last, groups - 1), (2,), False)
    for r in range(rows):
        edge_out[0, r] = totals[r, 0]
        edge_out[1, r] = totals[r, wide - 1] + ahead if r == last else totals[r, wide - 1]
    start("edge low", "edge high")
    cells_back, slots_back = list_of(1, 0)
    lines_back, left_back = chosen_of(cells_back, slots_back)
    arrive("edge low", "edge high")
    for r in range(rows):
        totals[r, 1] += jnp.where(has[0, -1], owed_low[r], 0.0)
        totals[r, cols] += jnp.where(has[0, 1], owed_high[r], 0.0)
    for c in range(7):
        msg_out[1, c : c + 1, :] = lines_back(totals[0, 1 : 1 + cols, c, :])
    msg_out[1, 7:8, :] = cells_back.astype(jnp.float32)
    msg_out[1, 8:9, :] = slots_back.astype(jnp.float32)
    start("backward")
    for r in range(1, last):
        for g in range(groups):
            step_group(r, g)

    for g in range(groups):
        arrive(("ghost", g))
        if g == 0:
            unpack(0)
            unpack(1)
            arrive("corner left")
        elif g < groups - 1:
            unpack(g * TILE + 1)
        else:
            unpack(g * TILE)
            arrive("corner right")
        group_of(last, g)
        start(("owed", g))
        if g == 0:
            start("late high", "diag high")
        if g == groups - 1:
            start("late low", "diag low")
        step_group(last, g)
    cells_on, slots_on = list_of(0, last)
    lines_on, left_on = chosen_of(cells_on, slots_on)
    for c in range(components):
        value = out_ref[c, last]
        line = lines_on(value)
        if c == 0:
            line = line - jnp.where(cells_on >= 0, 1.0, 0.0)
        msg_out[0, c : c + 1, :] = line
        out_ref[c, last] = jnp.where(left_on, 0.0, value)
    start("forward")

    arrive("late low", "late high", "backward")
    message = jnp.where(has[1, 0], msg_in[1], 0.0)
    cells_new = message[7:8].astype(jnp.int32)
    lines_new, _ = chosen_of(cells_new, message[8:9].astype(jnp.int32))
    sums = []
    for c in range(7):
        value = totals[rows, 1 : 1 + cols, c, :]
        value = value + jnp.where((cell_ids == 0) & has[0, -1], late_low[c : c + 1, :], 0.0)
        value = value + jnp.where((cell_ids == cols - 1) & has[0, 1], late_high[c : c + 1, :], 0.0)
        sums.append(lines_new(value) + message[c : c + 1])
    state = [lines_new(ghost[c, rows, own_cols, :]) for c in range(components)]
    moving = cells_new >= 0
    for c, value in enumerate(step(state, sums, moving)):
        if c == 0:
            value = value + jnp.where(moving, 1.0, 0.0)
        landed[c : c + 1, :] = value
    put(1, last, has[1, 0], landed[...])

    arrive(("owed", 0), "diag low")
    totals[0, 1] += jnp.where(has[-1, -1], owed_diag[0], 0.0)
    for g in range(groups):
        if g + 1 < groups:
            arrive(("owed", g + 1))
        if g == groups - 1:
            arrive("diag high")
            totals[0, cols] += jnp.where(has[-1, 1], owed_diag[1], 0.0)
        cells = slice(g * TILE, (g + 1) * TILE)
        for n in range(g * TILE, (g + 1) * TILE):
            totals[0, 1 + n] += jnp.where(has[-1, 0], owed[n], 0.0)
        step_group(0, g)
    for c in range(components):
        out_ref[c, 0] = jnp.where(left_back, 0.0, out_ref[c, 0])
    arrive("forward")
    put(0, 0, has[-1, 0], msg_in[0])
    sent(*moves)


def body(blades, spans, particles, filled, contact_pairs, contact_count, movers_out, movers_in, move_count):
    components, rows, cols, slots = particles.shape
    padded = -(-components // 8) * 8
    f32, i32 = jnp.float32, jnp.int32
    riders = packing(components, slots, movers_out.shape[3])[3]
    remote_copies = 2 * (cols // TILE) + 12
    return pl.pallas_call(
        functools.partial(kernel, particles.shape, blades, spans),
        out_shape=pltpu.VMEM(particles.shape, f32),
        in_specs=[pl.BlockSpec(memory_space=pl.ANY)] * 7,
        out_specs=pl.BlockSpec(memory_space=pltpu.VMEM),
        scratch_shapes=[
            pltpu.VMEM((components, rows + 1, cols + 2 * TILE, slots), f32),
            pltpu.VMEM((components - riders, cols, slots), f32),
            pltpu.VMEM((2, rows, cols, contact_pairs.shape[3]), i32),
            pltpu.VMEM((rows, cols), i32),
            pltpu.VMEM((rows, cols), i32),
            pltpu.SMEM(movers_out.shape, i32),
            pltpu.SMEM(movers_in.shape, i32),
            pltpu.SMEM((1, 1, 2), i32),
            pltpu.VMEM((rows * cols * 8, slots), f32),
            pltpu.VMEM((rows * cols * 8, slots), f32),
            pltpu.VMEM((rows, cols, slots), f32),
            pltpu.VMEM((rows, cols, slots), f32),
            pltpu.VMEM((rows + 1, cols + 2, 8, slots), f32),
            pltpu.VMEM((2, rows, 8, slots), f32),
            pltpu.VMEM((rows, 8, slots), f32),
            pltpu.VMEM((rows, 8, slots), f32),
            pltpu.VMEM((8, slots), f32),
            pltpu.VMEM((8, slots), f32),
            pltpu.VMEM((cols, 8, slots), f32),
            pltpu.VMEM((2, 8, slots), f32),
            pltpu.VMEM((2, padded, slots), f32),
            pltpu.VMEM((2, padded, slots), f32),
            pltpu.VMEM((padded, slots), f32),
            pltpu.SemaphoreType.DMA((8,)),
            pltpu.SemaphoreType.DMA((remote_copies,)),
            pltpu.SemaphoreType.DMA((remote_copies,)),
        ],
        compiler_params=pltpu.CompilerParams(
            collective_id=0, has_side_effects=True, vmem_limit_bytes=VMEM_GRANT
        ),
    )(
        *(
            pltpu.with_memory_space_constraint(x, pltpu.HBM)
            for x in (
                particles,
                filled,
                contact_pairs,
                contact_count,
                movers_out,
                movers_in,
                jnp.transpose(move_count, (1, 2, 0)),
            )
        )
    )


def solution(mesh):
    sizes = dict(mesh.shape)
    return jax.shard_map(
        functools.partial(body, sizes["blade"], sizes["span"]),
        mesh=mesh,
        in_specs=(
            P(None, "blade", "span", None),
            P("blade", "span"),
            P(None, "blade", "span", None),
            P("blade", "span"),
            P(None, None, "blade", "span"),
            P(None, None, "blade", "span"),
            P(None, "blade", "span"),
        ),
        out_specs=P(None, "blade", "span", None),
        check_vma=False,
    )
```

```python
import functools

import jax
import jax.numpy as jnp
from jax import lax
from jax.experimental import pallas as pl
from jax.experimental.pallas import tpu as pltpu
from jax.sharding import PartitionSpec as P

spring = 4.0
normal_damp = 0.5
tangent_damp = 0.3
conduct = 40.0
timestep_length = 0.05
density = 100.0
gravity = 9.81
soft_len = 0.05
row_steps = (0, 1, 0, 1, 1)
col_steps = (0, 0, 1, 1, -1)
MESH = pl.DeviceIdType.MESH
TILE = 8
VMEM_GRANT = 16 << 20


def cross(a, b):
    return (
        a[1] * b[2] - a[2] * b[1],
        a[2] * b[0] - a[0] * b[2],
        a[0] * b[1] - a[1] * b[0],
    )


def lanes_of(table, index):
    return jnp.take_along_axis(table, index, axis=1, mode="promise_in_bounds")


def pair_terms(first, second, row_shift, col_shift, live):
    gap = (
        second[0] + row_shift - first[0],
        second[1] + col_shift - first[1],
        second[2] - first[2],
    )
    distance = jnp.sqrt(gap[0] * gap[0] + gap[1] * gap[1] + gap[2] * gap[2] + soft_len * soft_len)
    inverse = 1.0 / distance
    normal = tuple(g * inverse for g in gap)
    rad_first, rad_second = first[9], second[9]
    intersection = rad_first + rad_second - distance
    spin = tuple(rad_first * first[6 + c] + rad_second * second[6 + c] for c in range(3))
    turn = cross(spin, normal)
    relative = tuple(second[3 + c] - first[3 + c] - turn[c] for c in range(3))
    speed = relative[0] * normal[0] + relative[1] * normal[1] + relative[2] * normal[2]
    friction = tuple(tangent_damp * (relative[c] - speed * normal[c]) for c in range(3))
    push = normal_damp * speed - spring * intersection
    force = tuple(push * normal[c] + friction[c] for c in range(3))
    torque = cross(normal, friction)
    denom = jnp.where(live, rad_first + rad_second, 1.0)
    heat = 2.0 * conduct * rad_first * rad_second / denom * (second[10] - first[10])
    on_first = force + tuple(rad_first * t for t in torque) + (heat,)
    on_second = tuple(-f for f in force) + tuple(rad_second * t for t in torque) + (-heat,)
    keep = lambda v: jnp.where(live, v, 0.0)
    return [keep(v) for v in on_first], [keep(v) for v in on_second]


def order_of(cols):
    groups = cols // TILE
    return [0, groups - 1, *range(1, groups - 1)]


def ghost_chunk(g, cols):
    groups = cols // TILE
    if g == 0:
        return 0, TILE + 1
    if g == groups - 1:
        return cols - TILE - 1, cols
    return g * TILE + 1, min((g + 1) * TILE + 1, cols - TILE - 1)


def owed_chunk(g, cols):
    groups = cols // TILE
    if g == 0:
        return 0, TILE - 1
    if g == groups - 1:
        return cols - TILE + 1, cols
    return g * TILE - 1, ((g + 1) * TILE - 1 if g < groups - 2 else cols - TILE + 1)


def packing(components, slots, movers):
    live = slots - 2 * movers
    spare = slots - live
    pieces = live // spare
    riders = components // (pieces + 1) if live % spare == 0 else 0
    return live, spare, pieces, riders


def far_boundaries(mesh):
    line = mesh.devices.reshape(mesh.devices.shape[0], -1)[:, 0]
    hops = [
        sum(abs(p - q) for p, q in zip(a.coords, b.coords)) for a, b in zip(line, line[1:])
    ]
    most = max(hops, default=0)
    if most == min(hops, default=0):
        return ()
    return tuple(n for n, h in enumerate(hops) if h >= most)


def is_far(boundary, blades, fars):
    for period in range(1, blades):
        if fars == tuple(range(period - 1, blades - 1, period)):
            return lax.rem(boundary + period, period) == period - 1
    far = boundary < -1
    for f in fars:
        far = far | (boundary == f)
    return far


def kernel(
    shape,
    blades,
    spans,
    fars,
    parts_hbm,
    filled_hbm,
    pairs_hbm,
    count_hbm,
    out_movers_hbm,
    in_movers_hbm,
    move_count_hbm,
    out_ref,
    ghost,
    packed,
    packed_last,
    pairs_ref,
    count_own,
    count_prev,
    filled_ref,
    out_movers,
    in_movers,
    move_count,
    first_terms,
    second_terms,
    count_wide,
    filled_wide,
    totals,
    edge_out,
    owed_low,
    owed_high,
    late_low,
    late_high,
    seam_out,
    seam_in,
    owed,
    owed_diag,
    msg_out,
    msg_in,
    landed,
    local_sem,
    send_sem,
    recv_sem,
):
    components, rows, cols, slots = shape
    movers = out_movers.shape[3]
    wide = cols + 2
    groups = cols // TILE
    live_slots, spare, pieces, riders = packing(components, slots, movers)
    carried = components - riders
    order = order_of(cols)
    middle = order[2:]
    seams = (TILE - 1, TILE, cols - TILE - 1, cols - TILE)
    i = lax.axis_index("blade")
    j = lax.axis_index("span")
    has = {}
    for di in (-1, 0, 1):
        for dj in (-1, 0, 1):
            if (di, dj) != (0, 0):
                a, b = i + di, j + dj
                has[di, dj] = (a >= 0) & (a < blades) & (b >= 0) & (b < spans)
    far_up = has[1, 0] & is_far(i, blades, fars)
    far_down = has[-1, 0] & is_far(i - 1, blades, fars)
    before = rows + 1

    own_cols = slice(TILE, TILE + cols)
    own = [
        pltpu.make_async_copy(source, target, local_sem.at[n])
        for n, (source, target) in enumerate(
            (
                (parts_hbm.at[:, 0], ghost.at[:, 0, own_cols, :]),
                (count_hbm, count_own),
                (filled_hbm, filled_ref),
                (pairs_hbm, pairs_ref.at[:, 0:rows]),
                (parts_hbm.at[:, 1:rows], ghost.at[:, 1:rows, own_cols, :]),
                (out_movers_hbm, out_movers),
                (in_movers_hbm, in_movers),
                (move_count_hbm, move_count),
            )
        )
    ]
    barrier = pltpu.get_barrier_semaphore()
    expected = jnp.int32(0)
    for (di, dj), there in has.items():
        expected = expected + there.astype(jnp.int32)

        @pl.when(there)
        def _(di=di, dj=dj):
            pl.semaphore_signal(
                barrier, inc=1, device_id=(i + di, j + dj), device_id_type=MESH
            )

    for copy in own:
        copy.start()

    moves = {}

    def move(name, source, target, di, dj, far=None):
        n = len(moves)
        copy = pltpu.make_async_remote_copy(
            src_ref=source,
            dst_ref=target,
            send_sem=send_sem.at[n],
            recv_sem=recv_sem.at[n],
            device_id=(i + di, j + dj),
            device_id_type=MESH,
        )
        sends, comes = has[di, dj], has[-di, -dj]
        if far is not None:
            sends = sends & (far_up if far else ~far_up)
            comes = comes & (far_down if far else ~far_down)
        moves[name] = (copy, sends, comes)

    low = slice(0, 1)
    high = slice(cols - 1, cols)
    left = slice(TILE - 1, TILE)
    right = slice(TILE + cols, TILE + cols + 1)
    for g in order:
        a, b = ghost_chunk(g, cols)
        target = ghost.at[0:carried, rows, TILE + a : TILE + b, :]
        move(("ghost", g), packed.at[:, a:b], target, -1, 0)
    move("corner right", parts_hbm.at[:, 0, low, :], ghost.at[:, rows, right, :], -1, -1)
    move("corner left", parts_hbm.at[:, 0, high, :], ghost.at[:, rows, left, :], -1, 1)
    move("side right", parts_hbm.at[:, :, low, :], ghost.at[:, 0:rows, right, :], 0, -1)
    move("side left", parts_hbm.at[:, :, high, :], ghost.at[:, 0:rows, left, :], 0, 1)
    move("edge low", edge_out.at[1], owed_low, 0, 1)
    move("edge high", edge_out.at[0], owed_high, 0, -1)
    move("late low", totals.at[rows, wide - 1], late_low, 0, 1)
    move("late high", totals.at[rows, 0], late_high, 0, -1)
    for g in order:
        a, b = owed_chunk(g, cols)
        mode = False if g in middle else None
        move(("owed", g), totals.at[rows, 1 + a : 1 + b], owed.at[a:b], 1, 0, mode)
    move("diag low", totals.at[rows, wide - 1], owed_diag.at[0], 1, 1)
    move("diag high", totals.at[rows, 0], owed_diag.at[1], 1, -1)
    move("seams", seam_out, seam_in, 1, 0, True)
    inner_cols = slice(TILE, cols - TILE)
    target = pairs_ref.at[:, rows, inner_cols]
    move("far pairs", pairs_hbm.at[:, rows - 1, inner_cols], target, 1, 0, True)
    move("far count", count_hbm, count_prev, 1, 0, True)
    for g in middle:
        a, b = g * TILE, (g + 1) * TILE
        target = ghost.at[0:carried, before, TILE + a : TILE + b, :]
        move(("far", g), packed_last.at[:, a:b], target, 1, 0, True)
    move("forward", msg_out.at[0], msg_in.at[0], 1, 0)
    move("backward", msg_out.at[1], msg_in.at[1], -1, 0)

    def start(*which):
        for w in which:
            copy, sends, comes = moves[w]

            @pl.when(sends)
            def _(copy=copy):
                copy.start()

    def arrive(*which):
        for w in which:
            copy, sends, comes = moves[w]

            @pl.when(comes)
            def _(copy=copy):
                copy.wait_recv()

    def sent(*which):
        for w in which:
            copy, sends, comes = moves[w]

            @pl.when(sends)
            def _(copy=copy):
                copy.wait_send()

    diagonal = lax.broadcasted_iota(jnp.int32, (cols, cols), 0) == lax.broadcasted_iota(
        jnp.int32, (cols, cols), 1
    )
    lane = lax.broadcasted_iota(jnp.int32, (TILE, slots), 1)
    lane_f = lane.astype(jnp.float32)
    slot_ids = lax.broadcasted_iota(jnp.int32, (slots, slots), 0)
    line_lane = lax.broadcasted_iota(jnp.int32, (1, slots), 1)
    cell_ids = lax.broadcasted_iota(jnp.int32, (cols, slots), 0)
    lane_ids = lax.broadcasted_iota(jnp.int32, (cols, slots), 1)

    def spread(source, r, target, at):
        line = jnp.broadcast_to(source[r : r + 1, :].astype(jnp.float32), (cols, cols))
        column = jnp.sum(jnp.where(diagonal, line, 0.0), axis=1, keepdims=True)
        target[at] = jnp.broadcast_to(column, (cols, slots))

    def clear(n, _):
        for r in range(rows + 2):
            totals[r, n] = jnp.zeros((8, slots), jnp.float32)
        return 0

    def pack(r, target):
        for c in range(carried):
            value = ghost[c, r, own_cols, :]
            if c < riders * pieces:
                rider, piece = carried + c // pieces, c % pieces
                shift = live_slots - piece * spare
                moved = pltpu.roll(ghost[rider, r, own_cols, :], shift, 1)
                value = jnp.where(lane_ids < live_slots, value, moved)
            target[c] = value

    def unpack(r, at):
        for e in range(riders):
            value = None
            for piece in range(pieces):
                shift = (piece * spare - live_slots) % slots
                tile = ghost[e * pieces + piece, r, TILE + at : 2 * TILE + at, :]
                moved = pltpu.roll(tile, shift, 1)
                value = moved if piece == 0 else jnp.where(lane >= piece * spare, moved, value)
            ghost[carried + e, r, TILE + at : 2 * TILE + at, :] = value

    def tiles_of(g):
        return g * TILE if isinstance(g, int) else pl.multiple_of(g * TILE, TILE)

    def row_of(r):
        if r == before:
            return before, rows, lambda d: 0
        return r, r, lambda d: r + row_steps[d]

    def contacts_of(r, g):
        at = tiles_of(g)
        _, listed, _ = row_of(r)
        ids = pairs_ref[0, listed, pl.ds(at, TILE), :]
        code = pairs_ref[1, listed, pl.ds(at, TILE), :]
        heading = code // slots
        return ids, heading, code - heading * slots

    def forces(r, g, headings):
        at = tiles_of(g)
        near, listed, far_row = row_of(r)
        ids, heading, target = contacts_of(r, g)
        live = lane_f < count_wide[listed, pl.ds(at, TILE), :]
        if len(headings) < len(row_steps):
            among = heading == headings[0]
            for d in headings[1:]:
                among = among | (heading == d)
            live = live & among
        first = [
            lanes_of(ghost[c, near, pl.ds(at + TILE, TILE), :], ids) for c in range(components)
        ]
        second = [None] * components
        for n, d in enumerate(headings):
            pick = heading == d
            for c in range(components):
                rows_at = pl.ds(at + TILE + col_steps[d], TILE)
                value = lanes_of(ghost[c, far_row(d), rows_at, :], target)
                second[c] = value if n == 0 else jnp.where(pick, value, second[c])
        row_shift = jnp.where((heading == 0) | (heading == 2), 0.0, 1.0)
        col_shift = jnp.where(
            (heading == 2) | (heading == 3), 1.0, jnp.where(heading == 4, -1.0, 0.0)
        )
        on_first, on_second = pair_terms(first, second, row_shift, col_shift, live)
        zero = jnp.zeros((TILE, slots), jnp.float32)
        base = (listed * cols + g * TILE) * 8
        for c, (a, b) in enumerate(zip(on_first + [zero], on_second + [zero])):
            first_terms[pl.ds(base + c, TILE, stride=8), :] = a
            second_terms[pl.ds(base + c, TILE, stride=8), :] = b

    def scatter(r, g, headings):
        near, listed, far_row = row_of(r)
        ids, heading, target = contacts_of(r, g)
        shared = 0 in headings
        zero = jnp.zeros((8, slots), jnp.float32)
        for n in range(TILE):
            base = (listed * cols + g * TILE + n) * 8
            if not isinstance(base, int):
                base = pl.multiple_of(base, 8)
            a = first_terms[pl.ds(base, 8), :]
            b = second_terms[pl.ds(base, 8), :]
            head = heading[n : n + 1]
            blocks = [jnp.where(head == d, b, 0.0) for d in headings]
            if not shared:
                blocks = [zero] + blocks
            near_blocks = [a] + [zero] * (len(blocks) - 1)
            terms = jnp.concatenate(
                [jnp.concatenate(near_blocks, axis=0), jnp.concatenate(blocks, axis=0)], axis=1
            )
            near_hot = jnp.where(slot_ids == ids[n : n + 1], 1.0, 0.0)
            hot = jnp.where(slot_ids == target[n : n + 1], 1.0, 0.0)
            hot = jnp.concatenate([near_hot, hot], axis=1)
            coarse = terms.astype(jnp.bfloat16).astype(jnp.float32)
            split = jnp.concatenate([coarse, terms - coarse], axis=0).astype(jnp.bfloat16)
            summed = lax.dot_general(
                split,
                hot.astype(jnp.bfloat16),
                (((1,), (1,)), ((), ())),
                preferred_element_type=jnp.float32,
            )
            count = len(blocks) * 8
            summed = summed[:count] + summed[count:]
            places = [(far_row(d), col_steps[d]) for d in headings]
            if not shared:
                places = [(near, 0)] + places
            for m, (row, shift) in enumerate(places):
                totals[row, g * TILE + n + 1 + shift] += summed[m * 8 : m * 8 + 8]

    every, inside, across = (0, 1, 2, 3, 4), (0, 2), (1, 3, 4)

    def group_of(r, g, headings):
        forces(r, g, headings)
        scatter(r, g, headings)

    def step(state, sums, live):
        safe = jnp.where(live, state[9], 1.0)
        mass = density * safe * safe * safe
        inverse = 1.0 / mass
        spin_inverse = 1.0 / (0.4 * mass * safe * safe)
        new = [None] * components
        for c in range(3):
            accel = sums[c] * inverse
            if c == 2:
                accel = accel - gravity
            speed = state[3 + c] + timestep_length * accel
            new[c] = state[c] + timestep_length * speed
            new[3 + c] = speed
            new[6 + c] = state[6 + c] + timestep_length * sums[3 + c] * spin_inverse
        new[9] = state[9]
        new[10] = state[10] + timestep_length * sums[6] * inverse
        return [jnp.where(live, v, 0.0) for v in new]

    def step_group(r, g, left=None):
        cells = slice(g * TILE, (g + 1) * TILE)
        sums = [totals[r, 1 + g * TILE : 1 + (g + 1) * TILE, c, :] for c in range(7)]
        live = lane_f < filled_wide[r, cells, :]
        state = [ghost[c, r, TILE + g * TILE : 2 * TILE + g * TILE, :] for c in range(components)]
        if left is not None:
            live = live & ~left[cells]
        for c, value in enumerate(step(state, sums, live)):
            out_ref[c, r, cells, :] = value

    def list_of(direction, r):
        cell_line = jnp.full((1, slots), -1, jnp.int32)
        slot_line = jnp.zeros((1, slots), jnp.int32)
        for k in range(movers):
            cell_line = jnp.where(line_lane == k, out_movers[direction, 0, 0, k] - r * cols, cell_line)
            slot_line = jnp.where(line_lane == k, out_movers[direction, 1, 0, k], slot_line)
        cell_line = jnp.where(line_lane < move_count[0, 0, direction], cell_line, -1)
        return cell_line, slot_line

    def chosen_of(cell_line, slot_line):
        chosen = cell_ids == cell_line
        slot_f = jnp.where(chosen, jnp.broadcast_to(slot_line + 1, (cols, slots)).astype(jnp.float32), 0.0)
        slot_of = jnp.sum(slot_f, axis=1, keepdims=True).astype(jnp.int32) - 1
        slot_of = jnp.broadcast_to(slot_of, (cols, slots))
        index = jnp.maximum(slot_of, 0)

        def line_of(value):
            return jnp.sum(jnp.where(chosen, lanes_of(value, index), 0.0), axis=0, keepdims=True)

        return line_of, lane_ids == slot_of

    def put(direction, r, there, message):
        key = jnp.zeros((1, slots), jnp.int32)
        cell_line = jnp.full((1, slots), -1, jnp.int32)
        for k in range(movers):
            hit = line_lane == in_movers[direction, 1, 0, k]
            key = jnp.where(hit, k, key)
            cell_line = jnp.where(hit, in_movers[direction, 0, 0, k] - r * cols, cell_line)
        cell_line = jnp.where(there, cell_line, -1)
        landing = cell_ids == cell_line
        key = jnp.broadcast_to(key, message.shape)
        values = lanes_of(message, key)
        for c in range(components):
            out_ref[c, r] = jnp.where(landing, values[c : c + 1], out_ref[c, r])

    def finish(direction, message, row, extra, state_of):
        cells_new = message[7:8].astype(jnp.int32)
        lines_new, _ = chosen_of(cells_new, message[8:9].astype(jnp.int32))
        sums = [
            lines_new(extra(c, totals[row, 1 : 1 + cols, c, :])) + message[c : c + 1]
            for c in range(7)
        ]
        state = [state_of(c, lines_new) for c in range(components)]
        moving = cells_new >= 0
        for c, value in enumerate(step(state, sums, moving)):
            if c == 0:
                value = value + jnp.where(moving, -1.0 if direction == 0 else 1.0, 0.0)
            landed[direction, c : c + 1, :] = value

    def share_of(direction, r, lines, cells_line, slots_line):
        for c in range(7):
            msg_out[direction, c : c + 1, :] = lines(totals[r, 1 : 1 + cols, c, :])
        msg_out[direction, 7:8, :] = cells_line.astype(jnp.float32)
        msg_out[direction, 8:9, :] = slots_line.astype(jnp.float32)

    last = rows - 1
    lax.fori_loop(0, wide, clear, 0)
    msg_out[...] = jnp.zeros(msg_out.shape, jnp.float32)
    landed[...] = jnp.zeros(landed.shape, jnp.float32)
    own[0].wait()
    pack(0, packed)
    own[4].wait()

    @pl.when(far_up)
    def _():
        pack(last, packed_last)

    pl.semaphore_wait(barrier, expected)
    start("side right", "side left", ("ghost", 0), "corner left", "corner right")
    start(*(("ghost", g) for g in order[1:]))
    for n, copy in enumerate(own):
        if n not in (0, 4):
            copy.wait()
    for r in range(rows):
        spread(count_own, r, count_wide, r)
        spread(filled_ref, r, filled_wide, r)

    def early(g):
        for r in range(last):
            group_of(r, g, every)
        group_of(last, g, inside)

    def inner(n, _):
        early(n)
        return 0

    def outer(n, _):
        early((groups - 1) * n)
        return 0

    lax.fori_loop(1, groups - 1, inner, 0)
    arrive("side right", "side left")
    lax.fori_loop(0, 2, outer, 0)
    for r in range(rows):
        edge_out[0, r] = totals[r, 0]
        edge_out[1, r] = totals[r, wide - 1]
    start("edge low", "edge high")
    cells_back, slots_back = list_of(1, 0)
    lines_back, left_back = chosen_of(cells_back, slots_back)
    cells_on, slots_on = list_of(0, last)
    lines_on, left_on = chosen_of(cells_on, slots_on)
    arrive("edge low", "edge high")
    for r in range(rows):
        totals[r, 1] += jnp.where(has[0, -1], owed_low[r], 0.0)
        totals[r, cols] += jnp.where(has[0, 1], owed_high[r], 0.0)
    share_of(1, 0, lines_back, cells_back, slots_back)
    start("backward")
    start("far pairs", "far count", *(("far", g) for g in middle))

    for r in range(1, last):
        for g in range(groups):
            step_group(r, g)

    def last_group(g):
        arrive(("ghost", g))
        if g == 0:
            unpack(rows, 0)
            unpack(rows, 1)
            arrive("corner left")
        elif g == groups - 1:
            unpack(rows, cols - TILE - 1)
            unpack(rows, cols - TILE)
            arrive("corner right")
        else:
            unpack(rows, g * TILE + 1)
        group_of(last, g, across)
        start(("owed", g))

    last_group(0)
    start("late high", "diag high")
    last_group(groups - 1)
    start("late low", "diag low")

    @pl.when(far_up)
    def _():
        for n, col in enumerate(seams):
            seam_out[n] = totals[rows, 1 + col]
        start("seams")
        share_of(0, last, lines_on, cells_on, slots_on)
        for c in range(components):
            msg_out[0, 9 + c : 10 + c, :] = lines_on(ghost[c, last, own_cols, :])
        start("forward")

    for g in middle:
        last_group(g)
    for g in range(groups):
        step_group(last, g)

    @pl.when(has[1, 0] & ~far_up)
    def _():
        for c in range(components):
            line = lines_on(out_ref[c, last])
            if c == 0:
                line = line - jnp.where(cells_on >= 0, 1.0, 0.0)
            msg_out[0, c : c + 1, :] = line
        start("forward")

    for c in range(components):
        out_ref[c, last] = jnp.where(left_on, 0.0, out_ref[c, last])

    def late_edges(c, value):
        value = value + jnp.where((cell_ids == 0) & has[0, -1], late_low[c : c + 1, :], 0.0)
        return value + jnp.where((cell_ids == cols - 1) & has[0, 1], late_high[c : c + 1, :], 0.0)

    arrive("late low", "late high", "backward")

    @pl.when(has[1, 0])
    def _():
        finish(1, msg_in[1], rows, late_edges, lambda c, lines: lines(ghost[c, rows, own_cols, :]))
        put(1, last, True, landed[1])

    def add_diagonals():
        totals[0, 1] += jnp.where(has[-1, -1], owed_diag[0], 0.0)
        totals[0, cols] += jnp.where(has[-1, 1], owed_diag[1], 0.0)

    @pl.when(far_down)
    def _():
        arrive("far count", "far pairs")
        spread(count_prev, last, count_wide, rows)
        for g in middle:
            arrive(("far", g))
            unpack(before, g * TILE)
            group_of(before, g, across)
        arrive(("owed", 0), ("owed", groups - 1), "seams", "diag low", "diag high")
        add_diagonals()
        for g in (0, groups - 1):
            for n in range(*owed_chunk(g, cols)):
                totals[0, 1 + n] += owed[n]
        for n, col in enumerate(seams):
            totals[0, 1 + col] += seam_in[n]
        for g in range(groups):
            step_group(0, g, left_back)
        arrive("forward")
        message = msg_in[0]
        finish(0, message, before, lambda c, value: value, lambda c, _: message[9 + c : 10 + c])

    @pl.when(~far_down)
    def _():
        arrive(("owed", 0), ("owed", groups - 1), "diag low", "diag high")
        add_diagonals()
        for k, g in enumerate(order):
            if k > 1:
                arrive(("owed", g))
            for n in range(*owed_chunk(g, cols)):
                totals[0, 1 + n] += jnp.where(has[-1, 0], owed[n], 0.0)
            if k > 1:
                step_group(0, g - 1, left_back)
        step_group(0, groups - 2, left_back)
        step_group(0, groups - 1, left_back)
        arrive("forward")
        landed[0, 0:components, :] = msg_in[0, 0:components, :]

    put(0, 0, has[-1, 0], landed[0])
    sent(*moves)


def body(blades, spans, fars, particles, filled, contact_pairs, contact_count, movers_out, movers_in, move_count):
    components, rows, cols, slots = particles.shape
    padded = -(-components // 8) * 8
    message = -(-(components + 9) // 8) * 8
    f32, i32 = jnp.float32, jnp.int32
    riders = packing(components, slots, movers_out.shape[3])[3]
    remote_copies = 3 * (cols // TILE) + 13
    return pl.pallas_call(
        functools.partial(kernel, particles.shape, blades, spans, fars),
        out_shape=pltpu.VMEM(particles.shape, f32),
        in_specs=[pl.BlockSpec(memory_space=pl.ANY)] * 7,
        out_specs=pl.BlockSpec(memory_space=pltpu.VMEM),
        scratch_shapes=[
            pltpu.VMEM((components, rows + 2, cols + 2 * TILE, slots), f32),
            pltpu.VMEM((components - riders, cols, slots), f32),
            pltpu.VMEM((components - riders, cols, slots), f32),
            pltpu.VMEM((2, rows + 1, cols, contact_pairs.shape[3]), i32),
            pltpu.VMEM((rows, cols), i32),
            pltpu.VMEM((rows, cols), i32),
            pltpu.VMEM((rows, cols), i32),
            pltpu.SMEM(movers_out.shape, i32),
            pltpu.SMEM(movers_in.shape, i32),
            pltpu.SMEM((1, 1, 2), i32),
            pltpu.VMEM(((rows + 1) * cols * 8, slots), f32),
            pltpu.VMEM(((rows + 1) * cols * 8, slots), f32),
            pltpu.VMEM((rows + 1, cols, slots), f32),
            pltpu.VMEM((rows, cols, slots), f32),
            pltpu.VMEM((rows + 2, cols + 2, 8, slots), f32),
            pltpu.VMEM((2, rows, 8, slots), f32),
            pltpu.VMEM((rows, 8, slots), f32),
            pltpu.VMEM((rows, 8, slots), f32),
            pltpu.VMEM((8, slots), f32),
            pltpu.VMEM((8, slots), f32),
            pltpu.VMEM((4, 8, slots), f32),
            pltpu.VMEM((4, 8, slots), f32),
            pltpu.VMEM((cols, 8, slots), f32),
            pltpu.VMEM((2, 8, slots), f32),
            pltpu.VMEM((2, message, slots), f32),
            pltpu.VMEM((2, message, slots), f32),
            pltpu.VMEM((2, padded, slots), f32),
            pltpu.SemaphoreType.DMA((8,)),
            pltpu.SemaphoreType.DMA((remote_copies,)),
            pltpu.SemaphoreType.DMA((remote_copies,)),
        ],
        compiler_params=pltpu.CompilerParams(
            collective_id=0, has_side_effects=True, vmem_limit_bytes=VMEM_GRANT
        ),
    )(
        *(
            pltpu.with_memory_space_constraint(x, pltpu.HBM)
            for x in (
                particles,
                filled,
                contact_pairs,
                contact_count,
                movers_out,
                movers_in,
                jnp.transpose(move_count, (1, 2, 0)),
            )
        )
    )


def solution(mesh):
    sizes = dict(mesh.shape)
    return jax.shard_map(
        functools.partial(body, sizes["blade"], sizes["span"], far_boundaries(mesh)),
        mesh=mesh,
        in_specs=(
            P(None, "blade", "span", None),
            P("blade", "span"),
            P(None, "blade", "span", None),
            P("blade", "span"),
            P(None, None, "blade", "span"),
            P(None, None, "blade", "span"),
            P(None, "blade", "span"),
        ),
        out_specs=P(None, "blade", "span", None),
        check_vma=False,
    )
```

```python
import functools

import jax
import jax.numpy as jnp
from jax import lax
from jax.experimental import pallas as pl
from jax.experimental.pallas import tpu as pltpu
from jax.sharding import PartitionSpec as P

spring = 4.0
normal_damp = 0.5
tangent_damp = 0.3
conduct = 40.0
timestep_length = 0.05
density = 100.0
gravity = 9.81
soft_len = 0.05
row_steps = (0, 1, 0, 1, 1)
col_steps = (0, 0, 1, 1, -1)
MESH = pl.DeviceIdType.MESH
TILE = 8
VMEM_GRANT = 16 << 20


def cross(a, b):
    return (
        a[1] * b[2] - a[2] * b[1],
        a[2] * b[0] - a[0] * b[2],
        a[0] * b[1] - a[1] * b[0],
    )


def lanes_of(table, index):
    return jnp.take_along_axis(table, index, axis=1, mode="promise_in_bounds")


def pair_terms(first, second, row_shift, col_shift, live):
    gap = (
        second[0] + row_shift - first[0],
        second[1] + col_shift - first[1],
        second[2] - first[2],
    )
    distance = jnp.sqrt(gap[0] * gap[0] + gap[1] * gap[1] + gap[2] * gap[2] + soft_len * soft_len)
    inverse = 1.0 / distance
    normal = tuple(g * inverse for g in gap)
    rad_first, rad_second = first[9], second[9]
    intersection = rad_first + rad_second - distance
    spin = tuple(rad_first * first[6 + c] + rad_second * second[6 + c] for c in range(3))
    turn = cross(spin, normal)
    relative = tuple(second[3 + c] - first[3 + c] - turn[c] for c in range(3))
    speed = relative[0] * normal[0] + relative[1] * normal[1] + relative[2] * normal[2]
    friction = tuple(tangent_damp * (relative[c] - speed * normal[c]) for c in range(3))
    push = normal_damp * speed - spring * intersection
    force = tuple(push * normal[c] + friction[c] for c in range(3))
    torque = cross(normal, friction)
    denom = jnp.where(live, rad_first + rad_second, 1.0)
    heat = 2.0 * conduct * rad_first * rad_second / denom * (second[10] - first[10])
    on_first = force + tuple(rad_first * t for t in torque) + (heat,)
    on_second = tuple(-f for f in force) + tuple(rad_second * t for t in torque) + (-heat,)
    keep = lambda v: jnp.where(live, v, 0.0)
    return [keep(v) for v in on_first], [keep(v) for v in on_second]


def order_of(cols):
    groups = cols // TILE
    return [0, groups - 1, *range(1, groups - 1)]


def ghost_chunk(g, cols):
    groups = cols // TILE
    if g == 0:
        return 0, TILE + 1
    if g == groups - 1:
        return cols - TILE - 1, cols
    return g * TILE + 1, min((g + 1) * TILE + 1, cols - TILE - 1)


def owed_chunk(g, cols):
    groups = cols // TILE
    if g == 0:
        return 0, TILE - 1
    if g == groups - 1:
        return cols - TILE + 1, cols
    return g * TILE - 1, ((g + 1) * TILE - 1 if g < groups - 2 else cols - TILE + 1)


def packing(components, slots, movers):
    live = slots - 2 * movers
    spare = slots - live
    pieces = live // spare
    riders = components // (pieces + 1) if live % spare == 0 else 0
    sent_rows = 6 if live % spare == 0 and pieces <= 6 else 8
    return live, spare, pieces, riders, sent_rows


def far_boundaries(mesh):
    line = mesh.devices.reshape(mesh.devices.shape[0], -1)[:, 0]
    hops = [
        sum(abs(p - q) for p, q in zip(a.coords, b.coords)) for a, b in zip(line, line[1:])
    ]
    most = max(hops, default=0)
    if most == min(hops, default=0):
        return ()
    return tuple(n for n, h in enumerate(hops) if h >= most)


def is_far(boundary, blades, fars):
    for period in range(1, blades):
        if fars == tuple(range(period - 1, blades - 1, period)):
            return lax.rem(boundary + period, period) == period - 1
    far = boundary < -1
    for f in fars:
        far = far | (boundary == f)
    return far


def kernel(
    shape,
    blades,
    spans,
    fars,
    parts_hbm,
    filled_hbm,
    pairs_hbm,
    count_hbm,
    out_movers_hbm,
    in_movers_hbm,
    move_count_hbm,
    out_ref,
    ghost,
    packed,
    packed_last,
    pairs_ref,
    count_own,
    count_prev,
    filled_ref,
    out_movers,
    in_movers,
    move_count,
    first_terms,
    second_terms,
    count_wide,
    filled_wide,
    totals,
    edge_out,
    owed_low,
    owed_high,
    late_low,
    late_high,
    seam_out,
    seam_in,
    owed,
    owed_diag,
    msg_out,
    msg_in,
    landed,
    local_sem,
    send_sem,
    recv_sem,
):
    components, rows, cols, slots = shape
    movers = out_movers.shape[3]
    wide = cols + 2
    groups = cols // TILE
    live_slots, spare, pieces, riders, sent_rows = packing(components, slots, movers)
    carried = components - riders
    order = order_of(cols)
    middle = order[2:]
    seams = (TILE - 1, TILE, cols - TILE - 1, cols - TILE)
    i = lax.axis_index("blade")
    j = lax.axis_index("span")
    has = {}
    for di in (-1, 0, 1):
        for dj in (-1, 0, 1):
            if (di, dj) != (0, 0):
                a, b = i + di, j + dj
                has[di, dj] = (a >= 0) & (a < blades) & (b >= 0) & (b < spans)
    far_up = has[1, 0] & is_far(i, blades, fars)
    far_down = has[-1, 0] & is_far(i - 1, blades, fars)
    before = rows + 1

    own_cols = slice(TILE, TILE + cols)
    own = [
        pltpu.make_async_copy(source, target, local_sem.at[n])
        for n, (source, target) in enumerate(
            (
                (parts_hbm.at[:, 0], ghost.at[:, 0, own_cols, :]),
                (count_hbm, count_own),
                (filled_hbm, filled_ref),
                (pairs_hbm, pairs_ref.at[:, 0:rows]),
                (parts_hbm.at[:, 1:rows], ghost.at[:, 1:rows, own_cols, :]),
                (out_movers_hbm, out_movers),
                (in_movers_hbm, in_movers),
                (move_count_hbm, move_count),
            )
        )
    ]
    barrier = pltpu.get_barrier_semaphore()
    expected = jnp.int32(0)
    for (di, dj), there in has.items():
        expected = expected + there.astype(jnp.int32)

        @pl.when(there)
        def _(di=di, dj=dj):
            pl.semaphore_signal(
                barrier, inc=1, device_id=(i + di, j + dj), device_id_type=MESH
            )

    for copy in own:
        copy.start()

    moves = {}

    def move(name, source, target, di, dj, far=None):
        n = len(moves)
        copy = pltpu.make_async_remote_copy(
            src_ref=source,
            dst_ref=target,
            send_sem=send_sem.at[n],
            recv_sem=recv_sem.at[n],
            device_id=(i + di, j + dj),
            device_id_type=MESH,
        )
        sends, comes = has[di, dj], has[-di, -dj]
        if far is not None:
            sends = sends & (far_up if far else ~far_up)
            comes = comes & (far_down if far else ~far_down)
        moves[name] = (copy, sends, comes)

    low = slice(0, 1)
    high = slice(cols - 1, cols)
    left = slice(TILE - 1, TILE)
    right = slice(TILE + cols, TILE + cols + 1)
    for g in order:
        a, b = ghost_chunk(g, cols)
        target = ghost.at[0:carried, rows, TILE + a : TILE + b, :]
        move(("ghost", g), packed.at[:, a:b], target, -1, 0)
    move("corner right", parts_hbm.at[:, 0, low, :], ghost.at[:, rows, right, :], -1, -1)
    move("corner left", parts_hbm.at[:, 0, high, :], ghost.at[:, rows, left, :], -1, 1)
    move("side right", parts_hbm.at[:, :, low, :], ghost.at[:, 0:rows, right, :], 0, -1)
    move("side left", parts_hbm.at[:, :, high, :], ghost.at[:, 0:rows, left, :], 0, 1)
    move("edge low", edge_out.at[1], owed_low, 0, 1)
    move("edge high", edge_out.at[0], owed_high, 0, -1)
    move("late low", totals.at[rows, wide - 1], late_low, 0, 1)
    move("late high", totals.at[rows, 0], late_high, 0, -1)
    for g in order:
        a, b = owed_chunk(g, cols)
        mode = False if g in middle else None
        source, target = totals.at[rows, 1 + a : 1 + b, 0:sent_rows], owed.at[a:b, 0:sent_rows]
        move(("owed", g), source, target, 1, 0, mode)
    move("diag low", totals.at[rows, wide - 1], owed_diag.at[0], 1, 1)
    move("diag high", totals.at[rows, 0], owed_diag.at[1], 1, -1)
    move("seams", seam_out, seam_in, 1, 0, True)
    inner_cols = slice(TILE, cols - TILE)
    target = pairs_ref.at[:, rows, inner_cols]
    move("far pairs", pairs_hbm.at[:, rows - 1, inner_cols], target, 1, 0, True)
    move("far count", count_hbm, count_prev, 1, 0, True)
    for g in middle:
        a, b = g * TILE, (g + 1) * TILE
        target = ghost.at[0:carried, before, TILE + a : TILE + b, :]
        move(("far", g), packed_last.at[:, a:b], target, 1, 0, True)
    move("forward", msg_out.at[0], msg_in.at[0], 1, 0)
    move("backward", msg_out.at[1], msg_in.at[1], -1, 0)

    def start(*which):
        for w in which:
            copy, sends, comes = moves[w]

            @pl.when(sends)
            def _(copy=copy):
                copy.start()

    def arrive(*which):
        for w in which:
            copy, sends, comes = moves[w]

            @pl.when(comes)
            def _(copy=copy):
                copy.wait_recv()

    def sent(*which):
        for w in which:
            copy, sends, comes = moves[w]

            @pl.when(sends)
            def _(copy=copy):
                copy.wait_send()

    diagonal = lax.broadcasted_iota(jnp.int32, (cols, cols), 0) == lax.broadcasted_iota(
        jnp.int32, (cols, cols), 1
    )
    lane = lax.broadcasted_iota(jnp.int32, (TILE, slots), 1)
    lane_f = lane.astype(jnp.float32)
    slot_ids = lax.broadcasted_iota(jnp.int32, (slots, slots), 0)
    line_lane = lax.broadcasted_iota(jnp.int32, (1, slots), 1)
    cell_ids = lax.broadcasted_iota(jnp.int32, (cols, slots), 0)
    lane_ids = lax.broadcasted_iota(jnp.int32, (cols, slots), 1)

    def spread(source, r, target, at):
        line = jnp.broadcast_to(source[r : r + 1, :].astype(jnp.float32), (cols, cols))
        column = jnp.sum(jnp.where(diagonal, line, 0.0), axis=1, keepdims=True)
        target[at] = jnp.broadcast_to(column, (cols, slots))

    def clear(n, _):
        for r in range(rows + 2):
            totals[r, n] = jnp.zeros((8, slots), jnp.float32)
        return 0

    def pack(r, target):
        for c in range(carried):
            value = ghost[c, r, own_cols, :]
            if c < riders * pieces:
                rider, piece = carried + c // pieces, c % pieces
                shift = live_slots - piece * spare
                moved = pltpu.roll(ghost[rider, r, own_cols, :], shift, 1)
                value = jnp.where(lane_ids < live_slots, value, moved)
            target[c] = value

    def unpack(r, at):
        for e in range(riders):
            value = None
            for piece in range(pieces):
                shift = (piece * spare - live_slots) % slots
                tile = ghost[e * pieces + piece, r, TILE + at : 2 * TILE + at, :]
                moved = pltpu.roll(tile, shift, 1)
                value = moved if piece == 0 else jnp.where(lane >= piece * spare, moved, value)
            ghost[carried + e, r, TILE + at : 2 * TILE + at, :] = value

    def load_heat(g):
        if sent_rows == 8:
            return
        a, b = owed_chunk(g, cols)
        for first in {a, b - TILE} if b - a >= TILE else {a}:
            n = min(TILE, b - a)
            cells = slice(1 + first, 1 + first + n)
            heat = totals[rows, cells, 6, :]
            spot = lax.broadcasted_iota(jnp.int32, (n, slots), 1) < live_slots
            for piece in range(pieces):
                moved = pltpu.roll(heat, live_slots - piece * spare, 1)
                totals[rows, cells, piece, :] = jnp.where(spot, totals[rows, cells, piece, :], moved)

    def owed_sum(c, cells):
        if c < 6 or sent_rows == 8:
            return owed[cells, c, :]
        value = None
        for piece in range(pieces):
            moved = pltpu.roll(owed[cells, piece, :], (piece * spare - live_slots) % slots, 1)
            value = moved if piece == 0 else jnp.where(lane >= piece * spare, moved, value)
        return value

    def tiles_of(g):
        return g * TILE if isinstance(g, int) else pl.multiple_of(g * TILE, TILE)

    def row_of(r):
        if r == before:
            return before, rows, lambda d: 0
        return r, r, lambda d: r + row_steps[d]

    def contacts_of(r, g):
        at = tiles_of(g)
        _, listed, _ = row_of(r)
        ids = pairs_ref[0, listed, pl.ds(at, TILE), :]
        code = pairs_ref[1, listed, pl.ds(at, TILE), :]
        heading = code // slots
        return ids, heading, code - heading * slots

    def forces(r, g, headings):
        at = tiles_of(g)
        near, listed, far_row = row_of(r)
        ids, heading, target = contacts_of(r, g)
        live = lane_f < count_wide[listed, pl.ds(at, TILE), :]
        if len(headings) < len(row_steps):
            among = heading == headings[0]
            for d in headings[1:]:
                among = among | (heading == d)
            live = live & among
        first = [
            lanes_of(ghost[c, near, pl.ds(at + TILE, TILE), :], ids) for c in range(components)
        ]
        second = [None] * components
        for n, d in enumerate(headings):
            pick = heading == d
            for c in range(components):
                rows_at = pl.ds(at + TILE + col_steps[d], TILE)
                value = lanes_of(ghost[c, far_row(d), rows_at, :], target)
                second[c] = value if n == 0 else jnp.where(pick, value, second[c])
        row_shift = jnp.where((heading == 0) | (heading == 2), 0.0, 1.0)
        col_shift = jnp.where(
            (heading == 2) | (heading == 3), 1.0, jnp.where(heading == 4, -1.0, 0.0)
        )
        on_first, on_second = pair_terms(first, second, row_shift, col_shift, live)
        zero = jnp.zeros((TILE, slots), jnp.float32)
        base = (listed * cols + g * TILE) * 8
        for c, (a, b) in enumerate(zip(on_first + [zero], on_second + [zero])):
            first_terms[pl.ds(base + c, TILE, stride=8), :] = a
            second_terms[pl.ds(base + c, TILE, stride=8), :] = b

    def scatter(r, g, headings):
        near, listed, far_row = row_of(r)
        ids, heading, target = contacts_of(r, g)
        shared = 0 in headings
        zero = jnp.zeros((8, slots), jnp.float32)
        for n in range(TILE):
            base = (listed * cols + g * TILE + n) * 8
            if not isinstance(base, int):
                base = pl.multiple_of(base, 8)
            a = first_terms[pl.ds(base, 8), :]
            b = second_terms[pl.ds(base, 8), :]
            head = heading[n : n + 1]
            blocks = [jnp.where(head == d, b, 0.0) for d in headings]
            if not shared:
                blocks = [zero] + blocks
            near_blocks = [a] + [zero] * (len(blocks) - 1)
            terms = jnp.concatenate(
                [jnp.concatenate(near_blocks, axis=0), jnp.concatenate(blocks, axis=0)], axis=1
            )
            near_hot = jnp.where(slot_ids == ids[n : n + 1], 1.0, 0.0)
            hot = jnp.where(slot_ids == target[n : n + 1], 1.0, 0.0)
            hot = jnp.concatenate([near_hot, hot], axis=1)
            coarse = terms.astype(jnp.bfloat16).astype(jnp.float32)
            split = jnp.concatenate([coarse, terms - coarse], axis=0).astype(jnp.bfloat16)
            summed = lax.dot_general(
                split,
                hot.astype(jnp.bfloat16),
                (((1,), (1,)), ((), ())),
                preferred_element_type=jnp.float32,
            )
            count = len(blocks) * 8
            summed = summed[:count] + summed[count:]
            places = [(far_row(d), col_steps[d]) for d in headings]
            if not shared:
                places = [(near, 0)] + places
            for m, (row, shift) in enumerate(places):
                totals[row, g * TILE + n + 1 + shift] += summed[m * 8 : m * 8 + 8]

    every, inside, across = (0, 1, 2, 3, 4), (0, 2), (1, 3, 4)

    def group_of(r, g, headings):
        forces(r, g, headings)
        scatter(r, g, headings)

    def step(state, sums, live):
        safe = jnp.where(live, state[9], 1.0)
        mass = density * safe * safe * safe
        inverse = 1.0 / mass
        spin_inverse = 1.0 / (0.4 * mass * safe * safe)
        new = [None] * components
        for c in range(3):
            accel = sums[c] * inverse
            if c == 2:
                accel = accel - gravity
            speed = state[3 + c] + timestep_length * accel
            new[c] = state[c] + timestep_length * speed
            new[3 + c] = speed
            new[6 + c] = state[6 + c] + timestep_length * sums[3 + c] * spin_inverse
        new[9] = state[9]
        new[10] = state[10] + timestep_length * sums[6] * inverse
        return [jnp.where(live, v, 0.0) for v in new]

    def step_group(r, g, left=None):
        cells = slice(g * TILE, (g + 1) * TILE)
        sums = [totals[r, 1 + g * TILE : 1 + (g + 1) * TILE, c, :] for c in range(7)]
        if r == 0:
            sums = [
                v + jnp.where(has[-1, 0], owed_sum(c, cells), 0.0) for c, v in enumerate(sums)
            ]
        live = lane_f < filled_wide[r, cells, :]
        state = [ghost[c, r, TILE + g * TILE : 2 * TILE + g * TILE, :] for c in range(components)]
        if left is not None:
            live = live & ~left[cells]
        for c, value in enumerate(step(state, sums, live)):
            out_ref[c, r, cells, :] = value

    def list_of(direction, r):
        cell_line = jnp.full((1, slots), -1, jnp.int32)
        slot_line = jnp.zeros((1, slots), jnp.int32)
        for k in range(movers):
            cell_line = jnp.where(line_lane == k, out_movers[direction, 0, 0, k] - r * cols, cell_line)
            slot_line = jnp.where(line_lane == k, out_movers[direction, 1, 0, k], slot_line)
        cell_line = jnp.where(line_lane < move_count[0, 0, direction], cell_line, -1)
        return cell_line, slot_line

    def chosen_of(cell_line, slot_line):
        chosen = cell_ids == cell_line
        slot_f = jnp.where(chosen, jnp.broadcast_to(slot_line + 1, (cols, slots)).astype(jnp.float32), 0.0)
        slot_of = jnp.sum(slot_f, axis=1, keepdims=True).astype(jnp.int32) - 1
        slot_of = jnp.broadcast_to(slot_of, (cols, slots))
        index = jnp.maximum(slot_of, 0)

        def line_of(value):
            return jnp.sum(jnp.where(chosen, lanes_of(value, index), 0.0), axis=0, keepdims=True)

        return line_of, lane_ids == slot_of

    def landing_of(direction, r):
        key = jnp.zeros((1, slots), jnp.int32)
        cell_line = jnp.full((1, slots), -1, jnp.int32)
        for k in range(movers):
            hit = line_lane == in_movers[direction, 1, 0, k]
            key = jnp.where(hit, k, key)
            cell_line = jnp.where(hit, in_movers[direction, 0, 0, k] - r * cols, cell_line)
        return key, cell_line

    def put(r, there, message, lists):
        key, cell_line = lists
        landing = cell_ids == jnp.where(there, cell_line, -1)
        values = lanes_of(message, jnp.broadcast_to(key, message.shape))
        for c in range(components):
            out_ref[c, r] = jnp.where(landing, values[c : c + 1], out_ref[c, r])

    def finish(direction, message, row, extra, state_of):
        cells_new = message[7:8].astype(jnp.int32)
        lines_new, _ = chosen_of(cells_new, message[8:9].astype(jnp.int32))
        sums = [
            lines_new(extra(c, totals[row, 1 : 1 + cols, c, :])) + message[c : c + 1]
            for c in range(7)
        ]
        state = [state_of(c, lines_new) for c in range(components)]
        moving = cells_new >= 0
        for c, value in enumerate(step(state, sums, moving)):
            if c == 0:
                value = value + jnp.where(moving, -1.0 if direction == 0 else 1.0, 0.0)
            landed[direction, c : c + 1, :] = value

    def share_of(direction, r, lines, cells_line, slots_line):
        for c in range(7):
            msg_out[direction, c : c + 1, :] = lines(totals[r, 1 : 1 + cols, c, :])
        msg_out[direction, 7:8, :] = cells_line.astype(jnp.float32)
        msg_out[direction, 8:9, :] = slots_line.astype(jnp.float32)

    last = rows - 1
    lax.fori_loop(0, wide, clear, 0)
    msg_out[...] = jnp.zeros(msg_out.shape, jnp.float32)
    landed[...] = jnp.zeros(landed.shape, jnp.float32)
    own[0].wait()
    pack(0, packed)
    own[4].wait()

    @pl.when(far_up)
    def _():
        pack(last, packed_last)

    pl.semaphore_wait(barrier, expected)
    start("side right", "side left", ("ghost", 0), "corner left", "corner right")
    start(*(("ghost", g) for g in order[1:]))
    start("far pairs", "far count")
    for n, copy in enumerate(own):
        if n not in (0, 4):
            copy.wait()
    for r in range(rows):
        spread(count_own, r, count_wide, r)
        spread(filled_ref, r, filled_wide, r)

    def early(g):
        for r in range(last):
            group_of(r, g, every)
        group_of(last, g, inside)

    def inner(n, _):
        early(n)
        return 0

    def outer(n, _):
        early((groups - 1) * n)
        return 0

    lax.fori_loop(1, groups - 1, inner, 0)
    arrive("side right", "side left")
    lax.fori_loop(0, 2, outer, 0)
    for r in range(rows):
        edge_out[0, r] = totals[r, 0]
        edge_out[1, r] = totals[r, wide - 1]
    start("edge low", "edge high")
    cells_back, slots_back = list_of(1, 0)
    lines_back, left_back = chosen_of(cells_back, slots_back)
    cells_on, slots_on = list_of(0, last)
    lines_on, left_on = chosen_of(cells_on, slots_on)
    arrive("edge low", "edge high")
    for r in range(rows):
        totals[r, 1] += jnp.where(has[0, -1], owed_low[r], 0.0)
        totals[r, cols] += jnp.where(has[0, 1], owed_high[r], 0.0)
    share_of(1, 0, lines_back, cells_back, slots_back)
    start("backward")
    start(*(("far", g) for g in middle))
    lists_first, lists_last = landing_of(0, 0), landing_of(1, last)

    for r in range(1, last):
        for g in range(groups):
            step_group(r, g)

    def last_group(g):
        arrive(("ghost", g))
        if g == 0:
            unpack(rows, 0)
            unpack(rows, 1)
            arrive("corner left")
        elif g == groups - 1:
            unpack(rows, cols - TILE - 1)
            unpack(rows, cols - TILE)
            arrive("corner right")
        else:
            unpack(rows, g * TILE + 1)
        group_of(last, g, across)
        load_heat(g)
        start(("owed", g))

    last_group(0)
    start("late high", "diag high")
    last_group(groups - 1)
    start("late low", "diag low")

    @pl.when(far_up)
    def _():
        for n, col in enumerate(seams):
            seam_out[n] = totals[rows, 1 + col]
        start("seams")
        share_of(0, last, lines_on, cells_on, slots_on)
        for c in range(components):
            msg_out[0, 9 + c : 10 + c, :] = lines_on(ghost[c, last, own_cols, :])
        start("forward")

    for g in middle:
        last_group(g)
    for g in range(groups):
        step_group(last, g)

    @pl.when(has[1, 0] & ~far_up)
    def _():
        for c in range(components):
            line = lines_on(out_ref[c, last])
            if c == 0:
                line = line - jnp.where(cells_on >= 0, 1.0, 0.0)
            msg_out[0, c : c + 1, :] = line
        start("forward")

    for c in range(components):
        out_ref[c, last] = jnp.where(left_on, 0.0, out_ref[c, last])

    def late_edges(c, value):
        value = value + jnp.where((cell_ids == 0) & has[0, -1], late_low[c : c + 1, :], 0.0)
        return value + jnp.where((cell_ids == cols - 1) & has[0, 1], late_high[c : c + 1, :], 0.0)

    arrive("late low", "late high", "backward")

    @pl.when(has[1, 0])
    def _():
        finish(1, msg_in[1], rows, late_edges, lambda c, lines: lines(ghost[c, rows, own_cols, :]))
        put(last, has[1, 0], landed[1], lists_last)

    sent(*moves)

    def add_diagonals():
        totals[0, 1] += jnp.where(has[-1, -1], owed_diag[0], 0.0)
        totals[0, cols] += jnp.where(has[-1, 1], owed_diag[1], 0.0)

    @pl.when(far_down)
    def _():
        arrive("far count", "far pairs")
        spread(count_prev, last, count_wide, rows)
        for g in middle:
            arrive(("far", g))
            unpack(before, g * TILE)
            group_of(before, g, across)
        arrive(("owed", 0), ("owed", groups - 1), "seams", "diag low", "diag high")
        add_diagonals()
        for n in range(TILE - 1, cols - TILE + 1):
            owed[n] = jnp.zeros((8, slots), jnp.float32)
        for n, col in enumerate(seams):
            totals[0, 1 + col] += seam_in[n]
        for g in range(groups):
            step_group(0, g, left_back)
        arrive("forward")
        message = msg_in[0]
        finish(0, message, before, lambda c, value: value, lambda c, _: message[9 + c : 10 + c])

    @pl.when(~far_down)
    def _():
        arrive(("owed", 0), ("owed", groups - 1), "diag low", "diag high")
        add_diagonals()
        for k, g in enumerate(order):
            if k > 1:
                arrive(("owed", g))
            if k > 1:
                step_group(0, g - 1, left_back)
        step_group(0, groups - 2, left_back)
        step_group(0, groups - 1, left_back)
        arrive("forward")
        landed[0, 0:components, :] = msg_in[0, 0:components, :]

    put(0, has[-1, 0], landed[0], lists_first)


def body(blades, spans, fars, particles, filled, contact_pairs, contact_count, movers_out, movers_in, move_count):
    components, rows, cols, slots = particles.shape
    padded = -(-components // 8) * 8
    message = -(-(components + 9) // 8) * 8
    f32, i32 = jnp.float32, jnp.int32
    riders = packing(components, slots, movers_out.shape[3])[3]
    remote_copies = 3 * (cols // TILE) + 13
    return pl.pallas_call(
        functools.partial(kernel, particles.shape, blades, spans, fars),
        out_shape=pltpu.VMEM(particles.shape, f32),
        in_specs=[pl.BlockSpec(memory_space=pl.ANY)] * 7,
        out_specs=pl.BlockSpec(memory_space=pltpu.VMEM),
        scratch_shapes=[
            pltpu.VMEM((components, rows + 2, cols + 2 * TILE, slots), f32),
            pltpu.VMEM((components - riders, cols, slots), f32),
            pltpu.VMEM((components - riders, cols, slots), f32),
            pltpu.VMEM((2, rows + 1, cols, contact_pairs.shape[3]), i32),
            pltpu.VMEM((rows, cols), i32),
            pltpu.VMEM((rows, cols), i32),
            pltpu.VMEM((rows, cols), i32),
            pltpu.SMEM(movers_out.shape, i32),
            pltpu.SMEM(movers_in.shape, i32),
            pltpu.SMEM((1, 1, 2), i32),
            pltpu.VMEM(((rows + 1) * cols * 8, slots), f32),
            pltpu.VMEM(((rows + 1) * cols * 8, slots), f32),
            pltpu.VMEM((rows + 1, cols, slots), f32),
            pltpu.VMEM((rows, cols, slots), f32),
            pltpu.VMEM((rows + 2, cols + 2, 8, slots), f32),
            pltpu.VMEM((2, rows, 8, slots), f32),
            pltpu.VMEM((rows, 8, slots), f32),
            pltpu.VMEM((rows, 8, slots), f32),
            pltpu.VMEM((8, slots), f32),
            pltpu.VMEM((8, slots), f32),
            pltpu.VMEM((4, 8, slots), f32),
            pltpu.VMEM((4, 8, slots), f32),
            pltpu.VMEM((cols, 8, slots), f32),
            pltpu.VMEM((2, 8, slots), f32),
            pltpu.VMEM((2, message, slots), f32),
            pltpu.VMEM((2, message, slots), f32),
            pltpu.VMEM((2, padded, slots), f32),
            pltpu.SemaphoreType.DMA((8,)),
            pltpu.SemaphoreType.DMA((remote_copies,)),
            pltpu.SemaphoreType.DMA((remote_copies,)),
        ],
        compiler_params=pltpu.CompilerParams(
            collective_id=0, has_side_effects=True, vmem_limit_bytes=VMEM_GRANT
        ),
    )(
        *(
            pltpu.with_memory_space_constraint(x, pltpu.HBM)
            for x in (
                particles,
                filled,
                contact_pairs,
                contact_count,
                movers_out,
                movers_in,
                jnp.transpose(move_count, (1, 2, 0)),
            )
        )
    )


def solution(mesh):
    sizes = dict(mesh.shape)
    return jax.shard_map(
        functools.partial(body, sizes["blade"], sizes["span"], far_boundaries(mesh)),
        mesh=mesh,
        in_specs=(
            P(None, "blade", "span", None),
            P("blade", "span"),
            P(None, "blade", "span", None),
            P("blade", "span"),
            P(None, None, "blade", "span"),
            P(None, None, "blade", "span"),
            P(None, "blade", "span"),
        ),
        out_specs=P(None, "blade", "span", None),
        check_vma=False,
    )
```

```python
import functools

import jax
import jax.numpy as jnp
from jax import lax
from jax.experimental import pallas as pl
from jax.experimental.pallas import tpu as pltpu
from jax.sharding import PartitionSpec as P

spring = 4.0
normal_damp = 0.5
tangent_damp = 0.3
conduct = 40.0
timestep_length = 0.05
density = 100.0
gravity = 9.81
soft_len = 0.05
row_steps = (0, 1, 0, 1, 1)
col_steps = (0, 0, 1, 1, -1)
MESH = pl.DeviceIdType.MESH
TILE = 8
VMEM_GRANT = 16 << 20


def cross(a, b):
    return (
        a[1] * b[2] - a[2] * b[1],
        a[2] * b[0] - a[0] * b[2],
        a[0] * b[1] - a[1] * b[0],
    )


def lanes_of(table, index):
    return jnp.take_along_axis(table, index, axis=1, mode="promise_in_bounds")


def pair_terms(first, second, row_shift, col_shift, live):
    gap = (
        second[0] + row_shift - first[0],
        second[1] + col_shift - first[1],
        second[2] - first[2],
    )
    distance = jnp.sqrt(gap[0] * gap[0] + gap[1] * gap[1] + gap[2] * gap[2] + soft_len * soft_len)
    inverse = 1.0 / distance
    normal = tuple(g * inverse for g in gap)
    rad_first, rad_second = first[9], second[9]
    intersection = rad_first + rad_second - distance
    spin = tuple(rad_first * first[6 + c] + rad_second * second[6 + c] for c in range(3))
    turn = cross(spin, normal)
    relative = tuple(second[3 + c] - first[3 + c] - turn[c] for c in range(3))
    speed = relative[0] * normal[0] + relative[1] * normal[1] + relative[2] * normal[2]
    friction = tuple(tangent_damp * (relative[c] - speed * normal[c]) for c in range(3))
    push = normal_damp * speed - spring * intersection
    force = tuple(push * normal[c] + friction[c] for c in range(3))
    torque = cross(normal, friction)
    denom = jnp.where(live, rad_first + rad_second, 1.0)
    heat = 2.0 * conduct * rad_first * rad_second / denom * (second[10] - first[10])
    on_first = force + tuple(rad_first * t for t in torque) + (heat,)
    on_second = tuple(-f for f in force) + tuple(rad_second * t for t in torque) + (-heat,)
    keep = lambda v: jnp.where(live, v, 0.0)
    return [keep(v) for v in on_first], [keep(v) for v in on_second]


def order_of(cols):
    groups = cols // TILE
    return [0, groups - 1, *range(1, groups - 1)]


def ghost_chunk(g, cols):
    groups = cols // TILE
    if g == 0:
        return 0, TILE + 1
    if g == groups - 1:
        return cols - TILE - 1, cols
    return g * TILE + 1, min((g + 1) * TILE + 1, cols - TILE - 1)


def owed_chunk(g, cols):
    groups = cols // TILE
    if g == 0:
        return 0, TILE - 1
    if g == groups - 1:
        return cols - TILE + 1, cols
    return g * TILE - 1, ((g + 1) * TILE - 1 if g < groups - 2 else cols - TILE + 1)


def packing(components, slots, movers):
    live = slots - 2 * movers
    spare = slots - live
    pieces = live // spare
    riders = components // (pieces + 1) if live % spare == 0 else 0
    sent_rows = 6 if live % spare == 0 and pieces <= 6 else 8
    return live, spare, pieces, riders, sent_rows


def far_boundaries(mesh):
    line = mesh.devices.reshape(mesh.devices.shape[0], -1)[:, 0]
    hops = [
        sum(abs(p - q) for p, q in zip(a.coords, b.coords)) for a, b in zip(line, line[1:])
    ]
    most = max(hops, default=0)
    if most == min(hops, default=0):
        return ()
    return tuple(n for n, h in enumerate(hops) if h >= most)


def is_far(boundary, blades, fars):
    for period in range(1, blades):
        if fars == tuple(range(period - 1, blades - 1, period)):
            return lax.rem(boundary + period, period) == period - 1
    far = boundary < -1
    for f in fars:
        far = far | (boundary == f)
    return far


def kernel(
    shape,
    blades,
    spans,
    fars,
    parts_hbm,
    filled_hbm,
    pairs_hbm,
    count_hbm,
    out_movers_hbm,
    in_movers_hbm,
    move_count_hbm,
    out_ref,
    ghost,
    packed,
    packed_last,
    pairs_ref,
    count_own,
    count_prev,
    filled_ref,
    out_movers,
    in_movers,
    move_count,
    first_terms,
    second_terms,
    count_wide,
    filled_wide,
    totals,
    edge_out,
    owed_low,
    owed_high,
    late_low,
    late_high,
    seam_out,
    seam_in,
    owed,
    owed_diag,
    msg_out,
    msg_in,
    landed,
    local_sem,
    send_sem,
    recv_sem,
):
    components, rows, cols, slots = shape
    movers = out_movers.shape[3]
    wide = cols + 2
    groups = cols // TILE
    live_slots, spare, pieces, riders, sent_rows = packing(components, slots, movers)
    carried = components - riders
    order = order_of(cols)
    middle = order[2:]
    seams = (TILE - 1, TILE, cols - TILE - 1, cols - TILE)
    i = lax.axis_index("blade")
    j = lax.axis_index("span")
    has = {}
    for di in (-1, 0, 1):
        for dj in (-1, 0, 1):
            if (di, dj) != (0, 0):
                a, b = i + di, j + dj
                has[di, dj] = (a >= 0) & (a < blades) & (b >= 0) & (b < spans)
    far_up = has[1, 0] & is_far(i, blades, fars)
    far_down = has[-1, 0] & is_far(i - 1, blades, fars)
    before = rows + 1

    own_cols = slice(TILE, TILE + cols)
    own = [
        pltpu.make_async_copy(source, target, local_sem.at[n])
        for n, (source, target) in enumerate(
            (
                (parts_hbm.at[:, 0], ghost.at[:, 0, own_cols, :]),
                (count_hbm, count_own),
                (filled_hbm, filled_ref),
                (pairs_hbm, pairs_ref.at[:, 0:rows]),
                (parts_hbm.at[:, 1:rows], ghost.at[:, 1:rows, own_cols, :]),
                (out_movers_hbm, out_movers),
                (in_movers_hbm, in_movers),
                (move_count_hbm, move_count),
            )
        )
    ]
    barrier = pltpu.get_barrier_semaphore()
    expected = jnp.int32(0)
    for (di, dj), there in has.items():
        expected = expected + there.astype(jnp.int32)

        @pl.when(there)
        def _(di=di, dj=dj):
            pl.semaphore_signal(
                barrier, inc=1, device_id=(i + di, j + dj), device_id_type=MESH
            )

    for copy in own:
        copy.start()

    moves = {}

    def move(name, source, target, di, dj, far=None):
        n = len(moves)
        copy = pltpu.make_async_remote_copy(
            src_ref=source,
            dst_ref=target,
            send_sem=send_sem.at[n],
            recv_sem=recv_sem.at[n],
            device_id=(i + di, j + dj),
            device_id_type=MESH,
        )
        sends, comes = has[di, dj], has[-di, -dj]
        if far is not None:
            sends = sends & (far_up if far else ~far_up)
            comes = comes & (far_down if far else ~far_down)
        moves[name] = (copy, sends, comes)

    low = slice(0, 1)
    high = slice(cols - 1, cols)
    left = slice(TILE - 1, TILE)
    right = slice(TILE + cols, TILE + cols + 1)
    for g in order:
        a, b = ghost_chunk(g, cols)
        target = ghost.at[0:carried, rows, TILE + a : TILE + b, :]
        move(("ghost", g), packed.at[:, a:b], target, -1, 0)
    move("corner right", parts_hbm.at[:, 0, low, :], ghost.at[:, rows, right, :], -1, -1)
    move("corner left", parts_hbm.at[:, 0, high, :], ghost.at[:, rows, left, :], -1, 1)
    move("side right", parts_hbm.at[:, :, low, :], ghost.at[:, 0:rows, right, :], 0, -1)
    move("side left", parts_hbm.at[:, :, high, :], ghost.at[:, 0:rows, left, :], 0, 1)
    move("edge low", edge_out.at[1], owed_low, 0, 1)
    move("edge high", edge_out.at[0], owed_high, 0, -1)
    move("late low", totals.at[rows, wide - 1], late_low, 0, 1)
    move("late high", totals.at[rows, 0], late_high, 0, -1)
    for g in order:
        a, b = owed_chunk(g, cols)
        mode = False if g in middle else None
        source, target = totals.at[rows, 1 + a : 1 + b, 0:sent_rows], owed.at[a:b, 0:sent_rows]
        move(("owed", g), source, target, 1, 0, mode)
    move("diag low", totals.at[rows, wide - 1], owed_diag.at[0], 1, 1)
    move("diag high", totals.at[rows, 0], owed_diag.at[1], 1, -1)
    move("seams", seam_out, seam_in, 1, 0, True)
    inner_cols = slice(TILE, cols - TILE)
    target = pairs_ref.at[:, rows, inner_cols]
    move("far pairs", pairs_hbm.at[:, rows - 1, inner_cols], target, 1, 0, True)
    move("far count", count_hbm, count_prev, 1, 0, True)
    for g in middle:
        a, b = g * TILE, (g + 1) * TILE
        target = ghost.at[0:carried, before, TILE + a : TILE + b, :]
        move(("far", g), packed_last.at[:, a:b], target, 1, 0, True)
    move("forward", msg_out.at[0], msg_in.at[0], 1, 0)
    move("backward", msg_out.at[1], msg_in.at[1], -1, 0)

    def start(*which):
        for w in which:
            copy, sends, comes = moves[w]

            @pl.when(sends)
            def _(copy=copy):
                copy.start()

    def arrive(*which):
        for w in which:
            copy, sends, comes = moves[w]

            @pl.when(comes)
            def _(copy=copy):
                copy.wait_recv()

    def sent(*which):
        for w in which:
            copy, sends, comes = moves[w]

            @pl.when(sends)
            def _(copy=copy):
                copy.wait_send()

    diagonal = lax.broadcasted_iota(jnp.int32, (cols, cols), 0) == lax.broadcasted_iota(
        jnp.int32, (cols, cols), 1
    )
    lane = lax.broadcasted_iota(jnp.int32, (TILE, slots), 1)
    lane_f = lane.astype(jnp.float32)
    slot_ids = lax.broadcasted_iota(jnp.int32, (slots, slots), 0)
    line_lane = lax.broadcasted_iota(jnp.int32, (1, slots), 1)
    cell_ids = lax.broadcasted_iota(jnp.int32, (cols, slots), 0)
    lane_ids = lax.broadcasted_iota(jnp.int32, (cols, slots), 1)

    def spread(source, r, target, at):
        line = jnp.broadcast_to(source[r : r + 1, :].astype(jnp.float32), (cols, cols))
        column = jnp.sum(jnp.where(diagonal, line, 0.0), axis=1, keepdims=True)
        target[at] = jnp.broadcast_to(column, (cols, slots))

    def clear(n, _):
        for r in range(rows + 2):
            totals[r, n] = jnp.zeros((8, slots), jnp.float32)
        return 0

    def pack(r, target):
        for c in range(carried):
            value = ghost[c, r, own_cols, :]
            if c < riders * pieces:
                rider, piece = carried + c // pieces, c % pieces
                shift = live_slots - piece * spare
                moved = pltpu.roll(ghost[rider, r, own_cols, :], shift, 1)
                value = jnp.where(lane_ids < live_slots, value, moved)
            target[c] = value

    def unpack(r, at):
        for e in range(riders):
            value = None
            for piece in range(pieces):
                shift = (piece * spare - live_slots) % slots
                tile = ghost[e * pieces + piece, r, TILE + at : 2 * TILE + at, :]
                moved = pltpu.roll(tile, shift, 1)
                value = moved if piece == 0 else jnp.where(lane >= piece * spare, moved, value)
            ghost[carried + e, r, TILE + at : 2 * TILE + at, :] = value

    def load_heat(g):
        if sent_rows == 8:
            return
        a, b = owed_chunk(g, cols)
        for first in {a, b - TILE} if b - a >= TILE else {a}:
            n = min(TILE, b - a)
            cells = slice(1 + first, 1 + first + n)
            heat = totals[rows, cells, 6, :]
            spot = lax.broadcasted_iota(jnp.int32, (n, slots), 1) < live_slots
            for piece in range(pieces):
                moved = pltpu.roll(heat, live_slots - piece * spare, 1)
                totals[rows, cells, piece, :] = jnp.where(spot, totals[rows, cells, piece, :], moved)

    def owed_sum(c, cells):
        if c < 6 or sent_rows == 8:
            return owed[cells, c, :]
        value = None
        for piece in range(pieces):
            moved = pltpu.roll(owed[cells, piece, :], (piece * spare - live_slots) % slots, 1)
            value = moved if piece == 0 else jnp.where(lane >= piece * spare, moved, value)
        return value

    def tiles_of(g):
        return g * TILE if isinstance(g, int) else pl.multiple_of(g * TILE, TILE)

    def row_of(r):
        if r == before:
            return before, rows, lambda d: 0
        return r, r, lambda d: r + row_steps[d]

    def contacts_of(r, g):
        at = tiles_of(g)
        _, listed, _ = row_of(r)
        ids = pairs_ref[0, listed, pl.ds(at, TILE), :]
        code = pairs_ref[1, listed, pl.ds(at, TILE), :]
        heading = code // slots
        return ids, heading, code - heading * slots

    def forces(r, g, headings):
        at = tiles_of(g)
        near, listed, far_row = row_of(r)
        ids, heading, target = contacts_of(r, g)
        live = lane_f < count_wide[listed, pl.ds(at, TILE), :]
        if len(headings) < len(row_steps):
            among = heading == headings[0]
            for d in headings[1:]:
                among = among | (heading == d)
            live = live & among
        first = [
            lanes_of(ghost[c, near, pl.ds(at + TILE, TILE), :], ids) for c in range(components)
        ]
        second = [None] * components
        for n, d in enumerate(headings):
            pick = heading == d
            for c in range(components):
                rows_at = pl.ds(at + TILE + col_steps[d], TILE)
                value = lanes_of(ghost[c, far_row(d), rows_at, :], target)
                second[c] = value if n == 0 else jnp.where(pick, value, second[c])
        row_shift = jnp.where((heading == 0) | (heading == 2), 0.0, 1.0)
        col_shift = jnp.where(
            (heading == 2) | (heading == 3), 1.0, jnp.where(heading == 4, -1.0, 0.0)
        )
        on_first, on_second = pair_terms(first, second, row_shift, col_shift, live)
        zero = jnp.zeros((TILE, slots), jnp.float32)
        base = (listed * cols + g * TILE) * 8
        for c, (a, b) in enumerate(zip(on_first + [zero], on_second + [zero])):
            first_terms[pl.ds(base + c, TILE, stride=8), :] = a
            second_terms[pl.ds(base + c, TILE, stride=8), :] = b

    def scatter(r, g, headings):
        near, listed, far_row = row_of(r)
        ids, heading, target = contacts_of(r, g)
        shared = 0 in headings
        zero = jnp.zeros((8, slots), jnp.float32)
        for n in range(TILE):
            base = (listed * cols + g * TILE + n) * 8
            if not isinstance(base, int):
                base = pl.multiple_of(base, 8)
            a = first_terms[pl.ds(base, 8), :]
            b = second_terms[pl.ds(base, 8), :]
            head = heading[n : n + 1]
            blocks = [jnp.where(head == d, b, 0.0) for d in headings]
            if not shared:
                blocks = [zero] + blocks
            near_blocks = [a] + [zero] * (len(blocks) - 1)
            terms = jnp.concatenate(
                [jnp.concatenate(near_blocks, axis=0), jnp.concatenate(blocks, axis=0)], axis=1
            )
            near_hot = jnp.where(slot_ids == ids[n : n + 1], 1.0, 0.0)
            hot = jnp.where(slot_ids == target[n : n + 1], 1.0, 0.0)
            hot = jnp.concatenate([near_hot, hot], axis=1)
            coarse = terms.astype(jnp.bfloat16).astype(jnp.float32)
            split = jnp.concatenate([coarse, terms - coarse], axis=0).astype(jnp.bfloat16)
            summed = lax.dot_general(
                split,
                hot.astype(jnp.bfloat16),
                (((1,), (1,)), ((), ())),
                preferred_element_type=jnp.float32,
            )
            count = len(blocks) * 8
            summed = summed[:count] + summed[count:]
            places = [(far_row(d), col_steps[d]) for d in headings]
            if not shared:
                places = [(near, 0)] + places
            for m, (row, shift) in enumerate(places):
                totals[row, g * TILE + n + 1 + shift] += summed[m * 8 : m * 8 + 8]

    every, inside, across = (0, 1, 2, 3, 4), (0, 2), (1, 3, 4)

    def group_of(r, g, headings):
        forces(r, g, headings)
        scatter(r, g, headings)

    def step(state, sums, live):
        safe = jnp.where(live, state[9], 1.0)
        mass = density * safe * safe * safe
        inverse = 1.0 / mass
        spin_inverse = 1.0 / (0.4 * mass * safe * safe)
        new = [None] * components
        for c in range(3):
            accel = sums[c] * inverse
            if c == 2:
                accel = accel - gravity
            speed = state[3 + c] + timestep_length * accel
            new[c] = state[c] + timestep_length * speed
            new[3 + c] = speed
            new[6 + c] = state[6 + c] + timestep_length * sums[3 + c] * spin_inverse
        new[9] = state[9]
        new[10] = state[10] + timestep_length * sums[6] * inverse
        return [jnp.where(live, v, 0.0) for v in new]

    def step_group(r, g, left=None):
        cells = slice(g * TILE, (g + 1) * TILE)
        sums = [totals[r, 1 + g * TILE : 1 + (g + 1) * TILE, c, :] for c in range(7)]
        if r == 0:
            sums = [
                v + jnp.where(has[-1, 0], owed_sum(c, cells), 0.0) for c, v in enumerate(sums)
            ]
        live = lane_f < filled_wide[r, cells, :]
        state = [ghost[c, r, TILE + g * TILE : 2 * TILE + g * TILE, :] for c in range(components)]
        if left is not None:
            live = live & ~left[cells]
        for c, value in enumerate(step(state, sums, live)):
            out_ref[c, r, cells, :] = value

    def list_of(direction, r):
        cell_line = jnp.full((1, slots), -1, jnp.int32)
        slot_line = jnp.zeros((1, slots), jnp.int32)
        for k in range(movers):
            cell_line = jnp.where(line_lane == k, out_movers[direction, 0, 0, k] - r * cols, cell_line)
            slot_line = jnp.where(line_lane == k, out_movers[direction, 1, 0, k], slot_line)
        cell_line = jnp.where(line_lane < move_count[0, 0, direction], cell_line, -1)
        return cell_line, slot_line

    def chosen_of(cell_line, slot_line):
        chosen = cell_ids == cell_line
        slot_f = jnp.where(chosen, jnp.broadcast_to(slot_line + 1, (cols, slots)).astype(jnp.float32), 0.0)
        slot_of = jnp.sum(slot_f, axis=1, keepdims=True).astype(jnp.int32) - 1
        slot_of = jnp.broadcast_to(slot_of, (cols, slots))
        index = jnp.maximum(slot_of, 0)

        def line_of(value):
            return jnp.sum(jnp.where(chosen, lanes_of(value, index), 0.0), axis=0, keepdims=True)

        return line_of, lane_ids == slot_of

    def landing_of(direction, r):
        key = jnp.zeros((1, slots), jnp.int32)
        cell_line = jnp.full((1, slots), -1, jnp.int32)
        for k in range(movers):
            hit = line_lane == in_movers[direction, 1, 0, k]
            key = jnp.where(hit, k, key)
            cell_line = jnp.where(hit, in_movers[direction, 0, 0, k] - r * cols, cell_line)
        return key, cell_line

    def put(r, there, message, lists):
        key, cell_line = lists
        landing = cell_ids == jnp.where(there, cell_line, -1)
        values = lanes_of(message, jnp.broadcast_to(key, message.shape))
        for c in range(components):
            out_ref[c, r] = jnp.where(landing, values[c : c + 1], out_ref[c, r])

    def finish(direction, message, row, extra, state_of):
        cells_new = message[7:8].astype(jnp.int32)
        lines_new, _ = chosen_of(cells_new, message[8:9].astype(jnp.int32))
        sums = [
            lines_new(extra(c, totals[row, 1 : 1 + cols, c, :])) + message[c : c + 1]
            for c in range(7)
        ]
        state = [state_of(c, lines_new) for c in range(components)]
        moving = cells_new >= 0
        for c, value in enumerate(step(state, sums, moving)):
            if c == 0:
                value = value + jnp.where(moving, -1.0 if direction == 0 else 1.0, 0.0)
            landed[direction, c : c + 1, :] = value

    def share_of(direction, r, lines, cells_line, slots_line):
        for c in range(7):
            msg_out[direction, c : c + 1, :] = lines(totals[r, 1 : 1 + cols, c, :])
        msg_out[direction, 7:8, :] = cells_line.astype(jnp.float32)
        msg_out[direction, 8:9, :] = slots_line.astype(jnp.float32)

    last = rows - 1
    lax.fori_loop(0, wide, clear, 0)
    msg_out[...] = jnp.zeros(msg_out.shape, jnp.float32)
    landed[...] = jnp.zeros(landed.shape, jnp.float32)
    own[0].wait()
    pack(0, packed)
    own[4].wait()

    @pl.when(far_up)
    def _():
        pack(last, packed_last)

    pl.semaphore_wait(barrier, expected)
    start("side right", "side left", ("ghost", 0), "corner left", ("ghost", groups - 1), "corner right")

    @pl.when(~far_down)
    def _():
        start(*(("ghost", g) for g in middle))

    start("far pairs", "far count")
    for n, copy in enumerate(own):
        if n not in (0, 4):
            copy.wait()
    for r in range(rows):
        spread(count_own, r, count_wide, r)
        spread(filled_ref, r, filled_wide, r)

    def early(g):
        for r in range(last):
            group_of(r, g, every)
        group_of(last, g, inside)

    def inner(n, _):
        early(n)
        return 0

    def outer(n, _):
        early((groups - 1) * n)
        return 0

    lax.fori_loop(1, groups - 1, inner, 0)
    arrive("side right", "side left")
    lax.fori_loop(0, 1, outer, 0)

    @pl.when(far_down)
    def _():
        start(*(("ghost", g) for g in middle))

    lax.fori_loop(1, 2, outer, 0)
    for r in range(rows):
        edge_out[0, r] = totals[r, 0]
        edge_out[1, r] = totals[r, wide - 1]
    start("edge low", "edge high")
    cells_back, slots_back = list_of(1, 0)
    lines_back, left_back = chosen_of(cells_back, slots_back)
    cells_on, slots_on = list_of(0, last)
    lines_on, left_on = chosen_of(cells_on, slots_on)
    arrive("edge low", "edge high")
    for r in range(rows):
        totals[r, 1] += jnp.where(has[0, -1], owed_low[r], 0.0)
        totals[r, cols] += jnp.where(has[0, 1], owed_high[r], 0.0)
    share_of(1, 0, lines_back, cells_back, slots_back)
    start("backward")
    start(*(("far", g) for g in middle))
    lists_first, lists_last = landing_of(0, 0), landing_of(1, last)

    for r in range(1, last):
        for g in range(groups):
            step_group(r, g)

    def last_group(g):
        arrive(("ghost", g))
        if g == 0:
            unpack(rows, 0)
            unpack(rows, 1)
            arrive("corner left")
        elif g == groups - 1:
            unpack(rows, cols - TILE - 1)
            unpack(rows, cols - TILE)
            arrive("corner right")
        else:
            unpack(rows, g * TILE + 1)
        group_of(last, g, across)
        load_heat(g)
        start(("owed", g))

    last_group(0)
    start("late high", "diag high")
    last_group(groups - 1)
    start("late low", "diag low")

    @pl.when(far_up)
    def _():
        for n, col in enumerate(seams):
            seam_out[n] = totals[rows, 1 + col]
        start("seams")
        share_of(0, last, lines_on, cells_on, slots_on)
        for c in range(components):
            msg_out[0, 9 + c : 10 + c, :] = lines_on(ghost[c, last, own_cols, :])
        start("forward")

    for g in middle:
        last_group(g)
    for g in range(groups):
        step_group(last, g)

    @pl.when(has[1, 0] & ~far_up)
    def _():
        for c in range(components):
            line = lines_on(out_ref[c, last])
            if c == 0:
                line = line - jnp.where(cells_on >= 0, 1.0, 0.0)
            msg_out[0, c : c + 1, :] = line
        start("forward")

    for c in range(components):
        out_ref[c, last] = jnp.where(left_on, 0.0, out_ref[c, last])

    def late_edges(c, value):
        value = value + jnp.where((cell_ids == 0) & has[0, -1], late_low[c : c + 1, :], 0.0)
        return value + jnp.where((cell_ids == cols - 1) & has[0, 1], late_high[c : c + 1, :], 0.0)

    arrive("late low", "late high", "backward")

    @pl.when(has[1, 0])
    def _():
        finish(1, msg_in[1], rows, late_edges, lambda c, lines: lines(ghost[c, rows, own_cols, :]))
        put(last, has[1, 0], landed[1], lists_last)

    sent(*moves)

    def add_diagonals():
        totals[0, 1] += jnp.where(has[-1, -1], owed_diag[0], 0.0)
        totals[0, cols] += jnp.where(has[-1, 1], owed_diag[1], 0.0)

    @pl.when(far_down)
    def _():
        arrive("far count", "far pairs")
        spread(count_prev, last, count_wide, rows)
        for g in middle:
            arrive(("far", g))
            unpack(before, g * TILE)
            group_of(before, g, across)
        arrive(("owed", 0), ("owed", groups - 1), "seams", "diag low", "diag high")
        add_diagonals()
        for n in range(TILE - 1, cols - TILE + 1):
            owed[n] = jnp.zeros((8, slots), jnp.float32)
        for n, col in enumerate(seams):
            totals[0, 1 + col] += seam_in[n]
        for g in range(groups):
            step_group(0, g, left_back)
        arrive("forward")
        message = msg_in[0]
        finish(0, message, before, lambda c, value: value, lambda c, _: message[9 + c : 10 + c])

    @pl.when(~far_down)
    def _():
        arrive(("owed", 0), ("owed", groups - 1), "diag low", "diag high")
        add_diagonals()
        for k, g in enumerate(order):
            if k > 1:
                arrive(("owed", g))
            if k > 1:
                step_group(0, g - 1, left_back)
        step_group(0, groups - 2, left_back)
        step_group(0, groups - 1, left_back)
        arrive("forward")
        landed[0, 0:components, :] = msg_in[0, 0:components, :]

    put(0, has[-1, 0], landed[0], lists_first)


def body(blades, spans, fars, particles, filled, contact_pairs, contact_count, movers_out, movers_in, move_count):
    components, rows, cols, slots = particles.shape
    padded = -(-components // 8) * 8
    message = -(-(components + 9) // 8) * 8
    f32, i32 = jnp.float32, jnp.int32
    riders = packing(components, slots, movers_out.shape[3])[3]
    remote_copies = 3 * (cols // TILE) + 13
    return pl.pallas_call(
        functools.partial(kernel, particles.shape, blades, spans, fars),
        out_shape=pltpu.VMEM(particles.shape, f32),
        in_specs=[pl.BlockSpec(memory_space=pl.ANY)] * 7,
        out_specs=pl.BlockSpec(memory_space=pltpu.VMEM),
        scratch_shapes=[
            pltpu.VMEM((components, rows + 2, cols + 2 * TILE, slots), f32),
            pltpu.VMEM((components - riders, cols, slots), f32),
            pltpu.VMEM((components - riders, cols, slots), f32),
            pltpu.VMEM((2, rows + 1, cols, contact_pairs.shape[3]), i32),
            pltpu.VMEM((rows, cols), i32),
            pltpu.VMEM((rows, cols), i32),
            pltpu.VMEM((rows, cols), i32),
            pltpu.SMEM(movers_out.shape, i32),
            pltpu.SMEM(movers_in.shape, i32),
            pltpu.SMEM((1, 1, 2), i32),
            pltpu.VMEM(((rows + 1) * cols * 8, slots), f32),
            pltpu.VMEM(((rows + 1) * cols * 8, slots), f32),
            pltpu.VMEM((rows + 1, cols, slots), f32),
            pltpu.VMEM((rows, cols, slots), f32),
            pltpu.VMEM((rows + 2, cols + 2, 8, slots), f32),
            pltpu.VMEM((2, rows, 8, slots), f32),
            pltpu.VMEM((rows, 8, slots), f32),
            pltpu.VMEM((rows, 8, slots), f32),
            pltpu.VMEM((8, slots), f32),
            pltpu.VMEM((8, slots), f32),
            pltpu.VMEM((4, 8, slots), f32),
            pltpu.VMEM((4, 8, slots), f32),
            pltpu.VMEM((cols, 8, slots), f32),
            pltpu.VMEM((2, 8, slots), f32),
            pltpu.VMEM((2, message, slots), f32),
            pltpu.VMEM((2, message, slots), f32),
            pltpu.VMEM((2, padded, slots), f32),
            pltpu.SemaphoreType.DMA((8,)),
            pltpu.SemaphoreType.DMA((remote_copies,)),
            pltpu.SemaphoreType.DMA((remote_copies,)),
        ],
        compiler_params=pltpu.CompilerParams(
            collective_id=0, has_side_effects=True, vmem_limit_bytes=VMEM_GRANT
        ),
    )(
        *(
            pltpu.with_memory_space_constraint(x, pltpu.HBM)
            for x in (
                particles,
                filled,
                contact_pairs,
                contact_count,
                movers_out,
                movers_in,
                jnp.transpose(move_count, (1, 2, 0)),
            )
        )
    )


def solution(mesh):
    sizes = dict(mesh.shape)
    return jax.shard_map(
        functools.partial(body, sizes["blade"], sizes["span"], far_boundaries(mesh)),
        mesh=mesh,
        in_specs=(
            P(None, "blade", "span", None),
            P("blade", "span"),
            P(None, "blade", "span", None),
            P("blade", "span"),
            P(None, None, "blade", "span"),
            P(None, None, "blade", "span"),
            P(None, "blade", "span"),
        ),
        out_specs=P(None, "blade", "span", None),
        check_vma=False,
    )
```

```python
import functools

import jax
import jax.numpy as jnp
from jax import lax
from jax.experimental import pallas as pl
from jax.experimental.pallas import tpu as pltpu
from jax.sharding import PartitionSpec as P

spring = 4.0
normal_damp = 0.5
tangent_damp = 0.3
conduct = 40.0
timestep_length = 0.05
density = 100.0
gravity = 9.81
soft_len = 0.05
row_steps = (0, 1, 0, 1, 1)
col_steps = (0, 0, 1, 1, -1)
MESH = pl.DeviceIdType.MESH
TILE = 8
VMEM_GRANT = 16 << 20


def cross(a, b):
    return (
        a[1] * b[2] - a[2] * b[1],
        a[2] * b[0] - a[0] * b[2],
        a[0] * b[1] - a[1] * b[0],
    )


def lanes_of(table, index):
    return jnp.take_along_axis(table, index, axis=1, mode="promise_in_bounds")


def pair_terms(first, second, row_shift, col_shift, live):
    gap = (
        second[0] + row_shift - first[0],
        second[1] + col_shift - first[1],
        second[2] - first[2],
    )
    distance = jnp.sqrt(gap[0] * gap[0] + gap[1] * gap[1] + gap[2] * gap[2] + soft_len * soft_len)
    inverse = 1.0 / distance
    normal = tuple(g * inverse for g in gap)
    rad_first, rad_second = first[9], second[9]
    intersection = rad_first + rad_second - distance
    spin = tuple(rad_first * first[6 + c] + rad_second * second[6 + c] for c in range(3))
    turn = cross(spin, normal)
    relative = tuple(second[3 + c] - first[3 + c] - turn[c] for c in range(3))
    speed = relative[0] * normal[0] + relative[1] * normal[1] + relative[2] * normal[2]
    friction = tuple(tangent_damp * (relative[c] - speed * normal[c]) for c in range(3))
    push = normal_damp * speed - spring * intersection
    force = tuple(push * normal[c] + friction[c] for c in range(3))
    torque = cross(normal, friction)
    denom = jnp.where(live, rad_first + rad_second, 1.0)
    heat = 2.0 * conduct * rad_first * rad_second / denom * (second[10] - first[10])
    on_first = force + tuple(rad_first * t for t in torque) + (heat,)
    on_second = tuple(-f for f in force) + tuple(rad_second * t for t in torque) + (-heat,)
    keep = lambda v: jnp.where(live, v, 0.0)
    return [keep(v) for v in on_first], [keep(v) for v in on_second]


def order_of(cols):
    groups = cols // TILE
    return [0, groups - 1, *range(1, groups - 1)]


def ghost_chunk(g, cols):
    groups = cols // TILE
    if g == 0:
        return 0, TILE + 1
    if g == groups - 1:
        return cols - TILE - 1, cols
    return g * TILE + 1, min((g + 1) * TILE + 1, cols - TILE - 1)


def owed_chunk(g, cols):
    groups = cols // TILE
    if g == 0:
        return 0, TILE - 1
    if g == groups - 1:
        return cols - TILE + 1, cols
    return g * TILE - 1, ((g + 1) * TILE - 1 if g < groups - 2 else cols - TILE + 1)


def packing(components, slots, movers, groups):
    live = slots - 2 * movers
    spare = slots - live
    pieces = live // spare
    riders = components // (pieces + 1) if live % spare == 0 else 0
    extra = (riders + 1) * pieces - (components - riders - 1)
    if riders and extra == 1 and spare * groups <= slots:
        riders += 1
    sent_rows = 6 if live % spare == 0 and pieces <= 6 else 8
    return live, spare, pieces, riders, sent_rows


def far_boundaries(mesh):
    line = mesh.devices.reshape(mesh.devices.shape[0], -1)[:, 0]
    hops = [
        sum(abs(p - q) for p, q in zip(a.coords, b.coords)) for a, b in zip(line, line[1:])
    ]
    most = max(hops, default=0)
    if most == min(hops, default=0):
        return ()
    return tuple(n for n, h in enumerate(hops) if h >= most)


def is_far(boundary, blades, fars):
    for period in range(1, blades):
        if fars == tuple(range(period - 1, blades - 1, period)):
            return lax.rem(boundary + period, period) == period - 1
    far = boundary < -1
    for f in fars:
        far = far | (boundary == f)
    return far


def kernel(
    shape,
    blades,
    spans,
    fars,
    parts_hbm,
    filled_hbm,
    pairs_hbm,
    count_hbm,
    out_movers_hbm,
    in_movers_hbm,
    move_count_hbm,
    out_ref,
    ghost,
    packed,
    packed_last,
    rest_out,
    rest_in,
    rest,
    pairs_ref,
    count_own,
    count_prev,
    filled_ref,
    out_movers,
    in_movers,
    move_count,
    first_terms,
    second_terms,
    count_wide,
    filled_wide,
    totals,
    edge_out,
    owed_low,
    owed_high,
    late_low,
    late_high,
    seam_out,
    seam_in,
    owed,
    owed_diag,
    msg_out,
    msg_in,
    landed,
    local_sem,
    send_sem,
    recv_sem,
):
    components, rows, cols, slots = shape
    movers = out_movers.shape[3]
    wide = cols + 2
    groups = cols // TILE
    live_slots, spare, pieces, riders, sent_rows = packing(components, slots, movers, groups)
    carried = components - riders
    has_rest = riders * pieces > carried
    order = order_of(cols)
    middle = order[2:]
    seams = (TILE - 1, TILE, cols - TILE - 1, cols - TILE)
    i = lax.axis_index("blade")
    j = lax.axis_index("span")
    has = {}
    for di in (-1, 0, 1):
        for dj in (-1, 0, 1):
            if (di, dj) != (0, 0):
                a, b = i + di, j + dj
                has[di, dj] = (a >= 0) & (a < blades) & (b >= 0) & (b < spans)
    far_up = has[1, 0] & is_far(i, blades, fars)
    far_down = has[-1, 0] & is_far(i - 1, blades, fars)
    before = rows + 1

    own_cols = slice(TILE, TILE + cols)
    own = [
        pltpu.make_async_copy(source, target, local_sem.at[n])
        for n, (source, target) in enumerate(
            (
                (parts_hbm.at[:, 0], ghost.at[:, 0, own_cols, :]),
                (count_hbm, count_own),
                (filled_hbm, filled_ref),
                (pairs_hbm, pairs_ref.at[:, 0:rows]),
                (parts_hbm.at[:, 1:rows], ghost.at[:, 1:rows, own_cols, :]),
                (out_movers_hbm, out_movers),
                (in_movers_hbm, in_movers),
                (move_count_hbm, move_count),
            )
        )
    ]
    barrier = pltpu.get_barrier_semaphore()
    expected = jnp.int32(0)
    for (di, dj), there in has.items():
        expected = expected + there.astype(jnp.int32)

        @pl.when(there)
        def _(di=di, dj=dj):
            pl.semaphore_signal(
                barrier, inc=1, device_id=(i + di, j + dj), device_id_type=MESH
            )

    for copy in own:
        copy.start()

    moves = {}

    def move(name, source, target, di, dj, far=None):
        n = len(moves)
        copy = pltpu.make_async_remote_copy(
            src_ref=source,
            dst_ref=target,
            send_sem=send_sem.at[n],
            recv_sem=recv_sem.at[n],
            device_id=(i + di, j + dj),
            device_id_type=MESH,
        )
        sends, comes = has[di, dj], has[-di, -dj]
        if far is not None:
            sends = sends & (far_up if far else ~far_up)
            comes = comes & (far_down if far else ~far_down)
        moves[name] = (copy, sends, comes)

    low = slice(0, 1)
    high = slice(cols - 1, cols)
    left = slice(TILE - 1, TILE)
    right = slice(TILE + cols, TILE + cols + 1)
    for g in order:
        a, b = ghost_chunk(g, cols)
        target = ghost.at[0:carried, rows, TILE + a : TILE + b, :]
        move(("ghost", g), packed.at[:, a:b], target, -1, 0)
    move("corner right", parts_hbm.at[:, 0, low, :], ghost.at[:, rows, right, :], -1, -1)
    move("corner left", parts_hbm.at[:, 0, high, :], ghost.at[:, rows, left, :], -1, 1)
    move("side right", parts_hbm.at[:, :, low, :], ghost.at[:, 0:rows, right, :], 0, -1)
    move("side left", parts_hbm.at[:, :, high, :], ghost.at[:, 0:rows, left, :], 0, 1)
    move("edge low", edge_out.at[1], owed_low, 0, 1)
    move("edge high", edge_out.at[0], owed_high, 0, -1)
    move("late low", totals.at[rows, wide - 1], late_low, 0, 1)
    move("late high", totals.at[rows, 0], late_high, 0, -1)
    for g in order:
        a, b = owed_chunk(g, cols)
        mode = False if g in middle else None
        source, target = totals.at[rows, 1 + a : 1 + b, 0:sent_rows], owed.at[a:b, 0:sent_rows]
        move(("owed", g), source, target, 1, 0, mode)
    move("diag low", totals.at[rows, wide - 1], owed_diag.at[0], 1, 1)
    move("diag high", totals.at[rows, 0], owed_diag.at[1], 1, -1)
    move("seams", seam_out, seam_in, 1, 0, True)
    move("rest", rest_out.at[0], rest_in.at[0], -1, 0)
    move("far rest", rest_out.at[1], rest_in.at[1], 1, 0, True)
    inner_cols = slice(TILE, cols - TILE)
    target = pairs_ref.at[:, rows, inner_cols]
    move("far pairs", pairs_hbm.at[:, rows - 1, inner_cols], target, 1, 0, True)
    move("far count", count_hbm, count_prev, 1, 0, True)
    for g in middle:
        a, b = g * TILE, (g + 1) * TILE
        target = ghost.at[0:carried, before, TILE + a : TILE + b, :]
        move(("far", g), packed_last.at[:, a:b], target, 1, 0, True)
    move("forward", msg_out.at[0], msg_in.at[0], 1, 0)
    move("backward", msg_out.at[1], msg_in.at[1], -1, 0)

    def start(*which):
        for w in which:
            copy, sends, comes = moves[w]

            @pl.when(sends)
            def _(copy=copy):
                copy.start()

    def arrive(*which):
        for w in which:
            copy, sends, comes = moves[w]

            @pl.when(comes)
            def _(copy=copy):
                copy.wait_recv()

    def sent(*which):
        for w in which:
            copy, sends, comes = moves[w]

            @pl.when(sends)
            def _(copy=copy):
                copy.wait_send()

    diagonal = lax.broadcasted_iota(jnp.int32, (cols, cols), 0) == lax.broadcasted_iota(
        jnp.int32, (cols, cols), 1
    )
    lane = lax.broadcasted_iota(jnp.int32, (TILE, slots), 1)
    lane_f = lane.astype(jnp.float32)
    slot_ids = lax.broadcasted_iota(jnp.int32, (slots, slots), 0)
    line_lane = lax.broadcasted_iota(jnp.int32, (1, slots), 1)
    cell_ids = lax.broadcasted_iota(jnp.int32, (cols, slots), 0)
    lane_ids = lax.broadcasted_iota(jnp.int32, (cols, slots), 1)

    def spread(source, r, target, at):
        line = jnp.broadcast_to(source[r : r + 1, :].astype(jnp.float32), (cols, cols))
        column = jnp.sum(jnp.where(diagonal, line, 0.0), axis=1, keepdims=True)
        target[at] = jnp.broadcast_to(column, (cols, slots))

    def clear(n, _):
        for r in range(rows + 2):
            totals[r, n] = jnp.zeros((8, slots), jnp.float32)
        return 0

    def pack(r, target):
        for c in range(carried):
            value = ghost[c, r, own_cols, :]
            if c < riders * pieces and c < carried:
                rider, piece = carried + c // pieces, c % pieces
                shift = live_slots - piece * spare
                moved = pltpu.roll(ghost[rider, r, own_cols, :], shift, 1)
                value = jnp.where(lane_ids < live_slots, value, moved)
            target[c] = value
        if has_rest:
            which = 0 if r == 0 else 1
            value = None
            for k in range(groups):
                piece = ghost[components - 1, r, TILE + k * TILE : 2 * TILE + k * TILE, :]
                moved = pltpu.roll(piece, (k * spare - (pieces - 1) * spare) % slots, 1)
                value = moved if k == 0 else jnp.where(lane >= k * spare, moved, value)
            rest_out[which] = value

    def expand(which):
        for k in range(groups):
            shift = ((pieces - 1) * spare - k * spare) % slots
            rest[which, k * TILE : (k + 1) * TILE] = pltpu.roll(rest_in[which], shift, 1)

    def unpack(r, at):
        for e in range(riders):
            value = None
            for piece in range(pieces):
                shift = (piece * spare - live_slots) % slots
                if e * pieces + piece < carried:
                    tile = ghost[e * pieces + piece, r, TILE + at : 2 * TILE + at, :]
                    moved = pltpu.roll(tile, shift, 1)
                else:
                    moved = rest[0 if r == rows else 1, at : at + TILE]
                value = moved if piece == 0 else jnp.where(lane >= piece * spare, moved, value)
            ghost[carried + e, r, TILE + at : 2 * TILE + at, :] = value

    def load_heat(g):
        if sent_rows == 8:
            return
        a, b = owed_chunk(g, cols)
        for first in {a, b - TILE} if b - a >= TILE else {a}:
            n = min(TILE, b - a)
            cells = slice(1 + first, 1 + first + n)
            heat = totals[rows, cells, 6, :]
            spot = lax.broadcasted_iota(jnp.int32, (n, slots), 1) < live_slots
            for piece in range(pieces):
                moved = pltpu.roll(heat, live_slots - piece * spare, 1)
                totals[rows, cells, piece, :] = jnp.where(spot, totals[rows, cells, piece, :], moved)

    def owed_sum(c, cells):
        if c < 6 or sent_rows == 8:
            return owed[cells, c, :]
        value = None
        for piece in range(pieces):
            moved = pltpu.roll(owed[cells, piece, :], (piece * spare - live_slots) % slots, 1)
            value = moved if piece == 0 else jnp.where(lane >= piece * spare, moved, value)
        return value

    def tiles_of(g):
        return g * TILE if isinstance(g, int) else pl.multiple_of(g * TILE, TILE)

    def row_of(r):
        if r == before:
            return before, rows, lambda d: 0
        return r, r, lambda d: r + row_steps[d]

    def contacts_of(r, g):
        at = tiles_of(g)
        _, listed, _ = row_of(r)
        ids = pairs_ref[0, listed, pl.ds(at, TILE), :]
        code = pairs_ref[1, listed, pl.ds(at, TILE), :]
        heading = code // slots
        return ids, heading, code - heading * slots

    def forces(r, g, headings):
        at = tiles_of(g)
        near, listed, far_row = row_of(r)
        ids, heading, target = contacts_of(r, g)
        live = lane_f < count_wide[listed, pl.ds(at, TILE), :]
        if len(headings) < len(row_steps):
            among = heading == headings[0]
            for d in headings[1:]:
                among = among | (heading == d)
            live = live & among
        first = [
            lanes_of(ghost[c, near, pl.ds(at + TILE, TILE), :], ids) for c in range(components)
        ]
        second = [None] * components
        for n, d in enumerate(headings):
            pick = heading == d
            for c in range(components):
                rows_at = pl.ds(at + TILE + col_steps[d], TILE)
                value = lanes_of(ghost[c, far_row(d), rows_at, :], target)
                second[c] = value if n == 0 else jnp.where(pick, value, second[c])
        row_shift = jnp.where((heading == 0) | (heading == 2), 0.0, 1.0)
        col_shift = jnp.where(
            (heading == 2) | (heading == 3), 1.0, jnp.where(heading == 4, -1.0, 0.0)
        )
        on_first, on_second = pair_terms(first, second, row_shift, col_shift, live)
        zero = jnp.zeros((TILE, slots), jnp.float32)
        base = (listed * cols + g * TILE) * 8
        for c, (a, b) in enumerate(zip(on_first + [zero], on_second + [zero])):
            first_terms[pl.ds(base + c, TILE, stride=8), :] = a
            second_terms[pl.ds(base + c, TILE, stride=8), :] = b

    def scatter(r, g, headings):
        near, listed, far_row = row_of(r)
        ids, heading, target = contacts_of(r, g)
        shared = 0 in headings
        zero = jnp.zeros((8, slots), jnp.float32)
        for n in range(TILE):
            base = (listed * cols + g * TILE + n) * 8
            if not isinstance(base, int):
                base = pl.multiple_of(base, 8)
            a = first_terms[pl.ds(base, 8), :]
            b = second_terms[pl.ds(base, 8), :]
            head = heading[n : n + 1]
            blocks = [jnp.where(head == d, b, 0.0) for d in headings]
            if not shared:
                blocks = [zero] + blocks
            near_blocks = [a] + [zero] * (len(blocks) - 1)
            terms = jnp.concatenate(
                [jnp.concatenate(near_blocks, axis=0), jnp.concatenate(blocks, axis=0)], axis=1
            )
            near_hot = jnp.where(slot_ids == ids[n : n + 1], 1.0, 0.0)
            hot = jnp.where(slot_ids == target[n : n + 1], 1.0, 0.0)
            hot = jnp.concatenate([near_hot, hot], axis=1)
            coarse = terms.astype(jnp.bfloat16).astype(jnp.float32)
            split = jnp.concatenate([coarse, terms - coarse], axis=0).astype(jnp.bfloat16)
            summed = lax.dot_general(
                split,
                hot.astype(jnp.bfloat16),
                (((1,), (1,)), ((), ())),
                preferred_element_type=jnp.float32,
            )
            count = len(blocks) * 8
            summed = summed[:count] + summed[count:]
            places = [(far_row(d), col_steps[d]) for d in headings]
            if not shared:
                places = [(near, 0)] + places
            for m, (row, shift) in enumerate(places):
                totals[row, g * TILE + n + 1 + shift] += summed[m * 8 : m * 8 + 8]

    every, inside, across = (0, 1, 2, 3, 4), (0, 2), (1, 3, 4)

    def group_of(r, g, headings):
        forces(r, g, headings)
        scatter(r, g, headings)

    def step(state, sums, live):
        safe = jnp.where(live, state[9], 1.0)
        mass = density * safe * safe * safe
        inverse = 1.0 / mass
        spin_inverse = 1.0 / (0.4 * mass * safe * safe)
        new = [None] * components
        for c in range(3):
            accel = sums[c] * inverse
            if c == 2:
                accel = accel - gravity
            speed = state[3 + c] + timestep_length * accel
            new[c] = state[c] + timestep_length * speed
            new[3 + c] = speed
            new[6 + c] = state[6 + c] + timestep_length * sums[3 + c] * spin_inverse
        new[9] = state[9]
        new[10] = state[10] + timestep_length * sums[6] * inverse
        return [jnp.where(live, v, 0.0) for v in new]

    def step_group(r, g, left=None):
        cells = slice(g * TILE, (g + 1) * TILE)
        sums = [totals[r, 1 + g * TILE : 1 + (g + 1) * TILE, c, :] for c in range(7)]
        if r == 0:
            sums = [
                v + jnp.where(has[-1, 0], owed_sum(c, cells), 0.0) for c, v in enumerate(sums)
            ]
        live = lane_f < filled_wide[r, cells, :]
        state = [ghost[c, r, TILE + g * TILE : 2 * TILE + g * TILE, :] for c in range(components)]
        if left is not None:
            live = live & ~left[cells]
        for c, value in enumerate(step(state, sums, live)):
            out_ref[c, r, cells, :] = value

    def list_of(direction, r):
        cell_line = jnp.full((1, slots), -1, jnp.int32)
        slot_line = jnp.zeros((1, slots), jnp.int32)
        for k in range(movers):
            cell_line = jnp.where(line_lane == k, out_movers[direction, 0, 0, k] - r * cols, cell_line)
            slot_line = jnp.where(line_lane == k, out_movers[direction, 1, 0, k], slot_line)
        cell_line = jnp.where(line_lane < move_count[0, 0, direction], cell_line, -1)
        return cell_line, slot_line

    def chosen_of(cell_line, slot_line):
        chosen = cell_ids == cell_line
        slot_f = jnp.where(chosen, jnp.broadcast_to(slot_line + 1, (cols, slots)).astype(jnp.float32), 0.0)
        slot_of = jnp.sum(slot_f, axis=1, keepdims=True).astype(jnp.int32) - 1
        slot_of = jnp.broadcast_to(slot_of, (cols, slots))
        index = jnp.maximum(slot_of, 0)

        def line_of(value):
            return jnp.sum(jnp.where(chosen, lanes_of(value, index), 0.0), axis=0, keepdims=True)

        return line_of, lane_ids == slot_of

    def landing_of(direction, r):
        key = jnp.zeros((1, slots), jnp.int32)
        cell_line = jnp.full((1, slots), -1, jnp.int32)
        for k in range(movers):
            hit = line_lane == in_movers[direction, 1, 0, k]
            key = jnp.where(hit, k, key)
            cell_line = jnp.where(hit, in_movers[direction, 0, 0, k] - r * cols, cell_line)
        return key, cell_line

    def put(r, there, message, lists):
        key, cell_line = lists
        landing = cell_ids == jnp.where(there, cell_line, -1)
        values = lanes_of(message, jnp.broadcast_to(key, message.shape))
        for c in range(components):
            out_ref[c, r] = jnp.where(landing, values[c : c + 1], out_ref[c, r])

    def finish(direction, message, row, extra, state_of):
        cells_new = message[7:8].astype(jnp.int32)
        lines_new, _ = chosen_of(cells_new, message[8:9].astype(jnp.int32))
        sums = [
            lines_new(extra(c, totals[row, 1 : 1 + cols, c, :])) + message[c : c + 1]
            for c in range(7)
        ]
        state = [state_of(c, lines_new) for c in range(components)]
        moving = cells_new >= 0
        for c, value in enumerate(step(state, sums, moving)):
            if c == 0:
                value = value + jnp.where(moving, -1.0 if direction == 0 else 1.0, 0.0)
            landed[direction, c : c + 1, :] = value

    def share_of(direction, r, lines, cells_line, slots_line):
        for c in range(7):
            msg_out[direction, c : c + 1, :] = lines(totals[r, 1 : 1 + cols, c, :])
        msg_out[direction, 7:8, :] = cells_line.astype(jnp.float32)
        msg_out[direction, 8:9, :] = slots_line.astype(jnp.float32)

    last = rows - 1
    lax.fori_loop(0, wide, clear, 0)
    msg_out[...] = jnp.zeros(msg_out.shape, jnp.float32)
    landed[...] = jnp.zeros(landed.shape, jnp.float32)
    own[0].wait()
    pack(0, packed)
    own[4].wait()

    @pl.when(far_up)
    def _():
        pack(last, packed_last)

    pl.semaphore_wait(barrier, expected)
    rest_out_used = ("rest",) if has_rest else ()
    start(*rest_out_used, ("ghost", 0), "corner left", ("ghost", groups - 1), "corner right", "side right", "side left")

    @pl.when(~far_down)
    def _():
        start(*(("ghost", g) for g in middle))

    far_rest_used = ("far rest",) if has_rest else ()
    start("far pairs", "far count", *far_rest_used)
    for n, copy in enumerate(own):
        if n not in (0, 4):
            copy.wait()
    for r in range(rows):
        spread(count_own, r, count_wide, r)
        spread(filled_ref, r, filled_wide, r)

    def early(g):
        for r in range(last):
            group_of(r, g, every)
        group_of(last, g, inside)

    def inner(n, _):
        early(n)
        return 0

    def outer(n, _):
        early((groups - 1) * n)
        return 0

    lax.fori_loop(1, groups - 1, inner, 0)
    arrive("side right", "side left")
    lax.fori_loop(0, 1, outer, 0)

    @pl.when(far_down)
    def _():
        start(*(("ghost", g) for g in middle))

    lax.fori_loop(1, 2, outer, 0)
    for r in range(rows):
        edge_out[0, r] = totals[r, 0]
        edge_out[1, r] = totals[r, wide - 1]
    start("edge low", "edge high")
    cells_back, slots_back = list_of(1, 0)
    lines_back, left_back = chosen_of(cells_back, slots_back)
    cells_on, slots_on = list_of(0, last)
    lines_on, left_on = chosen_of(cells_on, slots_on)
    arrive("edge low", "edge high")
    for r in range(rows):
        totals[r, 1] += jnp.where(has[0, -1], owed_low[r], 0.0)
        totals[r, cols] += jnp.where(has[0, 1], owed_high[r], 0.0)
    share_of(1, 0, lines_back, cells_back, slots_back)
    start("backward")
    start(*(("far", g) for g in middle))
    lists_first, lists_last = landing_of(0, 0), landing_of(1, last)

    @pl.when(far_up)
    def _():
        msg_out[0, 7:8, :] = cells_on.astype(jnp.float32)
        msg_out[0, 8:9, :] = slots_on.astype(jnp.float32)
        for c in range(components):
            msg_out[0, 9 + c : 10 + c, :] = lines_on(ghost[c, last, own_cols, :])

    @pl.when(far_down)
    def _():
        for n in range(TILE - 1, cols - TILE + 1):
            owed[n] = jnp.zeros((8, slots), jnp.float32)

    for r in range(1, last):
        for g in range(groups):
            step_group(r, g)

    def last_group(g):
        arrive(("ghost", g))
        if g == 0:
            if has_rest:
                arrive("rest")
                expand(0)
            unpack(rows, 0)
            unpack(rows, 1)
            arrive("corner left")
        elif g == groups - 1:
            unpack(rows, cols - TILE - 1)
            unpack(rows, cols - TILE)
            arrive("corner right")
        else:
            unpack(rows, g * TILE + 1)
        group_of(last, g, across)
        load_heat(g)
        start(("owed", g))

    last_group(0)
    start("late high", "diag high")
    last_group(groups - 1)
    start("late low", "diag low")

    @pl.when(far_up)
    def _():
        for n, col in enumerate(seams):
            seam_out[n] = totals[rows, 1 + col]
        start("seams")
        for c in range(7):
            msg_out[0, c : c + 1, :] = lines_on(totals[last, 1 : 1 + cols, c, :])
        start("forward")

    for g in middle:
        last_group(g)
    for g in range(groups):
        step_group(last, g)

    @pl.when(has[1, 0] & ~far_up)
    def _():
        for c in range(components):
            line = lines_on(out_ref[c, last])
            if c == 0:
                line = line - jnp.where(cells_on >= 0, 1.0, 0.0)
            msg_out[0, c : c + 1, :] = line
        start("forward")

    for c in range(components):
        out_ref[c, last] = jnp.where(left_on, 0.0, out_ref[c, last])

    def late_edges(c, value):
        value = value + jnp.where((cell_ids == 0) & has[0, -1], late_low[c : c + 1, :], 0.0)
        return value + jnp.where((cell_ids == cols - 1) & has[0, 1], late_high[c : c + 1, :], 0.0)

    arrive("late low", "late high", "backward")

    @pl.when(has[1, 0])
    def _():
        finish(1, msg_in[1], rows, late_edges, lambda c, lines: lines(ghost[c, rows, own_cols, :]))
        put(last, has[1, 0], landed[1], lists_last)

    sent(*(w for w in moves if has_rest or w not in ("rest", "far rest")))

    def add_diagonals():
        totals[0, 1] += jnp.where(has[-1, -1], owed_diag[0], 0.0)
        totals[0, cols] += jnp.where(has[-1, 1], owed_diag[1], 0.0)

    @pl.when(far_down)
    def _():
        arrive("far count", "far pairs", *far_rest_used)
        if has_rest:
            expand(1)
        spread(count_prev, last, count_wide, rows)
        for g in middle:
            arrive(("far", g))
            unpack(before, g * TILE)
            group_of(before, g, across)
        arrive(("owed", 0), ("owed", groups - 1), "seams", "diag low", "diag high")
        add_diagonals()
        for n, col in enumerate(seams):
            totals[0, 1 + col] += seam_in[n]
        for g in range(groups):
            step_group(0, g, left_back)
        arrive("forward")
        message = msg_in[0]
        finish(0, message, before, lambda c, value: value, lambda c, _: message[9 + c : 10 + c])

    @pl.when(~far_down)
    def _():
        arrive(("owed", 0), ("owed", groups - 1), "diag low", "diag high")
        add_diagonals()
        for k, g in enumerate(order):
            if k > 1:
                arrive(("owed", g))
            if k > 1:
                step_group(0, g - 1, left_back)
        step_group(0, groups - 2, left_back)
        step_group(0, groups - 1, left_back)
        arrive("forward")
        landed[0, 0:components, :] = msg_in[0, 0:components, :]

    put(0, has[-1, 0], landed[0], lists_first)


def body(blades, spans, fars, particles, filled, contact_pairs, contact_count, movers_out, movers_in, move_count):
    components, rows, cols, slots = particles.shape
    padded = -(-components // 8) * 8
    message = -(-(components + 9) // 8) * 8
    f32, i32 = jnp.float32, jnp.int32
    riders = packing(components, slots, movers_out.shape[3], cols // TILE)[3]
    remote_copies = 3 * (cols // TILE) + 15
    return pl.pallas_call(
        functools.partial(kernel, particles.shape, blades, spans, fars),
        out_shape=pltpu.VMEM(particles.shape, f32),
        in_specs=[pl.BlockSpec(memory_space=pl.ANY)] * 7,
        out_specs=pl.BlockSpec(memory_space=pltpu.VMEM),
        scratch_shapes=[
            pltpu.VMEM((components, rows + 2, cols + 2 * TILE, slots), f32),
            pltpu.VMEM((components - riders, cols, slots), f32),
            pltpu.VMEM((components - riders, cols, slots), f32),
            pltpu.VMEM((2, TILE, slots), f32),
            pltpu.VMEM((2, TILE, slots), f32),
            pltpu.VMEM((2, cols, slots), f32),
            pltpu.VMEM((2, rows + 1, cols, contact_pairs.shape[3]), i32),
            pltpu.VMEM((rows, cols), i32),
            pltpu.VMEM((rows, cols), i32),
            pltpu.VMEM((rows, cols), i32),
            pltpu.SMEM(movers_out.shape, i32),
            pltpu.SMEM(movers_in.shape, i32),
            pltpu.SMEM((1, 1, 2), i32),
            pltpu.VMEM(((rows + 1) * cols * 8, slots), f32),
            pltpu.VMEM(((rows + 1) * cols * 8, slots), f32),
            pltpu.VMEM((rows + 1, cols, slots), f32),
            pltpu.VMEM((rows, cols, slots), f32),
            pltpu.VMEM((rows + 2, cols + 2, 8, slots), f32),
            pltpu.VMEM((2, rows, 8, slots), f32),
            pltpu.VMEM((rows, 8, slots), f32),
            pltpu.VMEM((rows, 8, slots), f32),
            pltpu.VMEM((8, slots), f32),
            pltpu.VMEM((8, slots), f32),
            pltpu.VMEM((4, 8, slots), f32),
            pltpu.VMEM((4, 8, slots), f32),
            pltpu.VMEM((cols, 8, slots), f32),
            pltpu.VMEM((2, 8, slots), f32),
            pltpu.VMEM((2, message, slots), f32),
            pltpu.VMEM((2, message, slots), f32),
            pltpu.VMEM((2, padded, slots), f32),
            pltpu.SemaphoreType.DMA((8,)),
            pltpu.SemaphoreType.DMA((remote_copies,)),
            pltpu.SemaphoreType.DMA((remote_copies,)),
        ],
        compiler_params=pltpu.CompilerParams(
            collective_id=0, has_side_effects=True, vmem_limit_bytes=VMEM_GRANT
        ),
    )(
        *(
            pltpu.with_memory_space_constraint(x, pltpu.HBM)
            for x in (
                particles,
                filled,
                contact_pairs,
                contact_count,
                movers_out,
                movers_in,
                jnp.transpose(move_count, (1, 2, 0)),
            )
        )
    )


def solution(mesh):
    sizes = dict(mesh.shape)
    return jax.shard_map(
        functools.partial(body, sizes["blade"], sizes["span"], far_boundaries(mesh)),
        mesh=mesh,
        in_specs=(
            P(None, "blade", "span", None),
            P("blade", "span"),
            P(None, "blade", "span", None),
            P("blade", "span"),
            P(None, None, "blade", "span"),
            P(None, None, "blade", "span"),
            P(None, "blade", "span"),
        ),
        out_specs=P(None, "blade", "span", None),
        check_vma=False,
    )
```

```python
import functools

import jax
import jax.numpy as jnp
from jax import lax
from jax.experimental import pallas as pl
from jax.experimental.pallas import tpu as pltpu
from jax.sharding import PartitionSpec as P

spring = 4.0
normal_damp = 0.5
tangent_damp = 0.3
conduct = 40.0
timestep_length = 0.05
density = 100.0
gravity = 9.81
soft_len = 0.05
row_steps = (0, 1, 0, 1, 1)
col_steps = (0, 0, 1, 1, -1)
MESH = pl.DeviceIdType.MESH
TILE = 8
VMEM_GRANT = 16 << 20


def cross(a, b):
    return (
        a[1] * b[2] - a[2] * b[1],
        a[2] * b[0] - a[0] * b[2],
        a[0] * b[1] - a[1] * b[0],
    )


def lanes_of(table, index):
    return jnp.take_along_axis(table, index, axis=1, mode="promise_in_bounds")


def pair_terms(first, second, row_shift, col_shift, live):
    gap = (
        second[0] + row_shift - first[0],
        second[1] + col_shift - first[1],
        second[2] - first[2],
    )
    distance = jnp.sqrt(gap[0] * gap[0] + gap[1] * gap[1] + gap[2] * gap[2] + soft_len * soft_len)
    inverse = 1.0 / distance
    normal = tuple(g * inverse for g in gap)
    rad_first, rad_second = first[9], second[9]
    intersection = rad_first + rad_second - distance
    spin = tuple(rad_first * first[6 + c] + rad_second * second[6 + c] for c in range(3))
    turn = cross(spin, normal)
    relative = tuple(second[3 + c] - first[3 + c] - turn[c] for c in range(3))
    speed = relative[0] * normal[0] + relative[1] * normal[1] + relative[2] * normal[2]
    friction = tuple(tangent_damp * (relative[c] - speed * normal[c]) for c in range(3))
    push = normal_damp * speed - spring * intersection
    force = tuple(push * normal[c] + friction[c] for c in range(3))
    torque = cross(normal, friction)
    denom = jnp.where(live, rad_first + rad_second, 1.0)
    heat = 2.0 * conduct * rad_first * rad_second / denom * (second[10] - first[10])
    on_first = force + tuple(rad_first * t for t in torque) + (heat,)
    on_second = tuple(-f for f in force) + tuple(rad_second * t for t in torque) + (-heat,)
    keep = lambda v: jnp.where(live, v, 0.0)
    return [keep(v) for v in on_first], [keep(v) for v in on_second]


def order_of(cols):
    groups = cols // TILE
    return [0, groups - 1, *range(1, groups - 1)]


def ghost_chunk(g, cols):
    groups = cols // TILE
    if g == 0:
        return 0, TILE + 1
    if g == groups - 1:
        return cols - TILE - 1, cols
    return g * TILE + 1, min((g + 1) * TILE + 1, cols - TILE - 1)


def owed_chunk(g, cols):
    groups = cols // TILE
    if g == 0:
        return 0, TILE - 1
    if g == groups - 1:
        return cols - TILE + 1, cols
    return g * TILE - 1, ((g + 1) * TILE - 1 if g < groups - 2 else cols - TILE + 1)


def packing(components, slots, movers, groups):
    live = slots - 2 * movers
    spare = slots - live
    pieces = live // spare
    riders = components // (pieces + 1) if live % spare == 0 else 0
    extra = (riders + 1) * pieces - (components - riders - 1)
    if riders and extra == 1 and spare * groups <= slots:
        riders += 1
    sent_rows = 6 if live % spare == 0 and pieces <= 6 else 8
    return live, spare, pieces, riders, sent_rows


def far_boundaries(mesh):
    line = mesh.devices.reshape(mesh.devices.shape[0], -1)[:, 0]
    hops = [
        sum(abs(p - q) for p, q in zip(a.coords, b.coords)) for a, b in zip(line, line[1:])
    ]
    most = max(hops, default=0)
    if most == min(hops, default=0):
        return ()
    return tuple(n for n, h in enumerate(hops) if h >= most)


def is_far(boundary, blades, fars):
    for period in range(1, blades):
        if fars == tuple(range(period - 1, blades - 1, period)):
            return lax.rem(boundary + period, period) == period - 1
    far = boundary < -1
    for f in fars:
        far = far | (boundary == f)
    return far


def kernel(
    shape,
    blades,
    spans,
    fars,
    parts_hbm,
    filled_hbm,
    pairs_hbm,
    count_hbm,
    out_movers_hbm,
    in_movers_hbm,
    move_count_hbm,
    out_ref,
    ghost,
    packed,
    packed_last,
    rest_out,
    rest_in,
    rest,
    pairs_ref,
    count_own,
    count_prev,
    filled_ref,
    out_movers,
    in_movers,
    move_count,
    first_terms,
    second_terms,
    count_wide,
    filled_wide,
    totals,
    edge_out,
    owed_low,
    owed_high,
    late_low,
    late_high,
    seam_out,
    seam_in,
    owed,
    owed_diag,
    msg_out,
    msg_in,
    landed,
    local_sem,
    send_sem,
    recv_sem,
):
    components, rows, cols, slots = shape
    movers = out_movers.shape[3]
    wide = cols + 2
    groups = cols // TILE
    live_slots, spare, pieces, riders, sent_rows = packing(components, slots, movers, groups)
    carried = components - riders
    has_rest = riders * pieces > carried
    order = order_of(cols)
    middle = order[2:]
    seams = (TILE - 1, TILE, cols - TILE - 1, cols - TILE)
    i = lax.axis_index("blade")
    j = lax.axis_index("span")
    has = {}
    for di in (-1, 0, 1):
        for dj in (-1, 0, 1):
            if (di, dj) != (0, 0):
                a, b = i + di, j + dj
                has[di, dj] = (a >= 0) & (a < blades) & (b >= 0) & (b < spans)
    far_up = has[1, 0] & is_far(i, blades, fars)
    far_down = has[-1, 0] & is_far(i - 1, blades, fars)
    before = rows + 1

    own_cols = slice(TILE, TILE + cols)
    own = [
        pltpu.make_async_copy(source, target, local_sem.at[n])
        for n, (source, target) in enumerate(
            (
                (parts_hbm.at[:, 0], ghost.at[:, 0, own_cols, :]),
                (count_hbm, count_own),
                (filled_hbm, filled_ref),
                (pairs_hbm, pairs_ref.at[:, 0:rows]),
                (parts_hbm.at[:, 1:rows], ghost.at[:, 1:rows, own_cols, :]),
                (out_movers_hbm, out_movers),
                (in_movers_hbm, in_movers),
                (move_count_hbm, move_count),
            )
        )
    ]
    barrier = pltpu.get_barrier_semaphore()
    expected = jnp.int32(0)
    for (di, dj), there in has.items():
        expected = expected + there.astype(jnp.int32)

        @pl.when(there)
        def _(di=di, dj=dj):
            pl.semaphore_signal(
                barrier, inc=1, device_id=(i + di, j + dj), device_id_type=MESH
            )

    for copy in own:
        copy.start()

    moves = {}

    def move(name, source, target, di, dj, far=None):
        n = len(moves)
        copy = pltpu.make_async_remote_copy(
            src_ref=source,
            dst_ref=target,
            send_sem=send_sem.at[n],
            recv_sem=recv_sem.at[n],
            device_id=(i + di, j + dj),
            device_id_type=MESH,
        )
        sends, comes = has[di, dj], has[-di, -dj]
        if far is not None:
            sends = sends & (far_up if far else ~far_up)
            comes = comes & (far_down if far else ~far_down)
        moves[name] = (copy, sends, comes)

    low = slice(0, 1)
    high = slice(cols - 1, cols)
    left = slice(TILE - 1, TILE)
    right = slice(TILE + cols, TILE + cols + 1)
    for g in order:
        a, b = ghost_chunk(g, cols)
        target = ghost.at[0:carried, rows, TILE + a : TILE + b, :]
        move(("ghost", g), packed.at[:, a:b], target, -1, 0)
    move("corner right", parts_hbm.at[:, 0, low, :], ghost.at[:, rows, right, :], -1, -1)
    move("corner left", parts_hbm.at[:, 0, high, :], ghost.at[:, rows, left, :], -1, 1)
    move("side right", parts_hbm.at[:, :, low, :], ghost.at[:, 0:rows, right, :], 0, -1)
    move("side left", parts_hbm.at[:, :, high, :], ghost.at[:, 0:rows, left, :], 0, 1)
    move("edge low", edge_out.at[1], owed_low, 0, 1)
    move("edge high", edge_out.at[0], owed_high, 0, -1)
    move("late low", totals.at[rows, wide - 1], late_low, 0, 1)
    move("late high", totals.at[rows, 0], late_high, 0, -1)
    for g in order:
        a, b = owed_chunk(g, cols)
        mode = False if g in middle else None
        source, target = totals.at[rows, 1 + a : 1 + b, 0:sent_rows], owed.at[a:b, 0:sent_rows]
        move(("owed", g), source, target, 1, 0, mode)
    move("diag low", totals.at[rows, wide - 1], owed_diag.at[0], 1, 1)
    move("diag high", totals.at[rows, 0], owed_diag.at[1], 1, -1)
    move("seams", seam_out, seam_in, 1, 0, True)
    move("rest", rest_out.at[0], rest_in.at[0], -1, 0)
    move("far rest", rest_out.at[1], rest_in.at[1], 1, 0, True)
    inner_cols = slice(TILE, cols - TILE)
    target = pairs_ref.at[:, rows, inner_cols]
    move("far pairs", pairs_hbm.at[:, rows - 1, inner_cols], target, 1, 0, True)
    move("far count", count_hbm, count_prev, 1, 0, True)
    for g in middle:
        a, b = g * TILE, (g + 1) * TILE
        target = ghost.at[0:carried, before, TILE + a : TILE + b, :]
        move(("far", g), packed_last.at[:, a:b], target, 1, 0, True)
    move("forward", msg_out.at[0], msg_in.at[0], 1, 0)
    move("backward", msg_out.at[1], msg_in.at[1], -1, 0)

    def start(*which):
        for w in which:
            copy, sends, comes = moves[w]

            @pl.when(sends)
            def _(copy=copy):
                copy.start()

    def arrive(*which):
        for w in which:
            copy, sends, comes = moves[w]

            @pl.when(comes)
            def _(copy=copy):
                copy.wait_recv()

    def sent(*which):
        for w in which:
            copy, sends, comes = moves[w]

            @pl.when(sends)
            def _(copy=copy):
                copy.wait_send()

    diagonal = lax.broadcasted_iota(jnp.int32, (cols, cols), 0) == lax.broadcasted_iota(
        jnp.int32, (cols, cols), 1
    )
    lane = lax.broadcasted_iota(jnp.int32, (TILE, slots), 1)
    lane_f = lane.astype(jnp.float32)
    slot_ids = lax.broadcasted_iota(jnp.int32, (slots, slots), 0)
    line_lane = lax.broadcasted_iota(jnp.int32, (1, slots), 1)
    cell_ids = lax.broadcasted_iota(jnp.int32, (cols, slots), 0)
    lane_ids = lax.broadcasted_iota(jnp.int32, (cols, slots), 1)

    def spread(source, r, target, at):
        line = jnp.broadcast_to(source[r : r + 1, :].astype(jnp.float32), (cols, cols))
        column = jnp.sum(jnp.where(diagonal, line, 0.0), axis=1, keepdims=True)
        target[at] = jnp.broadcast_to(column, (cols, slots))

    def clear(n, _):
        for r in range(rows + 2):
            totals[r, n] = jnp.zeros((8, slots), jnp.float32)
        return 0

    def pack(r, target):
        for c in range(carried):
            value = ghost[c, r, own_cols, :]
            if c < riders * pieces and c < carried:
                rider, piece = carried + c // pieces, c % pieces
                shift = live_slots - piece * spare
                moved = pltpu.roll(ghost[rider, r, own_cols, :], shift, 1)
                value = jnp.where(lane_ids < live_slots, value, moved)
            target[c] = value
        if has_rest:
            which = 0 if r == 0 else 1
            value = None
            for k in range(groups):
                piece = ghost[components - 1, r, TILE + k * TILE : 2 * TILE + k * TILE, :]
                moved = pltpu.roll(piece, (k * spare - (pieces - 1) * spare) % slots, 1)
                value = moved if k == 0 else jnp.where(lane >= k * spare, moved, value)
            rest_out[which] = value

    def expand(which):
        for k in range(groups):
            shift = ((pieces - 1) * spare - k * spare) % slots
            rest[which, k * TILE : (k + 1) * TILE] = pltpu.roll(rest_in[which], shift, 1)

    def unpack(r, at):
        for e in range(riders):
            value = None
            for piece in range(pieces):
                shift = (piece * spare - live_slots) % slots
                if e * pieces + piece < carried:
                    tile = ghost[e * pieces + piece, r, TILE + at : 2 * TILE + at, :]
                    moved = pltpu.roll(tile, shift, 1)
                else:
                    moved = rest[0 if r == rows else 1, at : at + TILE]
                value = moved if piece == 0 else jnp.where(lane >= piece * spare, moved, value)
            ghost[carried + e, r, TILE + at : 2 * TILE + at, :] = value

    def load_heat(g):
        if sent_rows == 8:
            return
        a, b = owed_chunk(g, cols)
        for first in {a, b - TILE} if b - a >= TILE else {a}:
            n = min(TILE, b - a)
            cells = slice(1 + first, 1 + first + n)
            heat = totals[rows, cells, 6, :]
            spot = lax.broadcasted_iota(jnp.int32, (n, slots), 1) < live_slots
            for piece in range(pieces):
                moved = pltpu.roll(heat, live_slots - piece * spare, 1)
                totals[rows, cells, piece, :] = jnp.where(spot, totals[rows, cells, piece, :], moved)

    def owed_sum(c, cells):
        if c < 6 or sent_rows == 8:
            return owed[cells, c, :]
        value = None
        for piece in range(pieces):
            moved = pltpu.roll(owed[cells, piece, :], (piece * spare - live_slots) % slots, 1)
            value = moved if piece == 0 else jnp.where(lane >= piece * spare, moved, value)
        return value

    def tiles_of(g):
        return g * TILE if isinstance(g, int) else pl.multiple_of(g * TILE, TILE)

    def row_of(r):
        if r == before:
            return before, rows, lambda d: 0
        return r, r, lambda d: r + row_steps[d]

    def contacts_of(r, g):
        at = tiles_of(g)
        _, listed, _ = row_of(r)
        ids = pairs_ref[0, listed, pl.ds(at, TILE), :]
        code = pairs_ref[1, listed, pl.ds(at, TILE), :]
        heading = code // slots
        return ids, heading, code - heading * slots

    def forces(r, g, headings):
        at = tiles_of(g)
        near, listed, far_row = row_of(r)
        ids, heading, target = contacts_of(r, g)
        live = lane_f < count_wide[listed, pl.ds(at, TILE), :]
        if len(headings) < len(row_steps):
            among = heading == headings[0]
            for d in headings[1:]:
                among = among | (heading == d)
            live = live & among
        first = [
            lanes_of(ghost[c, near, pl.ds(at + TILE, TILE), :], ids) for c in range(components)
        ]
        second = [None] * components
        for n, d in enumerate(headings):
            pick = heading == d
            for c in range(components):
                rows_at = pl.ds(at + TILE + col_steps[d], TILE)
                value = lanes_of(ghost[c, far_row(d), rows_at, :], target)
                second[c] = value if n == 0 else jnp.where(pick, value, second[c])
        row_shift = jnp.where((heading == 0) | (heading == 2), 0.0, 1.0)
        col_shift = jnp.where(
            (heading == 2) | (heading == 3), 1.0, jnp.where(heading == 4, -1.0, 0.0)
        )
        on_first, on_second = pair_terms(first, second, row_shift, col_shift, live)
        zero = jnp.zeros((TILE, slots), jnp.float32)
        base = (listed * cols + g * TILE) * 8
        for c, (a, b) in enumerate(zip(on_first + [zero], on_second + [zero])):
            first_terms[pl.ds(base + c, TILE, stride=8), :] = a
            second_terms[pl.ds(base + c, TILE, stride=8), :] = b

    def scatter(r, g, headings):
        near, listed, far_row = row_of(r)
        ids, heading, target = contacts_of(r, g)
        shared = 0 in headings
        zero = jnp.zeros((8, slots), jnp.float32)
        for n in range(TILE):
            base = (listed * cols + g * TILE + n) * 8
            if not isinstance(base, int):
                base = pl.multiple_of(base, 8)
            a = first_terms[pl.ds(base, 8), :]
            b = second_terms[pl.ds(base, 8), :]
            head = heading[n : n + 1]
            blocks = [jnp.where(head == d, b, 0.0) for d in headings]
            if not shared:
                blocks = [zero] + blocks
            near_blocks = [a] + [zero] * (len(blocks) - 1)
            terms = jnp.concatenate(
                [jnp.concatenate(near_blocks, axis=0), jnp.concatenate(blocks, axis=0)], axis=1
            )
            near_hot = jnp.where(slot_ids == ids[n : n + 1], 1.0, 0.0)
            hot = jnp.where(slot_ids == target[n : n + 1], 1.0, 0.0)
            hot = jnp.concatenate([near_hot, hot], axis=1)
            coarse = terms.astype(jnp.bfloat16).astype(jnp.float32)
            split = jnp.concatenate([coarse, terms - coarse], axis=0).astype(jnp.bfloat16)
            summed = lax.dot_general(
                split,
                hot.astype(jnp.bfloat16),
                (((1,), (1,)), ((), ())),
                preferred_element_type=jnp.float32,
            )
            count = len(blocks) * 8
            summed = summed[:count] + summed[count:]
            places = [(far_row(d), col_steps[d]) for d in headings]
            if not shared:
                places = [(near, 0)] + places
            for m, (row, shift) in enumerate(places):
                totals[row, g * TILE + n + 1 + shift] += summed[m * 8 : m * 8 + 8]

    every, inside, across = (0, 1, 2, 3, 4), (0, 2), (1, 3, 4)

    def group_of(r, g, headings):
        forces(r, g, headings)
        scatter(r, g, headings)

    def step(state, sums, live):
        safe = jnp.where(live, state[9], 1.0)
        mass = density * safe * safe * safe
        inverse = 1.0 / mass
        spin_inverse = 1.0 / (0.4 * mass * safe * safe)
        new = [None] * components
        for c in range(3):
            accel = sums[c] * inverse
            if c == 2:
                accel = accel - gravity
            speed = state[3 + c] + timestep_length * accel
            new[c] = state[c] + timestep_length * speed
            new[3 + c] = speed
            new[6 + c] = state[6 + c] + timestep_length * sums[3 + c] * spin_inverse
        new[9] = state[9]
        new[10] = state[10] + timestep_length * sums[6] * inverse
        return [jnp.where(live, v, 0.0) for v in new]

    def step_group(r, g, left=None):
        cells = slice(g * TILE, (g + 1) * TILE)
        sums = [totals[r, 1 + g * TILE : 1 + (g + 1) * TILE, c, :] for c in range(7)]
        if r == 0:
            sums = [
                v + jnp.where(has[-1, 0], owed_sum(c, cells), 0.0) for c, v in enumerate(sums)
            ]
        live = lane_f < filled_wide[r, cells, :]
        state = [ghost[c, r, TILE + g * TILE : 2 * TILE + g * TILE, :] for c in range(components)]
        if left is not None:
            live = live & ~left[cells]
        for c, value in enumerate(step(state, sums, live)):
            out_ref[c, r, cells, :] = value

    def list_of(direction, r):
        cell_line = jnp.full((1, slots), -1, jnp.int32)
        slot_line = jnp.zeros((1, slots), jnp.int32)
        for k in range(movers):
            cell_line = jnp.where(line_lane == k, out_movers[direction, 0, 0, k] - r * cols, cell_line)
            slot_line = jnp.where(line_lane == k, out_movers[direction, 1, 0, k], slot_line)
        cell_line = jnp.where(line_lane < move_count[0, 0, direction], cell_line, -1)
        return cell_line, slot_line

    def chosen_of(cell_line, slot_line):
        chosen = cell_ids == cell_line
        slot_f = jnp.where(chosen, jnp.broadcast_to(slot_line + 1, (cols, slots)).astype(jnp.float32), 0.0)
        slot_of = jnp.sum(slot_f, axis=1, keepdims=True).astype(jnp.int32) - 1
        slot_of = jnp.broadcast_to(slot_of, (cols, slots))
        index = jnp.maximum(slot_of, 0)

        def line_of(value):
            return jnp.sum(jnp.where(chosen, lanes_of(value, index), 0.0), axis=0, keepdims=True)

        return line_of, lane_ids == slot_of

    def landing_of(direction, r):
        key = jnp.zeros((1, slots), jnp.int32)
        cell_line = jnp.full((1, slots), -1, jnp.int32)
        for k in range(movers):
            hit = line_lane == in_movers[direction, 1, 0, k]
            key = jnp.where(hit, k, key)
            cell_line = jnp.where(hit, in_movers[direction, 0, 0, k] - r * cols, cell_line)
        return key, cell_line

    def put(r, there, message, lists):
        key, cell_line = lists
        landing = cell_ids == jnp.where(there, cell_line, -1)
        values = lanes_of(message, jnp.broadcast_to(key, message.shape))
        for c in range(components):
            out_ref[c, r] = jnp.where(landing, values[c : c + 1], out_ref[c, r])

    def finish(direction, message, row, extra, state_of):
        cells_new = message[7:8].astype(jnp.int32)
        lines_new, _ = chosen_of(cells_new, message[8:9].astype(jnp.int32))
        sums = [
            lines_new(extra(c, totals[row, 1 : 1 + cols, c, :])) + message[c : c + 1]
            for c in range(7)
        ]
        state = [state_of(c, lines_new) for c in range(components)]
        moving = cells_new >= 0
        for c, value in enumerate(step(state, sums, moving)):
            if c == 0:
                value = value + jnp.where(moving, -1.0 if direction == 0 else 1.0, 0.0)
            landed[direction, c : c + 1, :] = value

    def share_of(direction, r, lines, cells_line, slots_line):
        for c in range(7):
            msg_out[direction, c : c + 1, :] = lines(totals[r, 1 : 1 + cols, c, :])
        msg_out[direction, 7:8, :] = cells_line.astype(jnp.float32)
        msg_out[direction, 8:9, :] = slots_line.astype(jnp.float32)

    last = rows - 1
    lax.fori_loop(0, wide, clear, 0)
    msg_out[...] = jnp.zeros(msg_out.shape, jnp.float32)
    landed[...] = jnp.zeros(landed.shape, jnp.float32)
    own[0].wait()
    pack(0, packed)
    own[4].wait()

    @pl.when(far_up)
    def _():
        pack(last, packed_last)

    pl.semaphore_wait(barrier, expected)
    rest_out_used = ("rest",) if has_rest else ()
    start(*rest_out_used, ("ghost", 0), "corner left", ("ghost", groups - 1), "corner right", "side right", "side left")

    @pl.when(~far_down)
    def _():
        start(*(("ghost", g) for g in middle))

    far_rest_used = ("far rest",) if has_rest else ()
    start("far pairs", "far count", *far_rest_used)
    for n, copy in enumerate(own):
        if n not in (0, 4):
            copy.wait()
    for r in range(rows):
        spread(count_own, r, count_wide, r)
        spread(filled_ref, r, filled_wide, r)

    def early(g):
        for r in range(last):
            group_of(r, g, every)
        group_of(last, g, inside)

    def inner(n, _):
        early(n)
        return 0

    def outer(n, _):
        early((groups - 1) * n)
        return 0

    lax.fori_loop(1, groups - 1, inner, 0)
    arrive("side right", "side left")
    lax.fori_loop(0, 1, outer, 0)

    @pl.when(far_down)
    def _():
        start(*(("ghost", g) for g in middle))

    lax.fori_loop(1, 2, outer, 0)
    for r in range(rows):
        edge_out[0, r] = totals[r, 0]
        edge_out[1, r] = totals[r, wide - 1]
    start("edge low", "edge high")
    cells_back, slots_back = list_of(1, 0)
    lines_back, left_back = chosen_of(cells_back, slots_back)
    cells_on, slots_on = list_of(0, last)
    lines_on, left_on = chosen_of(cells_on, slots_on)
    arrive("edge low", "edge high")
    start(*(("far", g) for g in middle))
    for r in range(rows):
        totals[r, 1] += jnp.where(has[0, -1], owed_low[r], 0.0)
        totals[r, cols] += jnp.where(has[0, 1], owed_high[r], 0.0)
    share_of(1, 0, lines_back, cells_back, slots_back)
    start("backward")
    lists_first, lists_last = landing_of(0, 0), landing_of(1, last)

    @pl.when(far_up)
    def _():
        msg_out[0, 7:8, :] = cells_on.astype(jnp.float32)
        msg_out[0, 8:9, :] = slots_on.astype(jnp.float32)
        for c in range(components):
            msg_out[0, 9 + c : 10 + c, :] = lines_on(ghost[c, last, own_cols, :])

    @pl.when(far_down)
    def _():
        for n in range(TILE - 1, cols - TILE + 1):
            owed[n] = jnp.zeros((8, slots), jnp.float32)

    for r in range(1, last):
        for g in range(groups):
            step_group(r, g)

    def last_group(g):
        arrive(("ghost", g))
        if g == 0:
            if has_rest:
                arrive("rest")
                expand(0)
            unpack(rows, 0)
            unpack(rows, 1)
            arrive("corner left")
        elif g == groups - 1:
            unpack(rows, cols - TILE - 1)
            unpack(rows, cols - TILE)
            arrive("corner right")
        else:
            unpack(rows, g * TILE + 1)
        group_of(last, g, across)
        load_heat(g)
        start(("owed", g))

    last_group(0)
    start("diag high")
    last_group(groups - 1)
    start("diag low")

    @pl.when(far_up)
    def _():
        for n, col in enumerate(seams):
            seam_out[n] = totals[rows, 1 + col]
        start("seams")
        for c in range(7):
            msg_out[0, c : c + 1, :] = lines_on(totals[last, 1 : 1 + cols, c, :])
        start("forward")

    start("late low", "late high")
    for g in middle:
        last_group(g)
    for g in range(groups):
        step_group(last, g)

    @pl.when(has[1, 0] & ~far_up)
    def _():
        for c in range(components):
            line = lines_on(out_ref[c, last])
            if c == 0:
                line = line - jnp.where(cells_on >= 0, 1.0, 0.0)
            msg_out[0, c : c + 1, :] = line
        start("forward")

    for c in range(components):
        out_ref[c, last] = jnp.where(left_on, 0.0, out_ref[c, last])

    def late_edges(c, value):
        value = value + jnp.where((cell_ids == 0) & has[0, -1], late_low[c : c + 1, :], 0.0)
        return value + jnp.where((cell_ids == cols - 1) & has[0, 1], late_high[c : c + 1, :], 0.0)

    arrive("late low", "late high", "backward")

    @pl.when(has[1, 0])
    def _():
        finish(1, msg_in[1], rows, late_edges, lambda c, lines: lines(ghost[c, rows, own_cols, :]))
        put(last, has[1, 0], landed[1], lists_last)

    sent(*(w for w in moves if has_rest or w not in ("rest", "far rest")))

    def add_diagonals():
        totals[0, 1] += jnp.where(has[-1, -1], owed_diag[0], 0.0)
        totals[0, cols] += jnp.where(has[-1, 1], owed_diag[1], 0.0)

    @pl.when(far_down)
    def _():
        arrive("far count", "far pairs", *far_rest_used)
        if has_rest:
            expand(1)
        spread(count_prev, last, count_wide, rows)
        for g in middle:
            arrive(("far", g))
            unpack(before, g * TILE)
            group_of(before, g, across)
        arrive(("owed", 0), ("owed", groups - 1), "seams", "diag low", "diag high")
        add_diagonals()
        for n, col in enumerate(seams):
            totals[0, 1 + col] += seam_in[n]
        for g in range(groups):
            step_group(0, g, left_back)
        arrive("forward")
        message = msg_in[0]
        finish(0, message, before, lambda c, value: value, lambda c, _: message[9 + c : 10 + c])

    @pl.when(~far_down)
    def _():
        arrive(("owed", 0), ("owed", groups - 1), "diag low", "diag high")
        add_diagonals()
        for k, g in enumerate(order):
            if k > 1:
                arrive(("owed", g))
            if k > 1:
                step_group(0, g - 1, left_back)
        step_group(0, groups - 2, left_back)
        step_group(0, groups - 1, left_back)
        arrive("forward")
        landed[0, 0:components, :] = msg_in[0, 0:components, :]

    put(0, has[-1, 0], landed[0], lists_first)


def body(blades, spans, fars, particles, filled, contact_pairs, contact_count, movers_out, movers_in, move_count):
    components, rows, cols, slots = particles.shape
    padded = -(-components // 8) * 8
    message = -(-(components + 9) // 8) * 8
    f32, i32 = jnp.float32, jnp.int32
    riders = packing(components, slots, movers_out.shape[3], cols // TILE)[3]
    remote_copies = 3 * (cols // TILE) + 15
    return pl.pallas_call(
        functools.partial(kernel, particles.shape, blades, spans, fars),
        out_shape=pltpu.VMEM(particles.shape, f32),
        in_specs=[pl.BlockSpec(memory_space=pl.ANY)] * 7,
        out_specs=pl.BlockSpec(memory_space=pltpu.VMEM),
        scratch_shapes=[
            pltpu.VMEM((components, rows + 2, cols + 2 * TILE, slots), f32),
            pltpu.VMEM((components - riders, cols, slots), f32),
            pltpu.VMEM((components - riders, cols, slots), f32),
            pltpu.VMEM((2, TILE, slots), f32),
            pltpu.VMEM((2, TILE, slots), f32),
            pltpu.VMEM((2, cols, slots), f32),
            pltpu.VMEM((2, rows + 1, cols, contact_pairs.shape[3]), i32),
            pltpu.VMEM((rows, cols), i32),
            pltpu.VMEM((rows, cols), i32),
            pltpu.VMEM((rows, cols), i32),
            pltpu.SMEM(movers_out.shape, i32),
            pltpu.SMEM(movers_in.shape, i32),
            pltpu.SMEM((1, 1, 2), i32),
            pltpu.VMEM(((rows + 1) * cols * 8, slots), f32),
            pltpu.VMEM(((rows + 1) * cols * 8, slots), f32),
            pltpu.VMEM((rows + 1, cols, slots), f32),
            pltpu.VMEM((rows, cols, slots), f32),
            pltpu.VMEM((rows + 2, cols + 2, 8, slots), f32),
            pltpu.VMEM((2, rows, 8, slots), f32),
            pltpu.VMEM((rows, 8, slots), f32),
            pltpu.VMEM((rows, 8, slots), f32),
            pltpu.VMEM((8, slots), f32),
            pltpu.VMEM((8, slots), f32),
            pltpu.VMEM((4, 8, slots), f32),
            pltpu.VMEM((4, 8, slots), f32),
            pltpu.VMEM((cols, 8, slots), f32),
            pltpu.VMEM((2, 8, slots), f32),
            pltpu.VMEM((2, message, slots), f32),
            pltpu.VMEM((2, message, slots), f32),
            pltpu.VMEM((2, padded, slots), f32),
            pltpu.SemaphoreType.DMA((8,)),
            pltpu.SemaphoreType.DMA((remote_copies,)),
            pltpu.SemaphoreType.DMA((remote_copies,)),
        ],
        compiler_params=pltpu.CompilerParams(
            collective_id=0, has_side_effects=True, vmem_limit_bytes=VMEM_GRANT
        ),
    )(
        *(
            pltpu.with_memory_space_constraint(x, pltpu.HBM)
            for x in (
                particles,
                filled,
                contact_pairs,
                contact_count,
                movers_out,
                movers_in,
                jnp.transpose(move_count, (1, 2, 0)),
            )
        )
    )


def solution(mesh):
    sizes = dict(mesh.shape)
    return jax.shard_map(
        functools.partial(body, sizes["blade"], sizes["span"], far_boundaries(mesh)),
        mesh=mesh,
        in_specs=(
            P(None, "blade", "span", None),
            P("blade", "span"),
            P(None, "blade", "span", None),
            P("blade", "span"),
            P(None, None, "blade", "span"),
            P(None, None, "blade", "span"),
            P(None, "blade", "span"),
        ),
        out_specs=P(None, "blade", "span", None),
        check_vma=False,
    )
```
